32 devices in a mesh: ep: 8 (over z, x), tp: 4 (over y, core).
Axes of the slice: x: 2, y: 2, z: 4, core: 2. Of those that a mesh axis runs over, the one named last changes fastest.
Arguments:
- tokens: bfloat16 [2048, 2880], P('ep', 'tp'), may hold values from -6 to 6
- expert_ids: int32 [2048, 4], P('ep'), may hold values from 0 to 15, all different within a row; in each aligned block of 256 rows (0 to 255, 256 to 511, ...) at most 128 rows name the same one
- combine_weights: float32 [2048, 4], P('ep'), may hold values from 0.05 to 0.6
- gate_weight: bfloat16 [16, 2880, 2880], P('ep', None, 'tp'), may hold values from -0.109375 to 0.109375
- up_weight: bfloat16 [16, 2880, 2880], P('ep', None, 'tp'), may hold values from -0.109375 to 0.109375
- down_weight: bfloat16 [16, 2880, 2880], P('ep', 'tp'), may hold values from -0.109375 to 0.109375
Outputs:
- mixed: bfloat16 [2048, 2880], P('ep', 'tp')
The draws below stay inside these ranges and needn't reach their ends.
Inputs may be any that keep to these rules, and one draw needn't show every extreme that they name: `expert_ids`: each row names 4 different experts; within the 256 rows of one index of ep no expert is named more than 128 times, a bound that some block reaches.
All inputs are finite; a program needn't handle non-finite values.
Results may differ from the reference program's by a relative error of at most 0.014.
Values may be sent and summed in bfloat16 or wider, within the bound.
A program may use at most 128 MiB of HBM per device.

```python
import math
import jax
import jax.numpy as jnp
import numpy as np
from jax import lax

D = 2880
FF = 2880
TOP = 4
TOK_DEV = 256
EXPERTS = 16
TOKENS = 2048
CAP = 128
FF_DEV = 720
N_EP = 8
N_TP = 4


def shard_levels(stream_key, shape, pieces, smallest, high):
    factor_of = 1.0
    for axis_at, shards_of in pieces:
        heights = jax.random.uniform(jax.random.fold_in(jax.random.fold_in(stream_key, 6), axis_at), (shards_of,), jnp.float32, smallest / len(pieces), high / len(pieces))
        factor_of = factor_of * jnp.repeat(jnp.exp(heights), shape[axis_at] // shards_of).reshape((-1,) + (1,) * (len(shape) - 1 - axis_at))
    return factor_of


def assign_block(key, own, number, rows, count, top, most, skew):
    ranking = jax.random.permutation(key, count)
    packed, usual = portions_of(count, rows * top, most, skew, True), portions_of(count, rows * top, most, skew, False)
    places = jnp.arange(count)

    def named(tallies, offset_by):
        used = int((tallies > 0).sum())
        fixed = max(1, used // 4)
        moved = fixed + (places - fixed + offset_by * (used - fixed)) % max(1, count - fixed)
        return jnp.zeros((count,), jnp.int32).at[ranking[jnp.where(places < fixed, places, moved)]].set(jnp.asarray(tallies, jnp.int32))

    tallies = jnp.where(number % 4 == 0, named(packed, number // 4), named(usual, number - number // 4 - 1))
    mixed = jax.random.permutation(jax.random.fold_in(own, 3), count)
    donor, taker = mixed[0:count // 2 * 2:2], mixed[1:count // 2 * 2:2]
    margin = jnp.minimum(tallies[donor] - 1, most - tallies[taker]) // 2
    margin = jnp.where((donor == ranking[0]) | (taker == ranking[0]) | (tallies[taker] == 0), 0, jnp.maximum(margin, 0))
    moved = jax.random.randint(jax.random.fold_in(own, 4), (count // 2,), 0, 1 << 20) % (margin + 1)
    tallies = tallies.at[donor].add(-moved).at[taker].add(moved)
    labels = jnp.searchsorted(jnp.cumsum(tallies), jnp.arange(rows * top), side="right").astype(jnp.int32)
    table = labels.reshape(top, rows).T
    table = table[jax.random.permutation(jax.random.fold_in(own, 1), rows)]
    offset_by = jax.random.randint(jax.random.fold_in(own, 2), (rows, 1), 0, top)
    return jnp.take_along_axis(table, (jnp.arange(top)[None, :] + offset_by) % top, axis=1)


def portions_of(count, total, limit, skew, full):
    loads = [(1 << 20) // math.isqrt(rank ** skew) + 1 for rank in range(1, count + 1)]
    largest = limit if full else min(limit, max(-(-total // count), total * loads[0] // sum(loads)))
    least = 1 if total - largest >= count - 1 else 0
    holding, spare = [largest] + [least] * (count - 1), total - largest - least * (count - 1)
    while spare > 0:
        free = [i for i in range(1, count) if holding[i] < largest] or [i for i in range(1, count) if holding[i] < limit]
        pool, left = sum([loads[i] for i in free]), spare
        for i in free:
            extra = min(limit - holding[i], max(1, left * loads[i] // pool), spare)
            holding[i] = holding[i] + extra
            spare = spare - extra
    return np.array(holding)


def normal_values(rng, dims, width, reach, cuts=(), held_as=jnp.bfloat16):
    gain = shard_levels(rng, dims, cuts, -0.22, 0.18) if cuts else 1.0
    array = jax.random.normal(rng, dims, jnp.float32) * width * gain
    return jnp.minimum(jnp.maximum(array, -reach), reach).astype(held_as)


def setup_inputs(seed: int = 0) -> dict:
    seeds = jax.random.split(jax.random.key(seed), 7)
    tokens = normal_values(seeds[0], (TOKENS, D), 1.0, 6.0, ((0, 8), (1, 4)))
    expert_ids_keys = jax.random.split(jax.random.fold_in(seeds[1], 1), TOKENS // TOK_DEV)
    expert_ids_turns = jax.random.permutation(jax.random.fold_in(seeds[1], 3), TOKENS // TOK_DEV)
    expert_ids = jax.vmap(lambda own, number: assign_block(jax.random.fold_in(seeds[1], 2), own, number, TOK_DEV, EXPERTS, TOP, CAP, 2))(expert_ids_keys, expert_ids_turns).reshape((TOKENS, TOP))
    combine_weights = jnp.clip(jnp.exp(math.log(0.6) - 2.4849067 * jax.random.uniform(seeds[2], (TOKENS, TOP), jnp.float32) ** shard_levels(seeds[2], (TOKENS, TOP), ((0, 8),), -0.2, 0.2)), 0.05, 0.6)
    gate_weight = normal_values(seeds[3], (EXPERTS, D, FF), D ** -0.5, 0.109375, ((0, 8), (2, 4)))
    up_weight = normal_values(seeds[4], (EXPERTS, D, FF), D ** -0.5, 0.109375, ((0, 8), (2, 4)))
    down_weight = normal_values(seeds[5], (EXPERTS, FF, D), FF ** -0.5, 0.109375, ((0, 8), (1, 4)))
    return {"tokens": tokens, "expert_ids": expert_ids, "combine_weights": combine_weights, "gate_weight": gate_weight, "up_weight": up_weight, "down_weight": down_weight}


def activate(gate_acc, up_acc):
    return (up_acc + 1.0) * gate_acc * jax.nn.sigmoid(1.702 * gate_acc)


def reference(tokens, expert_ids, combine_weights, gate_weight, up_weight, down_weight):
    groups = expert_ids.reshape(N_EP, TOK_DEV * TOP)
    onehot = (groups[:, :, None] == jnp.arange(EXPERTS, dtype=jnp.int32)[None, None, :]).astype(jnp.int32)
    slot_pos = jnp.sum((jnp.cumsum(onehot, axis=1) - onehot) * onehot, axis=2)
    group_ids = jnp.arange(N_EP, dtype=jnp.int32)[:, None]
    flat_slot = ((groups * N_EP + group_ids) * CAP + slot_pos).reshape(-1)
    token_idx = (group_ids * TOK_DEV + jnp.arange(TOK_DEV * TOP, dtype=jnp.int32)[None, :] // TOP).reshape(-1)
    token_src = jnp.zeros((EXPERTS * N_EP * CAP,), jnp.int32).at[flat_slot].set(token_idx)
    slot_weight = jnp.zeros((EXPERTS * N_EP * CAP,), jnp.float32).at[flat_slot].set(combine_weights.reshape(-1))
    token_src = token_src.reshape(EXPERTS, N_EP * CAP)
    slot_weight = slot_weight.reshape(EXPERTS, N_EP * CAP)

    def per_expert(accum, inputs):
        row_src, row_weight, gate_cols, up_cols, down_rows = inputs
        row_data = tokens[row_src]
        gate_acc = jnp.dot(row_data, gate_cols, preferred_element_type=jnp.float32)
        up_acc = jnp.dot(row_data, up_cols, preferred_element_type=jnp.float32)
        hidden = activate(gate_acc, up_acc).astype(jnp.bfloat16)
        partials = jnp.einsum("rtf,tfd->rtd",
                              hidden.reshape(N_EP * CAP, N_TP, FF_DEV).astype(jnp.float32),
                              down_rows.reshape(N_TP, FF_DEV, D).astype(jnp.float32))
        rounded = lax.optimization_barrier(partials.astype(jnp.bfloat16))
        expert_out = jnp.sum(rounded.astype(jnp.float32), axis=1)
        accum = accum.at[row_src].add(row_weight[:, None] * expert_out)
        return accum, None

    accum = jnp.zeros((TOKENS, D), jnp.float32)
    accum, unused = lax.scan(per_expert, accum, (token_src, slot_weight, gate_weight, up_weight, down_weight))
    return accum.astype(jnp.bfloat16)
```

```python
import functools

import jax
import jax.numpy as jnp
from jax import lax
from jax.experimental import pallas as pl
from jax.experimental.pallas import tpu as pltpu
from jax.sharding import PartitionSpec as P


def activate(gate_acc, up_acc):
    return (up_acc + 1.0) * gate_acc * jax.nn.sigmoid(1.702 * gate_acc)


MESH = pl.DeviceIdType.MESH


class Place:
    def __init__(self, depth):
        self.depth = depth
        e, t = lax.axis_index("ep"), lax.axis_index("tp")
        self.z, self.x, self.y, self.c = e // 2, e % 2, t // 2, t % 2

    def device(self, k=0, dx=0, dy=0, dc=0):
        ep = (self.z + k) % self.depth * 2 + (self.x + dx) % 2
        tp = (self.y + dy) % 2 * 2 + (self.c + dc) % 2
        return ep, tp

    def block(self, k=0, dx=0, dy=0, dc=0):
        ep, tp = self.device(k, dx, dy, dc)
        return ep * 4 + tp

    def greet(self):
        barrier = pltpu.get_barrier_semaphore()
        near = [self.device(k=k) for k in range(1, self.depth)]
        near += [self.device(dx=1), self.device(dy=1), self.device(dc=1)]
        for who in near:
            pl.semaphore_signal(barrier, inc=1, device_id=who, device_id_type=MESH)
        pl.semaphore_wait(barrier, len(near))


def gather_kernel(depth, own, out, lane_recv, pair_recv, lane_send, pair_send, own_sem):
    here = Place(depth)
    half = own.shape[0] // 2
    sent = []

    def piece(k, dx, dy, part):
        rows = pl.ds(part * half, half)
        if (k, dx, dy) == (0, 0, 0):
            return own.at[rows]
        return out.at[here.block(k, dx, dy), rows]

    def lane_slot(k, dx, dy):
        ep, tp = here.device(k, dx, dy)
        return ep * 2 + tp // 2

    def push(k, dx, dy, part, to):
        rows = pl.ds(part * half, half)
        copy = pltpu.make_async_remote_copy(
            src_ref=piece(k, dx, dy, part), dst_ref=out.at[here.block(k, dx, dy), rows],
            send_sem=lane_send.at[len(sent)], recv_sem=lane_recv.at[lane_slot(k, dx, dy), part],
            device_id=to, device_id_type=MESH)
        copy.start()
        sent.append(copy)

    def pair(k, dx, dy, part):
        rows = pl.ds(part * half, half)
        slot = lane_slot(k, dx, dy)
        copy = pltpu.make_async_remote_copy(
            src_ref=piece(k, dx, dy, part), dst_ref=out.at[here.block(k, dx, dy), rows],
            send_sem=pair_send.at[slot, part], recv_sem=pair_recv.at[slot, part],
            device_id=here.device(dc=1), device_id_type=MESH)
        copy.start()

    def landed(k, dx, dy, part, to):
        rows = pl.ds(part * half, half)
        ref = out.at[here.block(k, dx, dy), rows]
        pltpu.make_async_remote_copy(
            src_ref=ref, dst_ref=ref, send_sem=lane_send.at[0],
            recv_sem=lane_recv.at[lane_slot(k, dx, dy), part],
            device_id=to, device_id_type=MESH).wait_recv()

    here.greet()
    over_x, over_y = here.device(dx=1), here.device(dy=1)
    for k in range(1, depth):
        for part in (0, 1):
            push(0, 0, 0, part, here.device(k=depth - k))
    store = pltpu.make_async_copy(own, out.at[here.block()], own_sem)
    store.start()
    for k in range(depth):
        if k:
            landed(k, 0, 0, 0, here.device(k=k))
            landed(k, 0, 0, 1, here.device(k=k))
        push(k, 0, 0, 0, over_x)
        push(k, 0, 0, 1, over_y)
        push(k, 0, 0, 0, over_y)
        push(k, 0, 0, 1, over_x)
        pair(k, 0, 0, 0)
        pair(k, 0, 0, 1)
        landed(k, 1, 0, 0, over_x)
        push(k, 1, 0, 0, over_y)
        pair(k, 1, 0, 0)
        landed(k, 0, 1, 1, over_y)
        push(k, 0, 1, 1, over_x)
        pair(k, 0, 1, 1)
    for k in range(depth):
        landed(k, 0, 1, 0, over_y)
        pair(k, 0, 1, 0)
        landed(k, 1, 0, 1, over_x)
        pair(k, 1, 0, 1)
        landed(k, 1, 1, 0, over_y)
        pair(k, 1, 1, 0)
        landed(k, 1, 1, 1, over_x)
        pair(k, 1, 1, 1)
    store.wait()
    for copy in sent:
        copy.wait_send()
    for k in range(depth):
        for dx in (0, 1):
            for dy in (0, 1):
                slot = lane_slot(k, dx, dy)
                for part in (0, 1):
                    rows = pl.ds(part * half, half)
                    copy = pltpu.make_async_remote_copy(
                        src_ref=piece(k, dx, dy, part),
                        dst_ref=out.at[here.block(k, dx, dy, 1), rows],
                        send_sem=pair_send.at[slot, part], recv_sem=pair_recv.at[slot, part],
                        device_id=here.device(dc=1), device_id_type=MESH)
                    copy.wait_send()
                    copy.wait_recv()


def gather_all(tokens, ep_count, tp_count):
    rows, width = tokens.shape
    depth = ep_count // 2
    blocks = ep_count * tp_count
    sends = 2 * (depth - 1) + 6 * depth
    dma = pltpu.SemaphoreType.DMA
    return pl.pallas_call(
        functools.partial(gather_kernel, depth),
        out_shape=jax.ShapeDtypeStruct((blocks, rows, width), tokens.dtype),
        in_specs=[pl.BlockSpec(memory_space=pltpu.VMEM)],
        out_specs=pl.BlockSpec(memory_space=pl.ANY),
        scratch_shapes=[dma((blocks // 2, 2)), dma((blocks // 2, 2)), dma((sends,)),
                        dma((blocks // 2, 2)), dma(())],
        compiler_params=pltpu.CompilerParams(collective_id=0, has_side_effects=True),
    )(tokens)


def scatter_kernel(depth, part_ref, out, acc, inc, from_y, from_x, last_x, last_y, from_z,
                   load_sem, pair_send, pair_recv, send_sem, recv_sem):
    here = Place(depth)
    rows = out.shape[0]
    half = rows // 2
    low, high = pl.ds(0, half), pl.ds(half, half)
    order = list(range(1, depth)) + [0]
    spread = ((1, 1), (0, 1), (1, 0), (0, 0))
    over_x, over_y = here.device(dx=1), here.device(dy=1)
    sent = []
    loads, pairs = {}, {}
    cell = lambda k, dx, dy: (k * 2 + dx) * 2 + dy

    def add(at, part, got):
        acc[at, part] = (acc[at, part].astype(jnp.float32) + got.astype(jnp.float32)).astype(acc.dtype)

    def send(src, dst, to):
        copy = pltpu.make_async_remote_copy(
            src_ref=src, dst_ref=dst, send_sem=send_sem.at[len(sent)],
            recv_sem=recv_sem.at[len(sent)], device_id=to, device_id_type=MESH)
        copy.start()
        sent.append(copy)
        return copy

    here.greet()
    for k in order:
        for dx, dy in spread:
            i = cell(k, dx, dy)
            pairs[i] = pltpu.make_async_remote_copy(
                src_ref=part_ref.at[here.block(k, dx, dy, 1)], dst_ref=inc.at[i],
                send_sem=pair_send.at[i], recv_sem=pair_recv.at[i],
                device_id=here.device(dc=1), device_id_type=MESH)
            pairs[i].start()
            loads[i] = pltpu.make_async_copy(
                part_ref.at[here.block(k, dx, dy)], acc.at[i], load_sem.at[i])
            loads[i].start()

    wait_for = {}

    def first(k):
        for dx, dy in spread:
            i = cell(k, dx, dy)
            loads[i].wait()
            pairs[i].wait_recv()
            add(i, pl.ds(0, rows), inc[i])
            if dy:
                wait_for["y", k, dx] = send(acc.at[i, low], from_y.at[k * 2 + dx], over_y)
            if dx:
                wait_for["x", k, dy] = send(acc.at[i, high], from_x.at[k * 2 + dy], over_x)

    def second(k):
        wait_for["y", k, 1].wait_recv()
        add(cell(k, 1, 0), low, from_y[k * 2 + 1])
        wait_for["lx", k] = send(acc.at[cell(k, 1, 0), low], last_x.at[k], over_x)
        wait_for["x", k, 1].wait_recv()
        add(cell(k, 0, 1), high, from_x[k * 2 + 1])
        wait_for["ly", k] = send(acc.at[cell(k, 0, 1), high], last_y.at[k], over_y)
        wait_for["y", k, 0].wait_recv()
        add(cell(k, 0, 0), low, from_y[k * 2])
        wait_for["x", k, 0].wait_recv()
        add(cell(k, 0, 0), high, from_x[k * 2])

    def third(k):
        wait_for["lx", k].wait_recv()
        add(cell(k, 0, 0), low, last_x[k])
        wait_for["ly", k].wait_recv()
        add(cell(k, 0, 0), high, last_y[k])
        if k:
            wait_for["z", k] = send(acc.at[cell(k, 0, 0)], from_z.at[k - 1], here.device(k=k))

    for i in range(depth + 2):
        if i < depth:
            first(order[i])
        if 0 <= i - 1 < depth:
            second(order[i - 1])
        if 0 <= i - 2:
            third(order[i - 2])
    total = acc[0].astype(jnp.float32)
    for k in range(1, depth):
        wait_for["z", k].wait_recv()
        total = total + from_z[k - 1].astype(jnp.float32)
    out[...] = total.astype(out.dtype)
    for copy in sent:
        copy.wait_send()
    for copy in pairs.values():
        copy.wait_send()


def scatter_sum(partial, ep_count):
    blocks, rows, width = partial.shape
    depth = ep_count // 2
    lane, half = blocks // 2, rows // 2
    sends = 6 * depth + depth - 1
    dma, kind = pltpu.SemaphoreType.DMA, partial.dtype
    return pl.pallas_call(
        functools.partial(scatter_kernel, depth),
        out_shape=jax.ShapeDtypeStruct((rows, width), kind),
        in_specs=[pl.BlockSpec(memory_space=pl.ANY)],
        out_specs=pl.BlockSpec(memory_space=pltpu.VMEM),
        scratch_shapes=[
            pltpu.VMEM((lane, rows, width), kind), pltpu.VMEM((lane, rows, width), kind),
            pltpu.VMEM((2 * depth, half, width), kind), pltpu.VMEM((2 * depth, half, width), kind),
            pltpu.VMEM((depth, half, width), kind), pltpu.VMEM((depth, half, width), kind),
            pltpu.VMEM((depth - 1, rows, width), kind),
            dma((lane,)), dma((lane,)), dma((lane,)), dma((sends,)), dma((sends,)),
        ],
        compiler_params=pltpu.CompilerParams(
            collective_id=1, has_side_effects=True, vmem_limit_bytes=48 * 1024 * 1024),
    )(partial)


def act_weighted(gate_acc, up_acc, weight):
    return (activate(gate_acc, up_acc) * weight).astype(jnp.bfloat16)


PUSHES = (((0, 0), 0, "x"), ((0, 0), 1, "y"), ((0, 0), 0, "y"), ((0, 0), 1, "x"),
          ((1, 0), 0, "y"), ((0, 1), 1, "x"))


class Grid:
    def __init__(self):
        e, t = lax.axis_index("ep"), lax.axis_index("tp")
        self.ep, self.tp = e, t
        self.z, self.x, self.y, self.c = e // 2, e % 2, t // 2, t % 2

    def device(self, k=0, dx=0, dy=0, dc=0):
        z = (self.z // 2 + k // 2) % 2 * 2 + (self.z % 2 + k % 2) % 2
        return z * 2 + (self.x + dx) % 2, (self.y + dy) % 2 * 2 + (self.c + dc) % 2


def fused_kernel(tokens, meta, gate, up, down, out, buf, inc, from_y, from_x, last_x, last_y,
                 from_z, wide, deep, rows, hid, take, back, weigh, place, metas,
                 own_sem, w_sem, meta_send, meta_recv, z_send, z_recv, lane_send, lane_recv,
                 pair_send, pair_recv, sp_send, sp_recv, sx_send, sx_recv, sz_send, sz_recv):
    f32, bf16 = jnp.float32, jnp.bfloat16
    here = Grid()
    depth = from_z.shape[0] + 1
    tok, feat = buf.shape[1], buf.shape[2]
    half = tok // 2
    experts, cap = rows.shape[1], rows.shape[2]
    lanes = rows.shape[3] // 4
    ff = hid.shape[1]
    width = deep.shape[2]
    low, high = pl.ds(0, half), pl.ds(half, half)
    parts = (low, high)
    over = {"x": here.device(dx=1), "y": here.device(dy=1)}
    partner = here.device(dc=1)

    def cell(k, dx, dy, dc):
        return k * 8 + dx * 4 + dy * 2 + dc

    def remote(src, dst, send, recv, to):
        return pltpu.make_async_remote_copy(
            src_ref=src, dst_ref=dst, send_sem=send, recv_sem=recv,
            device_id=to, device_id_type=MESH)

    def z_push(k, p):
        return remote(tokens.at[parts[p]], buf.at[cell(k, 0, 0, 0), parts[p]],
                      z_send.at[k, p], z_recv.at[k, p], here.device(k=k))

    def lane_push(k, n):
        (dx, dy), p, axis = PUSHES[n]
        to = (1 - dx, dy) if axis == "x" else (dx, 1 - dy)
        return remote(buf.at[cell(k, dx, dy, 0), parts[p]], buf.at[cell(k, *to, 0), parts[p]],
                      lane_send.at[k, n], lane_recv.at[k, n], over[axis])

    def pair(k, dx, dy, p):
        n = (dx * 2 + dy) * 2 + p
        return remote(buf.at[cell(k, dx, dy, 0), parts[p]], buf.at[cell(k, dx, dy, 1), parts[p]],
                      pair_send.at[k, n], pair_recv.at[k, n], partner)

    def meta_push(k, dx):
        n = k * 2 + dx
        return remote(meta, metas.at[n], meta_send.at[n], meta_recv.at[n], here.device(k=k, dx=dx))

    def gather_a(k):
        for n in range(4):
            lane_push(k, n).start()
        pair(k, 0, 0, 0).start()
        pair(k, 0, 0, 1).start()

    def column(k):
        z_push(k, 0).wait_recv()
        z_push(k, 1).wait_recv()
        gather_a(k)

    def gather_b(k):
        lane_push(k, 0).wait_recv()
        lane_push(k, 4).start()
        pair(k, 1, 0, 0).start()
        lane_push(k, 1).wait_recv()
        lane_push(k, 5).start()
        pair(k, 0, 1, 1).start()

    def gather_c(k, first):
        if first:
            lane_push(k, 2).wait_recv()
            pair(k, 0, 1, 0).start()
            lane_push(k, 3).wait_recv()
            pair(k, 1, 0, 1).start()
        else:
            lane_push(k, 4).wait_recv()
            pair(k, 1, 1, 0).start()
            lane_push(k, 5).wait_recv()
            pair(k, 1, 1, 1).start()

    def gather_d(k):
        for dx in (0, 1):
            for dy in (0, 1):
                for p in (0, 1):
                    pair(k, dx, dy, p).wait_recv()

    def gather_sent(k):
        for n in range(6):
            lane_push(k, n).wait_send()
        for dx in (0, 1):
            for dy in (0, 1):
                for p in (0, 1):
                    pair(k, dx, dy, p).wait_send()

    def give(k, dx, dy):
        n = dx * 2 + dy
        return remote(buf.at[cell(k, dx, dy, 1)], inc.at[k * 4 + n],
                      sp_send.at[k, n], sp_recv.at[k, n], partner)

    def hop(k, n):
        src, dst, axis = (
            (buf.at[cell(k, 1, 1, 0), low], from_y.at[k * 2 + 1], "y"),
            (buf.at[cell(k, 0, 1, 0), low], from_y.at[k * 2], "y"),
            (buf.at[cell(k, 1, 1, 0), high], from_x.at[k * 2 + 1], "x"),
            (buf.at[cell(k, 1, 0, 0), high], from_x.at[k * 2], "x"),
            (buf.at[cell(k, 1, 0, 0), low], last_x.at[k], "x"),
            (buf.at[cell(k, 0, 1, 0), high], last_y.at[k], "y"))[n]
        return remote(src, dst, sx_send.at[k, n], sx_recv.at[k, n], over[axis])

    def home(k):
        return remote(buf.at[cell(k, 0, 0, 0)], from_z.at[k - 1],
                      sz_send.at[k], sz_recv.at[k], here.device(k=k))

    def add(at, part, got):
        buf[at, part] = (buf[at, part].astype(f32) + got.astype(f32)).astype(bf16)

    def scatter_b(k):
        for dx, dy in ((1, 1), (0, 1), (1, 0), (0, 0)):
            give(k, dx, dy).wait_recv()
            add(cell(k, dx, dy, 0), pl.ds(0, tok), inc[k * 4 + dx * 2 + dy])
            if dy:
                hop(k, 1 - dx).start()
            if dx:
                hop(k, 3 - dy).start()

    def scatter_c(k):
        hop(k, 0).wait_recv()
        add(cell(k, 1, 0, 0), low, from_y[k * 2 + 1])
        hop(k, 4).start()
        hop(k, 2).wait_recv()
        add(cell(k, 0, 1, 0), high, from_x[k * 2 + 1])
        hop(k, 5).start()
        hop(k, 1).wait_recv()
        add(cell(k, 0, 0, 0), low, from_y[k * 2])
        hop(k, 3).wait_recv()
        add(cell(k, 0, 0, 0), high, from_x[k * 2])

    def scatter_d(k):
        hop(k, 4).wait_recv()
        add(cell(k, 0, 0, 0), low, last_x[k])
        hop(k, 5).wait_recv()
        add(cell(k, 0, 0, 0), high, last_y[k])

    own = pltpu.make_async_copy(tokens, buf.at[cell(0, 0, 0, 0)], own_sem)
    own.start()
    barrier = pltpu.get_barrier_semaphore()
    near = [here.device(k=k, dx=dx) for k in range(depth) for dx in (0, 1) if k or dx]
    near += [over["y"], partner]
    for who in near:
        pl.semaphore_signal(barrier, inc=1, device_id=who, device_id_type=MESH)
    pl.semaphore_wait(barrier, len(near))
    for k in range(depth):
        for dx in (0, 1):
            if k or dx:
                meta_push(k, dx).start()
    for k in range(1, depth):
        z_push(k, 0).start()
        z_push(k, 1).start()
    own.wait()
    gather_a(0)
    loads = []
    for e in range(experts):
        for side, ref in enumerate((gate, up)):
            for j in range(4):
                loads.append(pltpu.make_async_copy(
                    ref.at[e, pl.ds(j * feat, feat)], wide.at[side, e, pl.ds(j * lanes, feat)],
                    w_sem.at[len(loads)]))
        loads.append(pltpu.make_async_copy(down.at[e], deep.at[e], w_sem.at[len(loads)]))
    for load in loads:
        load.start()
    metas[0] = meta[...]
    place[...] = jnp.zeros(place.shape, f32)
    for j in range(4):
        edge = pl.ds(j * lanes + feat, lanes - feat)
        for e in range(experts):
            for side in (0, 1):
                wide[side, e, edge, :] = jnp.zeros((lanes - feat, ff), bf16)
            for dx in (0, 1):
                rows[dx, e, :, edge] = jnp.zeros((cap, lanes - feat), bf16)
    gather_b(0)
    column(1)
    gather_c(0, True)
    gather_c(0, False)
    for load in loads:
        load.wait()

    ahead = (lax.broadcasted_iota(jnp.int32, (tok, tok), 0)
             < lax.broadcasted_iota(jnp.int32, (tok, tok), 1)).astype(f32).astype(bf16)
    slot_row = lax.broadcasted_iota(jnp.int32, (cap, tok), 0).astype(f32)
    slot_col = lax.broadcasted_iota(jnp.int32, (tok, cap), 1).astype(f32)
    row_at = lax.broadcasted_iota(jnp.int32, (8, tok), 0)

    def masks(k):
        picked = jnp.zeros((8, tok), f32)
        weights = []
        for dx in (0, 1):
            info = metas[k * 2 + dx]
            for e in range(experts):
                mine = (here.ep * experts + e).astype(f32)
                hit = (info[0:4] == mine).astype(f32)
                chosen = jnp.sum(hit, axis=0, keepdims=True)
                weights.append(jnp.sum(hit * info[4:8], axis=0, keepdims=True))
                picked = jnp.where(row_at == dx * experts + e, chosen, picked)
        slot = jnp.dot(picked.astype(bf16), ahead, preferred_element_type=f32)
        slot = jnp.where(picked > 0.5, slot, -1.0)
        place[0:8, :] = slot
        turned = jnp.transpose(place[...])
        for dx in (0, 1):
            for e in range(experts):
                n = dx * experts + e
                at = pl.ds(e * cap, cap)
                hot = (slot_row == slot[n:n + 1, :]).astype(f32)
                take[dx, at, :] = hot.astype(bf16)
                held = jnp.sum(hot * weights[n], axis=1, keepdims=True)
                weigh[e, pl.ds(dx * cap, cap), :] = jnp.broadcast_to(held, (cap, 128))
                back[dx, :, at] = (slot_col == turned[:, n:n + 1]).astype(f32).astype(bf16)

    def block(k, dx, j):
        return cell(k, dx, (here.y + j // 2) % 2, (here.c + j % 2) % 2)

    def dispatch(k):
        for dx in (0, 1):
            for j in range(4):
                got = jnp.dot(take[dx], buf[block(k, dx, j)], preferred_element_type=f32)
                rows[dx, :, :, pl.ds(j * lanes, feat)] = got.astype(bf16).reshape(experts, cap, feat)

    def enter(e):
        held = rows[:, e].reshape(2 * cap, 4 * lanes)
        for n in range(0, ff, 256):
            at = pl.ds(n, min(256, ff - n))
            g = jnp.dot(held, wide[0, e, :, at], preferred_element_type=f32)
            u = jnp.dot(held, wide[1, e, :, at], preferred_element_type=f32)
            hid[:, at] = act_weighted(g, u, weigh[e, :, 0:1])

    def leave(e):
        for n in range(0, width, 512):
            size = min(512, width - n)
            got = jnp.dot(hid[...], deep[e, :, pl.ds(n, size)], preferred_element_type=f32)
            rows[:, e, :, pl.ds(n, size)] = got.astype(bf16).reshape(2, cap, size)

    def combine(k, dx):
        for j in range(4):
            part = rows[dx, :, :, pl.ds(j * feat, feat)].reshape(experts * cap, feat)
            got = jnp.dot(back[dx], part, preferred_element_type=f32)
            buf[block(k, dx, j)] = got.astype(bf16)

    def plane(k, carry):
        last = depth - 1
        gather_d(k)

        @pl.when(k > 0)
        def _():
            meta_push(k, 0).wait_recv()
        meta_push(k, 1).wait_recv()
        masks(k)
        dispatch(k)

        @pl.when(k < last)
        def _():
            gather_b(k + 1)
        enter(0)

        @pl.when(k < last - 1)
        def _():
            column(k + 2)

        @pl.when(k > 1)
        def _():
            scatter_b(k - 1)
        leave(0)
        enter(1)

        @pl.when(k < last)
        def _():
            gather_c(k + 1, True)
        leave(1)
        gather_sent(k)

        @pl.when(k < last)
        def _():
            gather_c(k + 1, False)
        for dx in (1, 0):
            combine(k, dx)
            give(k, dx, 1).start()
            give(k, dx, 0).start()
        return carry

    lax.fori_loop(0, depth, plane, 0)

    scatter_c(1)
    scatter_b(3)
    scatter_c(2)
    scatter_d(1)
    home(1).start()
    scatter_b(0)
    scatter_c(3)
    scatter_d(2)
    home(2).start()
    scatter_c(0)
    scatter_d(3)
    home(3).start()
    scatter_d(0)
    total = buf[cell(0, 0, 0, 0)].astype(f32)
    for k in range(1, depth):
        home(k).wait_recv()
        total = total + from_z[k - 1].astype(f32)
    out[...] = total.astype(out.dtype)
    for k in range(depth):
        for dx in (0, 1):
            if k or dx:
                meta_push(k, dx).wait_send()
            for dy in (0, 1):
                give(k, dx, dy).wait_send()
        for n in range(6):
            hop(k, n).wait_send()
        if k:
            z_push(k, 0).wait_send()
            z_push(k, 1).wait_send()
            home(k).wait_send()


def fused(tokens, expert_ids, combine_weights, gate_weight, up_weight, down_weight, depth, capacity):
    tok, feat = tokens.shape
    experts, width, ff = gate_weight.shape
    f32, bf16 = jnp.float32, jnp.bfloat16
    lanes = -(-feat // 128) * 128
    half = tok // 2
    meta = jnp.concatenate([expert_ids.T.astype(f32), combine_weights.T], axis=0)
    dma = pltpu.SemaphoreType.DMA
    any_space, vmem = pl.BlockSpec(memory_space=pl.ANY), pl.BlockSpec(memory_space=pltpu.VMEM)
    loads = experts * 9
    scratch = [
        pltpu.VMEM((depth * 8, tok, feat), bf16), pltpu.VMEM((depth * 4, tok, feat), bf16),
        pltpu.VMEM((depth * 2, half, feat), bf16), pltpu.VMEM((depth * 2, half, feat), bf16),
        pltpu.VMEM((depth, half, feat), bf16), pltpu.VMEM((depth, half, feat), bf16),
        pltpu.VMEM((depth - 1, tok, feat), bf16),
        pltpu.VMEM((2, experts, 4 * lanes, ff), bf16), pltpu.VMEM((experts, ff, width), bf16),
        pltpu.VMEM((2, experts, capacity, 4 * lanes), bf16),
        pltpu.VMEM((2 * capacity, ff), bf16),
        pltpu.VMEM((2, experts * capacity, tok), bf16), pltpu.VMEM((2, tok, experts * capacity), bf16),
        pltpu.VMEM((experts, 2 * capacity, 128), f32), pltpu.VMEM((128, tok), f32),
        pltpu.VMEM((depth * 2, 8, tok), f32),
        dma(()), dma((loads,)), dma((depth * 2,)), dma((depth * 2,)),
        dma((depth, 2)), dma((depth, 2)), dma((depth, 6)), dma((depth, 6)),
        dma((depth, 8)), dma((depth, 8)), dma((depth, 4)), dma((depth, 4)),
        dma((depth, 6)), dma((depth, 6)), dma((depth,)), dma((depth,)),
    ]
    return pl.pallas_call(
        fused_kernel,
        out_shape=jax.ShapeDtypeStruct((tok, feat), bf16),
        in_specs=[any_space, vmem, any_space, any_space, any_space],
        out_specs=vmem,
        scratch_shapes=scratch,
        compiler_params=pltpu.CompilerParams(
            collective_id=0, has_side_effects=True, vmem_limit_bytes=63 * 1024 * 1024),
    )(tokens, meta, gate_weight, up_weight, down_weight)


def local(tokens, expert_ids, combine_weights, gate_weight, up_weight, down_weight):
    ep_count = lax.axis_size("ep")
    tp_count = lax.axis_size("tp")
    exp_local = gate_weight.shape[0]
    experts = exp_local * ep_count
    tok_rows = expert_ids.shape[0]
    top_count = expert_ids.shape[1]
    capacity = 2 * tok_rows * top_count // experts
    feat_width = tokens.shape[1]
    ff_width = gate_weight.shape[2]
    width = feat_width * tp_count
    f32, bf16 = jnp.float32, jnp.bfloat16
    if (ep_count, tp_count, exp_local, top_count) == (8, 4, 2, 4) and capacity % 128 == 0:
        return fused(tokens, expert_ids, combine_weights, gate_weight, up_weight, down_weight,
                     ep_count // 2, capacity)

    ids_all = lax.all_gather(expert_ids.T, "ep")
    weights_all = lax.all_gather(combine_weights.T, "ep")
    first = lax.axis_index("ep") * exp_local
    mine = first + jnp.arange(exp_local, dtype=jnp.int32)
    hit = ids_all[:, None, :, :] == mine[None, :, None, None]
    chosen = jnp.any(hit, axis=2)
    weight = jnp.sum(jnp.where(hit, weights_all[:, None, :, :], 0.0), axis=2)

    ahead = jnp.triu(jnp.ones((tok_rows, tok_rows), bf16), 1)
    slot = lax.dot_general(
        chosen.reshape(-1, tok_rows).astype(bf16), ahead, (((1,), (0,)), ((), ())),
        preferred_element_type=f32,
    ).astype(jnp.int32).reshape(chosen.shape)
    place = jnp.where(chosen, slot, -1)
    take = place[:, :, None, :] == jnp.arange(capacity, dtype=jnp.int32)[None, None, :, None]
    slot_weight = jnp.sum(jnp.where(take, weight[:, :, None, :], 0.0), axis=3)
    take = take.astype(bf16)

    paired = tp_count == 2 * 2 and ep_count % 2 == 0
    spread = gather_all(tokens, ep_count, tp_count) if paired else lax.all_gather(
        tokens, ("ep", "tp")
    )
    gathered = spread.reshape(
        ep_count, tp_count, tok_rows, feat_width
    )
    routed = jnp.einsum(
        "sect,sjtf->escjf", take, gathered, preferred_element_type=f32
    ).astype(bf16)
    rows = routed.reshape(exp_local, ep_count * capacity, width)
    gate_new = jnp.einsum("erd,edf->erf", rows, gate_weight, preferred_element_type=f32)
    up_new = jnp.einsum("erd,edf->erf", rows, up_weight, preferred_element_type=f32)
    row_weight = slot_weight.transpose(1, 0, 2).reshape(exp_local, ep_count * capacity, 1)
    hidden = (activate(gate_new, up_new) * row_weight).astype(bf16)
    expert_out = jnp.einsum(
        "erf,efd->erd", hidden, down_weight, preferred_element_type=f32
    ).astype(bf16)
    expert_out = expert_out.reshape(exp_local, ep_count, capacity, tp_count, feat_width)
    partial = jnp.einsum(
        "sect,escjf->sjtf", take, expert_out, preferred_element_type=f32
    ).astype(bf16)
    partial = partial.reshape(ep_count * tp_count, tok_rows, feat_width)
    if paired:
        return scatter_sum(partial, ep_count)
    mixed = lax.psum_scatter(partial, ("ep", "tp"), scatter_dimension=0, tiled=True)
    return mixed.reshape(tok_rows, feat_width)


def solution(mesh):
    in_specs = (
        P("ep", "tp"),
        P("ep", None),
        P("ep", None),
        P("ep", None, "tp"),
        P("ep", None, "tp"),
        P("ep", "tp", None),
    )
    out_specs = P("ep", "tp")
    return jax.shard_map(local, mesh=mesh, in_specs=in_specs, out_specs=out_specs, check_vma=False)
```

```python
import functools

import jax
import jax.numpy as jnp
from jax import lax
from jax.experimental import pallas as pl
from jax.experimental.pallas import tpu as pltpu
from jax.sharding import PartitionSpec as P


def activate(gate_acc, up_acc):
    return (up_acc + 1.0) * gate_acc * jax.nn.sigmoid(1.702 * gate_acc)


MESH = pl.DeviceIdType.MESH


class Place:
    def __init__(self, depth):
        self.depth = depth
        e, t = lax.axis_index("ep"), lax.axis_index("tp")
        self.z, self.x, self.y, self.c = e // 2, e % 2, t // 2, t % 2

    def device(self, k=0, dx=0, dy=0, dc=0):
        ep = (self.z + k) % self.depth * 2 + (self.x + dx) % 2
        tp = (self.y + dy) % 2 * 2 + (self.c + dc) % 2
        return ep, tp

    def block(self, k=0, dx=0, dy=0, dc=0):
        ep, tp = self.device(k, dx, dy, dc)
        return ep * 4 + tp

    def greet(self):
        barrier = pltpu.get_barrier_semaphore()
        near = [self.device(k=k) for k in range(1, self.depth)]
        near += [self.device(dx=1), self.device(dy=1), self.device(dc=1)]
        for who in near:
            pl.semaphore_signal(barrier, inc=1, device_id=who, device_id_type=MESH)
        pl.semaphore_wait(barrier, len(near))


def gather_kernel(depth, own, out, lane_recv, pair_recv, lane_send, pair_send, own_sem):
    here = Place(depth)
    half = own.shape[0] // 2
    sent = []

    def piece(k, dx, dy, part):
        rows = pl.ds(part * half, half)
        if (k, dx, dy) == (0, 0, 0):
            return own.at[rows]
        return out.at[here.block(k, dx, dy), rows]

    def lane_slot(k, dx, dy):
        ep, tp = here.device(k, dx, dy)
        return ep * 2 + tp // 2

    def push(k, dx, dy, part, to):
        rows = pl.ds(part * half, half)
        copy = pltpu.make_async_remote_copy(
            src_ref=piece(k, dx, dy, part), dst_ref=out.at[here.block(k, dx, dy), rows],
            send_sem=lane_send.at[len(sent)], recv_sem=lane_recv.at[lane_slot(k, dx, dy), part],
            device_id=to, device_id_type=MESH)
        copy.start()
        sent.append(copy)

    def pair(k, dx, dy, part):
        rows = pl.ds(part * half, half)
        slot = lane_slot(k, dx, dy)
        copy = pltpu.make_async_remote_copy(
            src_ref=piece(k, dx, dy, part), dst_ref=out.at[here.block(k, dx, dy), rows],
            send_sem=pair_send.at[slot, part], recv_sem=pair_recv.at[slot, part],
            device_id=here.device(dc=1), device_id_type=MESH)
        copy.start()

    def landed(k, dx, dy, part, to):
        rows = pl.ds(part * half, half)
        ref = out.at[here.block(k, dx, dy), rows]
        pltpu.make_async_remote_copy(
            src_ref=ref, dst_ref=ref, send_sem=lane_send.at[0],
            recv_sem=lane_recv.at[lane_slot(k, dx, dy), part],
            device_id=to, device_id_type=MESH).wait_recv()

    here.greet()
    over_x, over_y = here.device(dx=1), here.device(dy=1)
    for k in range(1, depth):
        for part in (0, 1):
            push(0, 0, 0, part, here.device(k=depth - k))
    store = pltpu.make_async_copy(own, out.at[here.block()], own_sem)
    store.start()
    for k in range(depth):
        if k:
            landed(k, 0, 0, 0, here.device(k=k))
            landed(k, 0, 0, 1, here.device(k=k))
        push(k, 0, 0, 0, over_x)
        push(k, 0, 0, 1, over_y)
        push(k, 0, 0, 0, over_y)
        push(k, 0, 0, 1, over_x)
        pair(k, 0, 0, 0)
        pair(k, 0, 0, 1)
        landed(k, 1, 0, 0, over_x)
        push(k, 1, 0, 0, over_y)
        pair(k, 1, 0, 0)
        landed(k, 0, 1, 1, over_y)
        push(k, 0, 1, 1, over_x)
        pair(k, 0, 1, 1)
    for k in range(depth):
        landed(k, 0, 1, 0, over_y)
        pair(k, 0, 1, 0)
        landed(k, 1, 0, 1, over_x)
        pair(k, 1, 0, 1)
        landed(k, 1, 1, 0, over_y)
        pair(k, 1, 1, 0)
        landed(k, 1, 1, 1, over_x)
        pair(k, 1, 1, 1)
    store.wait()
    for copy in sent:
        copy.wait_send()
    for k in range(depth):
        for dx in (0, 1):
            for dy in (0, 1):
                slot = lane_slot(k, dx, dy)
                for part in (0, 1):
                    rows = pl.ds(part * half, half)
                    copy = pltpu.make_async_remote_copy(
                        src_ref=piece(k, dx, dy, part),
                        dst_ref=out.at[here.block(k, dx, dy, 1), rows],
                        send_sem=pair_send.at[slot, part], recv_sem=pair_recv.at[slot, part],
                        device_id=here.device(dc=1), device_id_type=MESH)
                    copy.wait_send()
                    copy.wait_recv()


def gather_all(tokens, ep_count, tp_count):
    rows, width = tokens.shape
    depth = ep_count // 2
    blocks = ep_count * tp_count
    sends = 2 * (depth - 1) + 6 * depth
    dma = pltpu.SemaphoreType.DMA
    return pl.pallas_call(
        functools.partial(gather_kernel, depth),
        out_shape=jax.ShapeDtypeStruct((blocks, rows, width), tokens.dtype),
        in_specs=[pl.BlockSpec(memory_space=pltpu.VMEM)],
        out_specs=pl.BlockSpec(memory_space=pl.ANY),
        scratch_shapes=[dma((blocks // 2, 2)), dma((blocks // 2, 2)), dma((sends,)),
                        dma((blocks // 2, 2)), dma(())],
        compiler_params=pltpu.CompilerParams(collective_id=0, has_side_effects=True),
    )(tokens)


def scatter_kernel(depth, part_ref, out, acc, inc, from_y, from_x, last_x, last_y, from_z,
                   load_sem, pair_send, pair_recv, send_sem, recv_sem):
    here = Place(depth)
    rows = out.shape[0]
    half = rows // 2
    low, high = pl.ds(0, half), pl.ds(half, half)
    order = list(range(1, depth)) + [0]
    spread = ((1, 1), (0, 1), (1, 0), (0, 0))
    over_x, over_y = here.device(dx=1), here.device(dy=1)
    sent = []
    loads, pairs = {}, {}
    cell = lambda k, dx, dy: (k * 2 + dx) * 2 + dy

    def add(at, part, got):
        acc[at, part] = (acc[at, part].astype(jnp.float32) + got.astype(jnp.float32)).astype(acc.dtype)

    def send(src, dst, to):
        copy = pltpu.make_async_remote_copy(
            src_ref=src, dst_ref=dst, send_sem=send_sem.at[len(sent)],
            recv_sem=recv_sem.at[len(sent)], device_id=to, device_id_type=MESH)
        copy.start()
        sent.append(copy)
        return copy

    here.greet()
    for k in order:
        for dx, dy in spread:
            i = cell(k, dx, dy)
            pairs[i] = pltpu.make_async_remote_copy(
                src_ref=part_ref.at[here.block(k, dx, dy, 1)], dst_ref=inc.at[i],
                send_sem=pair_send.at[i], recv_sem=pair_recv.at[i],
                device_id=here.device(dc=1), device_id_type=MESH)
            pairs[i].start()
            loads[i] = pltpu.make_async_copy(
                part_ref.at[here.block(k, dx, dy)], acc.at[i], load_sem.at[i])
            loads[i].start()

    wait_for = {}

    def first(k):
        for dx, dy in spread:
            i = cell(k, dx, dy)
            loads[i].wait()
            pairs[i].wait_recv()
            add(i, pl.ds(0, rows), inc[i])
            if dy:
                wait_for["y", k, dx] = send(acc.at[i, low], from_y.at[k * 2 + dx], over_y)
            if dx:
                wait_for["x", k, dy] = send(acc.at[i, high], from_x.at[k * 2 + dy], over_x)

    def second(k):
        wait_for["y", k, 1].wait_recv()
        add(cell(k, 1, 0), low, from_y[k * 2 + 1])
        wait_for["lx", k] = send(acc.at[cell(k, 1, 0), low], last_x.at[k], over_x)
        wait_for["x", k, 1].wait_recv()
        add(cell(k, 0, 1), high, from_x[k * 2 + 1])
        wait_for["ly", k] = send(acc.at[cell(k, 0, 1), high], last_y.at[k], over_y)
        wait_for["y", k, 0].wait_recv()
        add(cell(k, 0, 0), low, from_y[k * 2])
        wait_for["x", k, 0].wait_recv()
        add(cell(k, 0, 0), high, from_x[k * 2])

    def third(k):
        wait_for["lx", k].wait_recv()
        add(cell(k, 0, 0), low, last_x[k])
        wait_for["ly", k].wait_recv()
        add(cell(k, 0, 0), high, last_y[k])
        if k:
            wait_for["z", k] = send(acc.at[cell(k, 0, 0)], from_z.at[k - 1], here.device(k=k))

    for i in range(depth + 2):
        if i < depth:
            first(order[i])
        if 0 <= i - 1 < depth:
            second(order[i - 1])
        if 0 <= i - 2:
            third(order[i - 2])
    total = acc[0].astype(jnp.float32)
    for k in range(1, depth):
        wait_for["z", k].wait_recv()
        total = total + from_z[k - 1].astype(jnp.float32)
    out[...] = total.astype(out.dtype)
    for copy in sent:
        copy.wait_send()
    for copy in pairs.values():
        copy.wait_send()


def scatter_sum(partial, ep_count):
    blocks, rows, width = partial.shape
    depth = ep_count // 2
    lane, half = blocks // 2, rows // 2
    sends = 6 * depth + depth - 1
    dma, kind = pltpu.SemaphoreType.DMA, partial.dtype
    return pl.pallas_call(
        functools.partial(scatter_kernel, depth),
        out_shape=jax.ShapeDtypeStruct((rows, width), kind),
        in_specs=[pl.BlockSpec(memory_space=pl.ANY)],
        out_specs=pl.BlockSpec(memory_space=pltpu.VMEM),
        scratch_shapes=[
            pltpu.VMEM((lane, rows, width), kind), pltpu.VMEM((lane, rows, width), kind),
            pltpu.VMEM((2 * depth, half, width), kind), pltpu.VMEM((2 * depth, half, width), kind),
            pltpu.VMEM((depth, half, width), kind), pltpu.VMEM((depth, half, width), kind),
            pltpu.VMEM((depth - 1, rows, width), kind),
            dma((lane,)), dma((lane,)), dma((lane,)), dma((sends,)), dma((sends,)),
        ],
        compiler_params=pltpu.CompilerParams(
            collective_id=1, has_side_effects=True, vmem_limit_bytes=48 * 1024 * 1024),
    )(partial)


def act_weighted(gate_acc, up_acc, weight):
    return (activate(gate_acc, up_acc) * weight).astype(jnp.bfloat16)


STEP = 240
PUSHES = (((0, 0), 0, "x"), ((0, 0), 1, "y"), ((0, 0), 0, "y"), ((0, 0), 1, "x"),
          ((1, 0), 0, "y"), ((0, 1), 1, "x"))


class Grid:
    def __init__(self):
        e, t = lax.axis_index("ep"), lax.axis_index("tp")
        self.ep, self.tp = e, t
        self.z, self.x, self.y, self.c = e // 2, e % 2, t // 2, t % 2

    def device(self, k=0, dx=0, dy=0, dc=0):
        z = (self.z // 2 + k // 2) % 2 * 2 + (self.z % 2 + k % 2) % 2
        return z * 2 + (self.x + dx) % 2, (self.y + dy) % 2 * 2 + (self.c + dc) % 2


def fused_kernel(tokens, ids, scales, gate, up, down, out, buf, inc, from_y, from_x, last_x, last_y,
                 from_z, wide, deep, stage, rows, hid, take, back, weigh, place, all_ids, all_scales,
                 own_sem, w_sem, meta_send, meta_recv, z_send, z_recv, lane_send, lane_recv,
                 pair_send, pair_recv, sp_send, sp_recv, sx_send, sx_recv, sz_send, sz_recv):
    f32, bf16 = jnp.float32, jnp.bfloat16
    here = Grid()
    depth = from_z.shape[0] + 1
    feat, tok = buf.shape[1], buf.shape[2]
    experts, cap = wide.shape[1], rows.shape[2] // wide.shape[1]
    ff, width = wide.shape[2], wide.shape[3]
    half = from_y.shape[1]
    low, high = pl.ds(0, half), pl.ds(half, feat - half)
    parts = (low, high)
    over = {"x": here.device(dx=1), "y": here.device(dy=1)}
    partner = here.device(dc=1)

    def cell(k, dx, dy, dc):
        return k * 8 + dx * 4 + dy * 2 + dc

    def remote(src, dst, send, recv, to):
        return pltpu.make_async_remote_copy(
            src_ref=src, dst_ref=dst, send_sem=send, recv_sem=recv,
            device_id=to, device_id_type=MESH)

    def z_push(k, p):
        return remote(tokens.at[parts[p]], buf.at[cell(k, 0, 0, 0), parts[p]],
                      z_send.at[k, p], z_recv.at[k, p], here.device(k=k))

    def lane_push(k, n):
        (dx, dy), p, axis = PUSHES[n]
        to = (1 - dx, dy) if axis == "x" else (dx, 1 - dy)
        return remote(buf.at[cell(k, dx, dy, 0), parts[p]], buf.at[cell(k, *to, 0), parts[p]],
                      lane_send.at[k, n], lane_recv.at[k, n], over[axis])

    def pair(k, dx, dy, p):
        n = (dx * 2 + dy) * 2 + p
        return remote(buf.at[cell(k, dx, dy, 0), parts[p]], buf.at[cell(k, dx, dy, 1), parts[p]],
                      pair_send.at[k, n], pair_recv.at[k, n], partner)

    class Both:
        def __init__(self, *copies):
            self.copies = copies

        def start(self):
            for copy in self.copies:
                copy.start()

        def wait_recv(self):
            for copy in self.copies:
                copy.wait_recv()

        def wait_send(self):
            for copy in self.copies:
                copy.wait_send()

    def meta_push(k, dx):
        n, to = k * 2 + dx, here.device(k=k, dx=dx)
        return Both(remote(ids, all_ids.at[n], meta_send.at[0, n], meta_recv.at[0, n], to),
                    remote(scales, all_scales.at[n], meta_send.at[1, n], meta_recv.at[1, n], to))

    def gather_a(k):
        for n in range(4):
            lane_push(k, n).start()
        pair(k, 0, 0, 0).start()
        pair(k, 0, 0, 1).start()

    def column(k):
        z_push(k, 0).wait_recv()
        z_push(k, 1).wait_recv()
        gather_a(k)

    def gather_b(k):
        lane_push(k, 0).wait_recv()
        lane_push(k, 4).start()
        pair(k, 1, 0, 0).start()
        lane_push(k, 1).wait_recv()
        lane_push(k, 5).start()
        pair(k, 0, 1, 1).start()

    def gather_c(k, first):
        if first:
            lane_push(k, 2).wait_recv()
            pair(k, 0, 1, 0).start()
            lane_push(k, 3).wait_recv()
            pair(k, 1, 0, 1).start()
        else:
            lane_push(k, 4).wait_recv()
            pair(k, 1, 1, 0).start()
            lane_push(k, 5).wait_recv()
            pair(k, 1, 1, 1).start()

    def gather_d(k):
        for dx in (0, 1):
            for dy in (0, 1):
                for p in (0, 1):
                    pair(k, dx, dy, p).wait_recv()

    def gather_sent(k):
        for n in range(6):
            lane_push(k, n).wait_send()
        for dx in (0, 1):
            for dy in (0, 1):
                for p in (0, 1):
                    pair(k, dx, dy, p).wait_send()

    def give(k, dx, dy):
        n = dx * 2 + dy
        return remote(buf.at[cell(k, dx, dy, 1)], inc.at[k * 4 + n],
                      sp_send.at[k, n], sp_recv.at[k, n], partner)

    def hop(k, n):
        src, dst, axis = (
            (buf.at[cell(k, 1, 1, 0), low], from_y.at[k * 2 + 1], "y"),
            (buf.at[cell(k, 0, 1, 0), low], from_y.at[k * 2], "y"),
            (buf.at[cell(k, 1, 1, 0), high], from_x.at[k * 2 + 1], "x"),
            (buf.at[cell(k, 1, 0, 0), high], from_x.at[k * 2], "x"),
            (buf.at[cell(k, 1, 0, 0), low], last_x.at[k], "x"),
            (buf.at[cell(k, 0, 1, 0), high], last_y.at[k], "y"))[n]
        return remote(src, dst, sx_send.at[k, n], sx_recv.at[k, n], over[axis])

    def home(k):
        return remote(buf.at[cell(k, 0, 0, 0)], from_z.at[k - 1],
                      sz_send.at[k], sz_recv.at[k], here.device(k=k))

    def add(at, part, got):
        buf[at, part] = (buf[at, part].astype(f32) + got.astype(f32)).astype(bf16)

    def scatter_b(k):
        for dx, dy in ((1, 1), (0, 1), (1, 0), (0, 0)):
            give(k, dx, dy).wait_recv()
            add(cell(k, dx, dy, 0), pl.ds(0, feat), inc[k * 4 + dx * 2 + dy])
            if dy:
                hop(k, 1 - dx).start()
            if dx:
                hop(k, 3 - dy).start()

    def scatter_c(k):
        hop(k, 0).wait_recv()
        add(cell(k, 1, 0, 0), low, from_y[k * 2 + 1])
        hop(k, 4).start()
        hop(k, 2).wait_recv()
        add(cell(k, 0, 1, 0), high, from_x[k * 2 + 1])
        hop(k, 5).start()
        hop(k, 1).wait_recv()
        add(cell(k, 0, 0, 0), low, from_y[k * 2])
        hop(k, 3).wait_recv()
        add(cell(k, 0, 0, 0), high, from_x[k * 2])

    def scatter_d(k):
        hop(k, 4).wait_recv()
        add(cell(k, 0, 0, 0), low, last_x[k])
        hop(k, 5).wait_recv()
        add(cell(k, 0, 0, 0), high, last_y[k])

    own = [pltpu.make_async_copy(tokens, buf.at[cell(0, 0, 0, 0)], own_sem.at[0]),
           pltpu.make_async_copy(ids, all_ids.at[0], own_sem.at[1]),
           pltpu.make_async_copy(scales, all_scales.at[0], own_sem.at[2])]
    for copy in own:
        copy.start()
    barrier = pltpu.get_barrier_semaphore()
    near = [here.device(k=k, dx=dx) for k in range(depth) for dx in (0, 1) if k or dx]
    near += [over["y"], partner]
    for who in near:
        pl.semaphore_signal(barrier, inc=1, device_id=who, device_id_type=MESH)
    pl.semaphore_wait(barrier, len(near))
    for k in range(depth):
        for dx in (0, 1):
            if k or dx:
                meta_push(k, dx).start()
    for k in range(1, depth):
        z_push(k, 0).start()
        z_push(k, 1).start()
    for copy in own:
        copy.wait()
    gather_a(0)
    loads = [pltpu.make_async_copy(ref.at[e], wide.at[side, e], w_sem.at[side, e])
             for side, ref in enumerate((gate, up)) for e in range(experts)]
    deeps = [pltpu.make_async_copy(down.at[e], stage, w_sem.at[2, e]) for e in range(experts)]
    deeps[0].start()
    for load in loads:
        load.start()
    place[...] = jnp.zeros(place.shape, f32)

    def turn(e):
        deeps[e].wait()
        for n in range(0, width, 256):
            size = min(256, width - n)
            eye = (lax.broadcasted_iota(jnp.int32, (size, size), 0)
                   == lax.broadcasted_iota(jnp.int32, (size, size), 1)).astype(f32).astype(bf16)
            got = lax.dot_general(eye, stage[:, pl.ds(n, size)], (((1,), (1,)), ((), ())),
                                  preferred_element_type=f32)
            deep[e, pl.ds(n, size), :] = got.astype(bf16)
        if e + 1 < experts:
            deeps[e + 1].start()

    turn(0)
    gather_b(0)
    column(1)
    for e in range(1, experts):
        turn(e)
    gather_c(0, True)
    gather_c(0, False)
    for load in loads:
        load.wait()

    ahead = (lax.broadcasted_iota(jnp.int32, (tok, tok), 0)
             < lax.broadcasted_iota(jnp.int32, (tok, tok), 1)).astype(f32).astype(bf16)
    slot_row = lax.broadcasted_iota(jnp.int32, (cap, tok), 0).astype(f32)
    slot_col = lax.broadcasted_iota(jnp.int32, (tok, cap), 1).astype(f32)
    row_at = lax.broadcasted_iota(jnp.int32, (8, tok), 0)

    def masks(k):
        picked = jnp.zeros((8, tok), f32)
        known = jnp.zeros((8, tok), f32)
        for dx in (0, 1):
            named, scaled = all_ids[k * 2 + dx], all_scales[k * 2 + dx]
            for e in range(experts):
                n = dx * experts + e
                hit = (named == here.ep * experts + e).astype(f32)
                chosen = jnp.sum(hit, axis=0, keepdims=True)
                picked = jnp.where(row_at == n, chosen, picked)
                held = jnp.sum(hit * scaled, axis=0, keepdims=True)
                known = jnp.where(row_at == 2 * experts + n, held, known)
        slot = jnp.dot(picked.astype(bf16), ahead, preferred_element_type=f32)
        slot = jnp.where(picked > 0.5, slot, -1.0)
        place[0:8, :] = jnp.where(row_at < 2 * experts, slot, known)
        turned = jnp.transpose(place[...])
        for dx in (0, 1):
            for e in range(experts):
                n = dx * experts + e
                at = pl.ds(e * cap, cap)
                take[dx, at, :] = (slot_row == slot[n:n + 1, :]).astype(f32).astype(bf16)
                hot = (slot_col == turned[:, n:n + 1]).astype(f32)
                back[dx, :, at] = hot.astype(bf16)
                held = turned[:, 2 * experts + n:2 * experts + n + 1]
                weigh[e, :, pl.ds(dx * cap, cap)] = jnp.broadcast_to(
                    jnp.sum(hot * held, axis=0, keepdims=True), (8, cap))

    def block(k, dx, j):
        return cell(k, dx, (here.y + j // 2) % 2, (here.c + j % 2) % 2)

    def dispatch(k):
        for dx in (0, 1):
            for j in range(4):
                got = jnp.dot(buf[block(k, dx, j)], back[dx], preferred_element_type=f32)
                rows[dx, pl.ds(j * feat, feat), :] = got.astype(bf16)

    def enter(e):
        at = pl.ds(e * cap, cap)
        held = jnp.concatenate([rows[0, :, at], rows[1, :, at]], axis=1)
        for n in range(0, ff, STEP):
            part = pl.ds(n, min(STEP, ff - n))
            g = jnp.dot(wide[0, e, part, :], held, preferred_element_type=f32)
            u = jnp.dot(wide[1, e, part, :], held, preferred_element_type=f32)
            hid[part, :] = act_weighted(g, u, weigh[e, 0:1, :])

    def leave(e):
        at = pl.ds(e * cap, cap)
        for n in range(0, width, 2 * STEP):
            part = pl.ds(n, min(2 * STEP, width - n))
            got = jnp.dot(deep[e, part, :], hid[...], preferred_element_type=f32).astype(bf16)
            rows[0, part, at] = got[:, 0:cap]
            rows[1, part, at] = got[:, cap:2 * cap]

    def combine(k, dx):
        for j in range(4):
            got = jnp.dot(rows[dx, pl.ds(j * feat, feat), :], take[dx], preferred_element_type=f32)
            buf[block(k, dx, j)] = got.astype(bf16)

    def plane(k, carry):
        last = depth - 1
        gather_d(k)

        @pl.when(k > 0)
        def _():
            meta_push(k, 0).wait_recv()
        meta_push(k, 1).wait_recv()
        masks(k)
        dispatch(k)

        @pl.when(k < last)
        def _():
            gather_b(k + 1)
        enter(0)

        @pl.when(k < last - 1)
        def _():
            column(k + 2)

        @pl.when(k > 1)
        def _():
            scatter_b(k - 1)
        leave(0)
        enter(1)

        @pl.when(k < last)
        def _():
            gather_c(k + 1, True)
        leave(1)
        gather_sent(k)

        @pl.when(k < last)
        def _():
            gather_c(k + 1, False)
        for dx in (1, 0):
            combine(k, dx)
            give(k, dx, 1).start()
            give(k, dx, 0).start()
        return carry

    lax.fori_loop(0, depth, plane, 0)

    scatter_c(1)
    scatter_b(3)
    scatter_c(2)
    scatter_d(1)
    home(1).start()
    scatter_b(0)
    scatter_c(3)
    scatter_d(2)
    home(2).start()
    scatter_c(0)
    scatter_d(3)
    home(3).start()
    scatter_d(0)
    total = buf[cell(0, 0, 0, 0)].astype(f32)
    for k in range(1, depth):
        home(k).wait_recv()
        total = total + from_z[k - 1].astype(f32)
    out[...] = total.astype(out.dtype)
    for k in range(depth):
        for dx in (0, 1):
            if k or dx:
                meta_push(k, dx).wait_send()
            for dy in (0, 1):
                give(k, dx, dy).wait_send()
        for n in range(6):
            hop(k, n).wait_send()
        if k:
            z_push(k, 0).wait_send()
            z_push(k, 1).wait_send()
            home(k).wait_send()


def fused(tokens, expert_ids, combine_weights, gate_weight, up_weight, down_weight, depth, capacity):
    tok, feat = tokens.shape
    experts, width, ff = gate_weight.shape
    top = expert_ids.shape[1]
    f32, bf16 = jnp.float32, jnp.bfloat16
    half = -(-feat // 32) * 16
    rest = feat - half
    dma = pltpu.SemaphoreType.DMA
    scratch = [
        pltpu.VMEM((depth * 8, feat, tok), bf16), pltpu.VMEM((depth * 4, feat, tok), bf16),
        pltpu.VMEM((depth * 2, half, tok), bf16), pltpu.VMEM((depth * 2, rest, tok), bf16),
        pltpu.VMEM((depth, half, tok), bf16), pltpu.VMEM((depth, rest, tok), bf16),
        pltpu.VMEM((depth - 1, feat, tok), bf16),
        pltpu.VMEM((2, experts, ff, width), bf16), pltpu.VMEM((experts, width, ff), bf16),
        pltpu.VMEM((ff, width), bf16),
        pltpu.VMEM((2, width, experts * capacity), bf16),
        pltpu.VMEM((ff, 2 * capacity), bf16),
        pltpu.VMEM((2, experts * capacity, tok), bf16), pltpu.VMEM((2, tok, experts * capacity), bf16),
        pltpu.VMEM((experts, 8, 2 * capacity), f32), pltpu.VMEM((128, tok), f32),
        pltpu.VMEM((depth * 2, top, tok), jnp.int32), pltpu.VMEM((depth * 2, top, tok), f32),
        dma((3,)), dma((3, experts)), dma((2, depth * 2)), dma((2, depth * 2)),
        dma((depth, 2)), dma((depth, 2)), dma((depth, 6)), dma((depth, 6)),
        dma((depth, 8)), dma((depth, 8)), dma((depth, 4)), dma((depth, 4)),
        dma((depth, 6)), dma((depth, 6)), dma((depth,)), dma((depth,)),
    ]
    mixed = pl.pallas_call(
        fused_kernel,
        out_shape=jax.ShapeDtypeStruct((feat, tok), bf16),
        in_specs=[pl.BlockSpec(memory_space=pl.ANY)] * 6,
        out_specs=pl.BlockSpec(memory_space=pltpu.VMEM),
        scratch_shapes=scratch,
        compiler_params=pltpu.CompilerParams(
            collective_id=0, has_side_effects=True, vmem_limit_bytes=63 * 1024 * 1024),
    )(tokens.T, expert_ids.T, combine_weights.T, gate_weight.transpose(0, 2, 1),
      up_weight.transpose(0, 2, 1), down_weight)
    return mixed.T


def local(tokens, expert_ids, combine_weights, gate_weight, up_weight, down_weight):
    ep_count = lax.axis_size("ep")
    tp_count = lax.axis_size("tp")
    exp_local = gate_weight.shape[0]
    experts = exp_local * ep_count
    tok_rows = expert_ids.shape[0]
    top_count = expert_ids.shape[1]
    capacity = 2 * tok_rows * top_count // experts
    feat_width = tokens.shape[1]
    ff_width = gate_weight.shape[2]
    width = feat_width * tp_count
    f32, bf16 = jnp.float32, jnp.bfloat16
    if (ep_count, tp_count, exp_local, top_count) == (8, 4, 2, 4) and capacity % 128 == 0:
        return fused(tokens, expert_ids, combine_weights, gate_weight, up_weight, down_weight,
                     ep_count // 2, capacity)

    ids_all = lax.all_gather(expert_ids.T, "ep")
    weights_all = lax.all_gather(combine_weights.T, "ep")
    first = lax.axis_index("ep") * exp_local
    mine = first + jnp.arange(exp_local, dtype=jnp.int32)
    hit = ids_all[:, None, :, :] == mine[None, :, None, None]
    chosen = jnp.any(hit, axis=2)
    weight = jnp.sum(jnp.where(hit, weights_all[:, None, :, :], 0.0), axis=2)

    ahead = jnp.triu(jnp.ones((tok_rows, tok_rows), bf16), 1)
    slot = lax.dot_general(
        chosen.reshape(-1, tok_rows).astype(bf16), ahead, (((1,), (0,)), ((), ())),
        preferred_element_type=f32,
    ).astype(jnp.int32).reshape(chosen.shape)
    place = jnp.where(chosen, slot, -1)
    take = place[:, :, None, :] == jnp.arange(capacity, dtype=jnp.int32)[None, None, :, None]
    slot_weight = jnp.sum(jnp.where(take, weight[:, :, None, :], 0.0), axis=3)
    take = take.astype(bf16)

    paired = tp_count == 2 * 2 and ep_count % 2 == 0
    spread = gather_all(tokens, ep_count, tp_count) if paired else lax.all_gather(
        tokens, ("ep", "tp")
    )
    gathered = spread.reshape(
        ep_count, tp_count, tok_rows, feat_width
    )
    routed = jnp.einsum(
        "sect,sjtf->escjf", take, gathered, preferred_element_type=f32
    ).astype(bf16)
    rows = routed.reshape(exp_local, ep_count * capacity, width)
    gate_new = jnp.einsum("erd,edf->erf", rows, gate_weight, preferred_element_type=f32)
    up_new = jnp.einsum("erd,edf->erf", rows, up_weight, preferred_element_type=f32)
    row_weight = slot_weight.transpose(1, 0, 2).reshape(exp_local, ep_count * capacity, 1)
    hidden = (activate(gate_new, up_new) * row_weight).astype(bf16)
    expert_out = jnp.einsum(
        "erf,efd->erd", hidden, down_weight, preferred_element_type=f32
    ).astype(bf16)
    expert_out = expert_out.reshape(exp_local, ep_count, capacity, tp_count, feat_width)
    partial = jnp.einsum(
        "sect,escjf->sjtf", take, expert_out, preferred_element_type=f32
    ).astype(bf16)
    partial = partial.reshape(ep_count * tp_count, tok_rows, feat_width)
    if paired:
        return scatter_sum(partial, ep_count)
    mixed = lax.psum_scatter(partial, ("ep", "tp"), scatter_dimension=0, tiled=True)
    return mixed.reshape(tok_rows, feat_width)


def solution(mesh):
    in_specs = (
        P("ep", "tp"),
        P("ep", None),
        P("ep", None),
        P("ep", None, "tp"),
        P("ep", None, "tp"),
        P("ep", "tp", None),
    )
    out_specs = P("ep", "tp")
    return jax.shard_map(local, mesh=mesh, in_specs=in_specs, out_specs=out_specs, check_vma=False)
```

```python
import functools

import jax
import jax.numpy as jnp
from jax import lax
from jax.experimental import pallas as pl
from jax.experimental.pallas import tpu as pltpu
from jax.sharding import PartitionSpec as P


def activate(gate_acc, up_acc):
    return (up_acc + 1.0) * gate_acc * jax.nn.sigmoid(1.702 * gate_acc)


MESH = pl.DeviceIdType.MESH


class Place:
    def __init__(self, depth):
        self.depth = depth
        e, t = lax.axis_index("ep"), lax.axis_index("tp")
        self.z, self.x, self.y, self.c = e // 2, e % 2, t // 2, t % 2

    def device(self, k=0, dx=0, dy=0, dc=0):
        ep = (self.z + k) % self.depth * 2 + (self.x + dx) % 2
        tp = (self.y + dy) % 2 * 2 + (self.c + dc) % 2
        return ep, tp

    def block(self, k=0, dx=0, dy=0, dc=0):
        ep, tp = self.device(k, dx, dy, dc)
        return ep * 4 + tp

    def greet(self):
        barrier = pltpu.get_barrier_semaphore()
        near = [self.device(k=k) for k in range(1, self.depth)]
        near += [self.device(dx=1), self.device(dy=1), self.device(dc=1)]
        for who in near:
            pl.semaphore_signal(barrier, inc=1, device_id=who, device_id_type=MESH)
        pl.semaphore_wait(barrier, len(near))


def gather_kernel(depth, own, out, lane_recv, pair_recv, lane_send, pair_send, own_sem):
    here = Place(depth)
    half = own.shape[0] // 2
    sent = []

    def piece(k, dx, dy, part):
        rows = pl.ds(part * half, half)
        if (k, dx, dy) == (0, 0, 0):
            return own.at[rows]
        return out.at[here.block(k, dx, dy), rows]

    def lane_slot(k, dx, dy):
        ep, tp = here.device(k, dx, dy)
        return ep * 2 + tp // 2

    def push(k, dx, dy, part, to):
        rows = pl.ds(part * half, half)
        copy = pltpu.make_async_remote_copy(
            src_ref=piece(k, dx, dy, part), dst_ref=out.at[here.block(k, dx, dy), rows],
            send_sem=lane_send.at[len(sent)], recv_sem=lane_recv.at[lane_slot(k, dx, dy), part],
            device_id=to, device_id_type=MESH)
        copy.start()
        sent.append(copy)

    def pair(k, dx, dy, part):
        rows = pl.ds(part * half, half)
        slot = lane_slot(k, dx, dy)
        copy = pltpu.make_async_remote_copy(
            src_ref=piece(k, dx, dy, part), dst_ref=out.at[here.block(k, dx, dy), rows],
            send_sem=pair_send.at[slot, part], recv_sem=pair_recv.at[slot, part],
            device_id=here.device(dc=1), device_id_type=MESH)
        copy.start()

    def landed(k, dx, dy, part, to):
        rows = pl.ds(part * half, half)
        ref = out.at[here.block(k, dx, dy), rows]
        pltpu.make_async_remote_copy(
            src_ref=ref, dst_ref=ref, send_sem=lane_send.at[0],
            recv_sem=lane_recv.at[lane_slot(k, dx, dy), part],
            device_id=to, device_id_type=MESH).wait_recv()

    here.greet()
    over_x, over_y = here.device(dx=1), here.device(dy=1)
    for k in range(1, depth):
        for part in (0, 1):
            push(0, 0, 0, part, here.device(k=depth - k))
    store = pltpu.make_async_copy(own, out.at[here.block()], own_sem)
    store.start()
    for k in range(depth):
        if k:
            landed(k, 0, 0, 0, here.device(k=k))
            landed(k, 0, 0, 1, here.device(k=k))
        push(k, 0, 0, 0, over_x)
        push(k, 0, 0, 1, over_y)
        push(k, 0, 0, 0, over_y)
        push(k, 0, 0, 1, over_x)
        pair(k, 0, 0, 0)
        pair(k, 0, 0, 1)
        landed(k, 1, 0, 0, over_x)
        push(k, 1, 0, 0, over_y)
        pair(k, 1, 0, 0)
        landed(k, 0, 1, 1, over_y)
        push(k, 0, 1, 1, over_x)
        pair(k, 0, 1, 1)
    for k in range(depth):
        landed(k, 0, 1, 0, over_y)
        pair(k, 0, 1, 0)
        landed(k, 1, 0, 1, over_x)
        pair(k, 1, 0, 1)
        landed(k, 1, 1, 0, over_y)
        pair(k, 1, 1, 0)
        landed(k, 1, 1, 1, over_x)
        pair(k, 1, 1, 1)
    store.wait()
    for copy in sent:
        copy.wait_send()
    for k in range(depth):
        for dx in (0, 1):
            for dy in (0, 1):
                slot = lane_slot(k, dx, dy)
                for part in (0, 1):
                    rows = pl.ds(part * half, half)
                    copy = pltpu.make_async_remote_copy(
                        src_ref=piece(k, dx, dy, part),
                        dst_ref=out.at[here.block(k, dx, dy, 1), rows],
                        send_sem=pair_send.at[slot, part], recv_sem=pair_recv.at[slot, part],
                        device_id=here.device(dc=1), device_id_type=MESH)
                    copy.wait_send()
                    copy.wait_recv()


def gather_all(tokens, ep_count, tp_count):
    rows, width = tokens.shape
    depth = ep_count // 2
    blocks = ep_count * tp_count
    sends = 2 * (depth - 1) + 6 * depth
    dma = pltpu.SemaphoreType.DMA
    return pl.pallas_call(
        functools.partial(gather_kernel, depth),
        out_shape=jax.ShapeDtypeStruct((blocks, rows, width), tokens.dtype),
        in_specs=[pl.BlockSpec(memory_space=pltpu.VMEM)],
        out_specs=pl.BlockSpec(memory_space=pl.ANY),
        scratch_shapes=[dma((blocks // 2, 2)), dma((blocks // 2, 2)), dma((sends,)),
                        dma((blocks // 2, 2)), dma(())],
        compiler_params=pltpu.CompilerParams(collective_id=0, has_side_effects=True),
    )(tokens)


def scatter_kernel(depth, part_ref, out, acc, inc, from_y, from_x, last_x, last_y, from_z,
                   load_sem, pair_send, pair_recv, send_sem, recv_sem):
    here = Place(depth)
    rows = out.shape[0]
    half = rows // 2
    low, high = pl.ds(0, half), pl.ds(half, half)
    order = list(range(1, depth)) + [0]
    spread = ((1, 1), (0, 1), (1, 0), (0, 0))
    over_x, over_y = here.device(dx=1), here.device(dy=1)
    sent = []
    loads, pairs = {}, {}
    cell = lambda k, dx, dy: (k * 2 + dx) * 2 + dy

    def add(at, part, got):
        acc[at, part] = (acc[at, part].astype(jnp.float32) + got.astype(jnp.float32)).astype(acc.dtype)

    def send(src, dst, to):
        copy = pltpu.make_async_remote_copy(
            src_ref=src, dst_ref=dst, send_sem=send_sem.at[len(sent)],
            recv_sem=recv_sem.at[len(sent)], device_id=to, device_id_type=MESH)
        copy.start()
        sent.append(copy)
        return copy

    here.greet()
    for k in order:
        for dx, dy in spread:
            i = cell(k, dx, dy)
            pairs[i] = pltpu.make_async_remote_copy(
                src_ref=part_ref.at[here.block(k, dx, dy, 1)], dst_ref=inc.at[i],
                send_sem=pair_send.at[i], recv_sem=pair_recv.at[i],
                device_id=here.device(dc=1), device_id_type=MESH)
            pairs[i].start()
            loads[i] = pltpu.make_async_copy(
                part_ref.at[here.block(k, dx, dy)], acc.at[i], load_sem.at[i])
            loads[i].start()

    wait_for = {}

    def first(k):
        for dx, dy in spread:
            i = cell(k, dx, dy)
            loads[i].wait()
            pairs[i].wait_recv()
            add(i, pl.ds(0, rows), inc[i])
            if dy:
                wait_for["y", k, dx] = send(acc.at[i, low], from_y.at[k * 2 + dx], over_y)
            if dx:
                wait_for["x", k, dy] = send(acc.at[i, high], from_x.at[k * 2 + dy], over_x)

    def second(k):
        wait_for["y", k, 1].wait_recv()
        add(cell(k, 1, 0), low, from_y[k * 2 + 1])
        wait_for["lx", k] = send(acc.at[cell(k, 1, 0), low], last_x.at[k], over_x)
        wait_for["x", k, 1].wait_recv()
        add(cell(k, 0, 1), high, from_x[k * 2 + 1])
        wait_for["ly", k] = send(acc.at[cell(k, 0, 1), high], last_y.at[k], over_y)
        wait_for["y", k, 0].wait_recv()
        add(cell(k, 0, 0), low, from_y[k * 2])
        wait_for["x", k, 0].wait_recv()
        add(cell(k, 0, 0), high, from_x[k * 2])

    def third(k):
        wait_for["lx", k].wait_recv()
        add(cell(k, 0, 0), low, last_x[k])
        wait_for["ly", k].wait_recv()
        add(cell(k, 0, 0), high, last_y[k])
        if k:
            wait_for["z", k] = send(acc.at[cell(k, 0, 0)], from_z.at[k - 1], here.device(k=k))

    for i in range(depth + 2):
        if i < depth:
            first(order[i])
        if 0 <= i - 1 < depth:
            second(order[i - 1])
        if 0 <= i - 2:
            third(order[i - 2])
    total = acc[0].astype(jnp.float32)
    for k in range(1, depth):
        wait_for["z", k].wait_recv()
        total = total + from_z[k - 1].astype(jnp.float32)
    out[...] = total.astype(out.dtype)
    for copy in sent:
        copy.wait_send()
    for copy in pairs.values():
        copy.wait_send()


def scatter_sum(partial, ep_count):
    blocks, rows, width = partial.shape
    depth = ep_count // 2
    lane, half = blocks // 2, rows // 2
    sends = 6 * depth + depth - 1
    dma, kind = pltpu.SemaphoreType.DMA, partial.dtype
    return pl.pallas_call(
        functools.partial(scatter_kernel, depth),
        out_shape=jax.ShapeDtypeStruct((rows, width), kind),
        in_specs=[pl.BlockSpec(memory_space=pl.ANY)],
        out_specs=pl.BlockSpec(memory_space=pltpu.VMEM),
        scratch_shapes=[
            pltpu.VMEM((lane, rows, width), kind), pltpu.VMEM((lane, rows, width), kind),
            pltpu.VMEM((2 * depth, half, width), kind), pltpu.VMEM((2 * depth, half, width), kind),
            pltpu.VMEM((depth, half, width), kind), pltpu.VMEM((depth, half, width), kind),
            pltpu.VMEM((depth - 1, rows, width), kind),
            dma((lane,)), dma((lane,)), dma((lane,)), dma((sends,)), dma((sends,)),
        ],
        compiler_params=pltpu.CompilerParams(
            collective_id=1, has_side_effects=True, vmem_limit_bytes=48 * 1024 * 1024),
    )(partial)


def act_weighted(gate_acc, up_acc, weight):
    return (activate(gate_acc, up_acc) * weight).astype(jnp.bfloat16)


STEP = 240
def when(condition, run):
    if isinstance(condition, bool):
        if condition:
            run()
    else:
        pl.when(condition)(run)


PUSHES = (((0, 0), 0, "x"), ((0, 0), 1, "y"), ((0, 0), 0, "y"), ((0, 0), 1, "x"),
          ((1, 0), 0, "y"), ((0, 1), 1, "x"))


class Grid:
    def __init__(self):
        e, t = lax.axis_index("ep"), lax.axis_index("tp")
        self.ep, self.tp = e, t
        self.z, self.x, self.y, self.c = e // 2, e % 2, t // 2, t % 2
        self.mid = (self.z + 1) // 2 % 2

    def away(self, m, dx=0, dy=0, dc=0):
        z = (self.z // 2 + m // 2) % 2 * 2 + (self.z % 2 + m % 2) % 2
        return z * 2 + (self.x + dx) % 2, (self.y + dy) % 2 * 2 + (self.c + dc) % 2

    def device(self, k=0, dx=0, dy=0, dc=0):
        return self.away((k + self.mid * (4 - 2 * k)) % 4, dx, dy, dc)

    def seen(self, k):
        return 3 - 2 * self.mid if k % 2 else k


def fused_kernel(tokens, ids, scales, gate, up, down, out, buf, inc, from_y, from_x, last_x, last_y,
                 from_z, aside, wide, deep, stage, rows, hid, take, back, weigh, place, all_ids, all_scales,
                 own_sem, w_sem, meta_send, meta_recv, z_send, z_recv, lane_send, lane_recv,
                 pair_send, pair_recv, sp_send, sp_recv, sx_send, sx_recv, sz_send, sz_recv,
                 cross_send, cross_recv, ferry_send, ferry_recv):
    f32, bf16 = jnp.float32, jnp.bfloat16
    here = Grid()
    depth = from_z.shape[0] + 1
    feat, tok = buf.shape[1], buf.shape[2]
    experts, cap = wide.shape[1], rows.shape[2] // wide.shape[1]
    ff, width = wide.shape[2], wide.shape[3]
    half = from_y.shape[1]
    low, high = pl.ds(0, half), pl.ds(half, feat - half)
    parts = (low, high)
    over = {"x": here.device(dx=1), "y": here.device(dy=1)}
    partner = here.device(dc=1)

    def cell(k, dx, dy, dc):
        return k * 8 + dx * 4 + dy * 2 + dc

    def remote(src, dst, send, recv, to):
        return pltpu.make_async_remote_copy(
            src_ref=src, dst_ref=dst, send_sem=send, recv_sem=recv,
            device_id=to, device_id_type=MESH)

    near, other = here.away(1), here.away(3)
    mid, end = here.mid == 1, here.mid == 0

    def flow(n, p):
        source, label = ((None, here.seen(1)), (None, 1), (1, 2), (3, 2), (2, 3))[n]
        src = tokens if source is None else buf.at[cell(source, 0, 0, 0)]
        return remote(src.at[parts[p]], buf.at[cell(label, 0, 0, 0), parts[p]],
                      z_send.at[n, p], z_recv.at[label, p], other if n in (1, 3) else near)

    def flow_start(n):
        flow(n, 0).start()
        flow(n, 1).start()

    def flow_sent(n):
        flow(n, 0).wait_send()
        flow(n, 1).wait_send()

    def arrive(k):
        for p in (0, 1):
            at = buf.at[cell(k, 0, 0, 0), parts[p]]
            remote(at, at, z_send.at[0, p], z_recv.at[k, p], near).wait_recv()

    def lane_push(k, n):
        (dx, dy), p, axis = PUSHES[n]
        to = (1 - dx, dy) if axis == "x" else (dx, 1 - dy)
        return remote(buf.at[cell(k, dx, dy, 0), parts[p]], buf.at[cell(k, *to, 0), parts[p]],
                      lane_send.at[k, n], lane_recv.at[k, n], over[axis])

    def pair(k, dx, dy, p):
        n = (dx * 2 + dy) * 2 + p
        return remote(buf.at[cell(k, dx, dy, 0), parts[p]], buf.at[cell(k, dx, dy, 1), parts[p]],
                      pair_send.at[k, n], pair_recv.at[k, n], partner)

    class Both:
        def __init__(self, *copies):
            self.copies = copies

        def start(self):
            for copy in self.copies:
                copy.start()

        def wait_recv(self):
            for copy in self.copies:
                copy.wait_recv()

        def wait_send(self):
            for copy in self.copies:
                copy.wait_send()

    def meta_push(k, dx, to_me=False):
        to = here.device(k=k, dx=dx)
        n = k * 2 + dx if to_me else here.seen(k) * 2 + dx
        return Both(remote(ids, all_ids.at[n], meta_send.at[0, n], meta_recv.at[0, n], to),
                    remote(scales, all_scales.at[n], meta_send.at[1, n], meta_recv.at[1, n], to))

    def gather_a(k):
        for n in range(4):
            lane_push(k, n).start()
        pair(k, 0, 0, 0).start()
        pair(k, 0, 0, 1).start()

    def column(k):
        if k == 3:
            when(end, lambda: arrive(3))
        else:
            arrive(k)
            when(mid, lambda: flow_start(2 if k == 1 else 4))
        gather_a(k)

    def turn_early():
        arrive(3)
        flow_start(3)

    def cross(n, p):
        source, label = ((0, 3), (2, 3), (1, 2))[n]
        return remote(buf.at[cell(source, 1, 1, 0), parts[p]],
                      buf.at[cell(label, 1, 1, 0), parts[p]],
                      cross_send.at[n, p], cross_recv.at[label - 2, p], near)

    def crossed(k, p):
        at = buf.at[cell(k, 1, 1, 0), parts[p]]
        remote(at, at, cross_send.at[0, p], cross_recv.at[k - 2, p], near).wait_recv()

    def inside(k):
        if isinstance(k, int):
            return (True, True, mid, False)[k]
        return k < 2 + here.mid

    def outside(k):
        if isinstance(k, int):
            return (False, False, end, True)[k]
        return k >= 2 + here.mid

    def gather_b(k):
        lane_push(k, 0).wait_recv()
        when(inside(k), lambda: lane_push(k, 4).start())
        pair(k, 1, 0, 0).start()
        lane_push(k, 1).wait_recv()
        when(inside(k), lambda: lane_push(k, 5).start())
        pair(k, 0, 1, 1).start()

    def gather_c(k, first):
        if first:
            lane_push(k, 2).wait_recv()
            pair(k, 0, 1, 0).start()
            lane_push(k, 3).wait_recv()
            pair(k, 1, 0, 1).start()
        else:
            for p in (0, 1):
                def relayed():
                    lane_push(k, 4 + p).wait_recv()
                    if isinstance(k, int):
                        if k == 0:
                            when(end, lambda: cross(0, p).start())
                        if k == 1:
                            when(mid, lambda: cross(2, p).start())
                    else:
                        when((k == 2) & mid, lambda: cross(1, p).start())
                when(inside(k), relayed)
                when(outside(k), lambda: crossed(k, p))
                pair(k, 1, 1, p).start()

    def gather_d(k):
        for dx in (0, 1):
            for dy in (0, 1):
                for p in (0, 1):
                    pair(k, dx, dy, p).wait_recv()

    def gather_sent(k):
        for n in range(4):
            lane_push(k, n).wait_send()

        def relayed():
            for p in (0, 1):
                lane_push(k, 4 + p).wait_send()
        when(inside(k), relayed)
        for at, n, side in ((0, 0, end), (2, 1, mid), (1, 2, mid)):
            @pl.when((k == at) & side)
            def _():
                cross(n, 0).wait_send()
                cross(n, 1).wait_send()

        @pl.when(mid)
        def _():
            for at, n in ((1, 2), (3, 3), (2, 4)):
                @pl.when(k == at)
                def _():
                    flow_sent(n)

        for dx in (0, 1):
            for dy in (0, 1):
                for p in (0, 1):
                    pair(k, dx, dy, p).wait_send()

    def give(k, dx, dy):
        n = dx * 2 + dy
        return remote(buf.at[cell(k, dx, dy, 1)], inc.at[k * 4 + n],
                      sp_send.at[k, n], sp_recv.at[k, n], partner)

    def hop(k, n):
        src, dst, axis = (
            (buf.at[cell(k, 1, 1, 0), low], from_y.at[k * 2 + 1], "y"),
            (buf.at[cell(k, 0, 1, 0), low], from_y.at[k * 2], "y"),
            (buf.at[cell(k, 1, 1, 0), high], from_x.at[k * 2 + 1], "x"),
            (buf.at[cell(k, 1, 0, 0), high], from_x.at[k * 2], "x"),
            (buf.at[cell(k, 1, 0, 0), low], last_x.at[k], "x"),
            (buf.at[cell(k, 0, 1, 0), high], last_y.at[k], "y"))[n]
        return remote(src, dst, sx_send.at[k, n], sx_recv.at[k, n], over[axis])

    def home(k, to_me=False):
        at = k if to_me else here.seen(k)
        return remote(buf.at[cell(k, 0, 0, 0)], from_z.at[at - 1],
                      sz_send.at[k], sz_recv.at[at], here.device(k=k))

    def add(at, part, got):
        buf[at, part] = (buf[at, part].astype(f32) + got.astype(f32)).astype(bf16)

    def ferry(k):
        slot = 1 - here.mid if k == 1 else k - 2
        return remote(buf.at[cell(k, 1, 1, 0)], aside.at[slot], ferry_send.at[k - 1],
                      ferry_recv.at[slot], here.away(1 + 2 * here.mid) if k == 1 else near)

    def ferried(k, slot):
        remote(aside.at[slot], aside.at[slot], ferry_send.at[0], ferry_recv.at[slot],
               near).wait_recv()
        add(cell(k, 1, 1, 0), pl.ds(0, feat), aside[slot])

    def merge(k, dx, dy):
        give(k, dx, dy).wait_recv()
        add(cell(k, dx, dy, 0), pl.ds(0, feat), inc[k * 4 + dx * 2 + dy])

    def scatter_near(k):
        merge(k, 1, 1)
        ferry(k).start()
        merge(k, 0, 1)
        hop(k, 1).start()
        hop(k, 5).start()
        merge(k, 1, 0)
        hop(k, 3).start()
        hop(k, 4).start()
        merge(k, 0, 0)

    def scatter_sides(k):
        merge(k, 0, 1)
        hop(k, 1).start()
        merge(k, 1, 0)
        hop(k, 3).start()
        merge(k, 0, 0)

    def scatter_corner(k):
        merge(k, 1, 1)
        if k == 0:
            when(mid, lambda: ferried(0, 0))
            when(mid, lambda: ferried(0, 1))
        if k == 3:
            when(end, lambda: ferried(3, 0))
        hop(k, 0).start()
        hop(k, 2).start()

    def scatter_far(k):
        scatter_corner(k)
        scatter_sides(k)

    def scatter_turn(k):
        hop(k, 0).wait_recv()
        add(cell(k, 1, 0, 0), low, from_y[k * 2 + 1])
        hop(k, 4).start()
        hop(k, 2).wait_recv()
        add(cell(k, 0, 1, 0), high, from_x[k * 2 + 1])
        hop(k, 5).start()

    def scatter_end(k):
        hop(k, 1).wait_recv()
        add(cell(k, 0, 0, 0), low, from_y[k * 2])
        hop(k, 3).wait_recv()
        add(cell(k, 0, 0, 0), high, from_x[k * 2])
        hop(k, 4).wait_recv()
        add(cell(k, 0, 0, 0), low, last_x[k])
        hop(k, 5).wait_recv()
        add(cell(k, 0, 0, 0), high, last_y[k])
        if k:
            home(k).start()

    own = [pltpu.make_async_copy(tokens, buf.at[cell(0, 0, 0, 0)], own_sem.at[0]),
           pltpu.make_async_copy(ids, all_ids.at[0], own_sem.at[1]),
           pltpu.make_async_copy(scales, all_scales.at[0], own_sem.at[2])]
    for copy in own:
        copy.start()
    barrier = pltpu.get_barrier_semaphore()
    greeted = [here.device(k=k, dx=dx) for k in range(depth) for dx in (0, 1) if k or dx]
    greeted += [over["y"], partner]
    for who in greeted:
        pl.semaphore_signal(barrier, inc=1, device_id=who, device_id_type=MESH)
    pl.semaphore_wait(barrier, len(greeted))
    for k in range(depth):
        for dx in (0, 1):
            if k or dx:
                meta_push(k, dx).start()
    flow_start(0)
    when(mid, lambda: flow_start(1))
    for copy in own:
        copy.wait()
    gather_a(0)
    loads = [pltpu.make_async_copy(ref.at[e], wide.at[side, e], w_sem.at[side, e])
             for side, ref in enumerate((gate, up)) for e in range(experts)]
    deeps = [pltpu.make_async_copy(down.at[e], stage, w_sem.at[2, e]) for e in range(experts)]
    deeps[0].start()
    for load in loads:
        load.start()
    place[...] = jnp.zeros(place.shape, f32)

    def turn(e):
        deeps[e].wait()
        for n in range(0, width, 256):
            size = min(256, width - n)
            eye = (lax.broadcasted_iota(jnp.int32, (size, size), 0)
                   == lax.broadcasted_iota(jnp.int32, (size, size), 1)).astype(f32).astype(bf16)
            got = lax.dot_general(eye, stage[:, pl.ds(n, size)], (((1,), (1,)), ((), ())),
                                  preferred_element_type=f32)
            deep[e, pl.ds(n, size), :] = got.astype(bf16)
        if e + 1 < experts:
            deeps[e + 1].start()

    turn(0)
    gather_b(0)
    when(mid, turn_early)
    column(1)
    ahead = (lax.broadcasted_iota(jnp.int32, (tok, tok), 0)
             < lax.broadcasted_iota(jnp.int32, (tok, tok), 1)).astype(f32).astype(bf16)
    slot_row = lax.broadcasted_iota(jnp.int32, (cap, tok), 0).astype(f32)
    slot_col = lax.broadcasted_iota(jnp.int32, (tok, cap), 1).astype(f32)
    row_at = lax.broadcasted_iota(jnp.int32, (8, tok), 0)

    def masks(k):
        picked = jnp.zeros((8, tok), f32)
        known = jnp.zeros((8, tok), f32)
        for dx in (0, 1):
            named, scaled = all_ids[k * 2 + dx], all_scales[k * 2 + dx]
            for e in range(experts):
                n = dx * experts + e
                hit = (named == here.ep * experts + e).astype(f32)
                chosen = jnp.sum(hit, axis=0, keepdims=True)
                picked = jnp.where(row_at == n, chosen, picked)
                held = jnp.sum(hit * scaled, axis=0, keepdims=True)
                known = jnp.where(row_at == 2 * experts + n, held, known)
        slot = jnp.dot(picked.astype(bf16), ahead, preferred_element_type=f32)
        slot = jnp.where(picked > 0.5, slot, -1.0)
        place[0:8, :] = jnp.where(row_at < 2 * experts, slot, known)
        turned = jnp.transpose(place[...])
        for dx in (0, 1):
            for e in range(experts):
                n = dx * experts + e
                at = pl.ds(e * cap, cap)
                take[k, dx, at, :] = (slot_row == slot[n:n + 1, :]).astype(f32).astype(bf16)
                hot = (slot_col == turned[:, n:n + 1]).astype(f32)
                back[k, dx, :, at] = hot.astype(bf16)
                held = turned[:, 2 * experts + n:2 * experts + n + 1]
                weigh[k, e, :, pl.ds(dx * cap, cap)] = jnp.broadcast_to(
                    jnp.sum(hot * held, axis=0, keepdims=True), (8, cap))

    def prepare(k, carry):
        @pl.when(k > 0)
        def _():
            meta_push(k, 0, True).wait_recv()
        meta_push(k, 1, True).wait_recv()
        masks(k)
        return carry

    for e in range(1, experts):
        turn(e)
    lax.fori_loop(0, depth, prepare, 0)
    gather_c(0, True)
    gather_c(0, False)
    for load in loads:
        load.wait()

    def block(k, dx, j):
        return cell(k, dx, (here.y + j // 2) % 2, (here.c + j % 2) % 2)

    def dispatch(k):
        for dx in (0, 1):
            for j in range(4):
                got = jnp.dot(buf[block(k, dx, j)], back[k, dx], preferred_element_type=f32)
                rows[dx, pl.ds(j * feat, feat), :] = got.astype(bf16)

    def enter(k, e):
        at = pl.ds(e * cap, cap)
        held = jnp.concatenate([rows[0, :, at], rows[1, :, at]], axis=1)
        for n in range(0, ff, STEP):
            part = pl.ds(n, min(STEP, ff - n))
            g = jnp.dot(wide[0, e, part, :], held, preferred_element_type=f32)
            u = jnp.dot(wide[1, e, part, :], held, preferred_element_type=f32)
            hid[part, :] = act_weighted(g, u, weigh[k, e, 0:1, :])

    def leave(e):
        at = pl.ds(e * cap, cap)
        for n in range(0, width, 2 * STEP):
            part = pl.ds(n, min(2 * STEP, width - n))
            got = jnp.dot(deep[e, part, :], hid[...], preferred_element_type=f32).astype(bf16)
            rows[0, part, at] = got[:, 0:cap]
            rows[1, part, at] = got[:, cap:2 * cap]

    def combine(k, dx):
        for j in range(4):
            got = jnp.dot(rows[dx, pl.ds(j * feat, feat), :], take[k, dx], preferred_element_type=f32)
            buf[block(k, dx, j)] = got.astype(bf16)

    def at(condition):
        return pl.when(condition)

    def plane(step, carry):
        last = depth - 1
        k = (step + here.mid) % depth
        ahead_of = (k < last) & (end | (k > 0))
        gather_d(k)
        dispatch(k)

        @at((k == 0) & mid)
        def _():
            scatter_far(3)
            scatter_end(2)

        @at((k == 2) & end)
        def _():
            scatter_near(1)
            scatter_sides(0)

        @at((k == last) & end)
        def _():
            scatter_far(2)
        enter(k, 0)

        @at((k == 0) & end)
        def _():
            gather_b(1)

        @at(k == 1)
        def _():
            gather_b(2)
            column(3)

        @at((k == 2) & mid)
        def _():
            scatter_near(1)

        @at((k == last) & mid)
        def _():
            scatter_near(2)
        leave(0)

        @at((k == 0) & end)
        def _():
            column(2)

        @at((k == 0) & mid)
        def _():
            scatter_turn(3)
        enter(k, 1)

        @at(k == 2)
        def _():
            gather_b(3)

        @at(ahead_of)
        def _():
            gather_c(k + 1, True)

        @at(k == last)
        def _():
            scatter_end(1)
        leave(1)

        @at((k == last) & end)
        def _():
            scatter_turn(2)
        gather_sent(k)

        @at(ahead_of)
        def _():
            gather_c(k + 1, False)
        for dx in (1, 0):
            combine(k, dx)
            give(k, dx, 1).start()
            give(k, dx, 0).start()
        return carry

    @pl.when(mid)
    def _():
        gather_b(1)
        column(2)
        gather_c(1, True)
        gather_c(1, False)
    lax.fori_loop(0, depth, plane, 0)

    @pl.when(end)
    def _():
        scatter_far(3)
        scatter_end(2)
        scatter_turn(3)
        scatter_corner(0)

    @pl.when(mid)
    def _():
        scatter_far(0)
    scatter_end(3)
    scatter_turn(0)
    scatter_end(0)
    total = buf[cell(0, 0, 0, 0)].astype(f32)
    for k in range(1, depth):
        home(k, True).wait_recv()
        total = total + from_z[k - 1].astype(f32)
    out[...] = total.astype(out.dtype)
    for k in range(depth):
        for dx in (0, 1):
            if k or dx:
                meta_push(k, dx).wait_send()
            for dy in (0, 1):
                give(k, dx, dy).wait_send()
        for n in (1, 3, 4, 5):
            hop(k, n).wait_send()

        def cornered():
            hop(k, 0).wait_send()
            hop(k, 2).wait_send()
        if k == 2:
            when(end, cornered)
        elif k != 1:
            cornered()
        if k:
            home(k).wait_send()
    ferry(1).wait_send()
    flow_sent(0)

    @pl.when(mid)
    def _():
        ferry(2).wait_send()
        flow_sent(1)


def fused(tokens, expert_ids, combine_weights, gate_weight, up_weight, down_weight, depth, capacity):
    tok, feat = tokens.shape
    experts, width, ff = gate_weight.shape
    top = expert_ids.shape[1]
    f32, bf16 = jnp.float32, jnp.bfloat16
    half = -(-feat // 32) * 16
    rest = feat - half
    dma = pltpu.SemaphoreType.DMA
    scratch = [
        pltpu.VMEM((depth * 8, feat, tok), bf16), pltpu.VMEM((depth * 4, feat, tok), bf16),
        pltpu.VMEM((depth * 2, half, tok), bf16), pltpu.VMEM((depth * 2, rest, tok), bf16),
        pltpu.VMEM((depth, half, tok), bf16), pltpu.VMEM((depth, rest, tok), bf16),
        pltpu.VMEM((depth - 1, feat, tok), bf16), pltpu.VMEM((2, feat, tok), bf16),
        pltpu.VMEM((2, experts, ff, width), bf16), pltpu.VMEM((experts, width, ff), bf16),
        pltpu.VMEM((ff, width), bf16),
        pltpu.VMEM((2, width, experts * capacity), bf16),
        pltpu.VMEM((ff, 2 * capacity), bf16),
        pltpu.VMEM((depth, 2, experts * capacity, tok), bf16),
        pltpu.VMEM((depth, 2, tok, experts * capacity), bf16),
        pltpu.VMEM((depth, experts, 8, 2 * capacity), f32), pltpu.VMEM((128, tok), f32),
        pltpu.VMEM((depth * 2, top, tok), jnp.int32), pltpu.VMEM((depth * 2, top, tok), f32),
        dma((3,)), dma((3, experts)), dma((2, depth * 2)), dma((2, depth * 2)),
        dma((5, 2)), dma((depth, 2)), dma((depth, 6)), dma((depth, 6)),
        dma((depth, 8)), dma((depth, 8)), dma((depth, 4)), dma((depth, 4)),
        dma((depth, 6)), dma((depth, 6)), dma((depth,)), dma((depth,)),
        dma((3, 2)), dma((2, 2)), dma((2,)), dma((2,)),
    ]
    mixed = pl.pallas_call(
        fused_kernel,
        out_shape=jax.ShapeDtypeStruct((feat, tok), bf16),
        in_specs=[pl.BlockSpec(memory_space=pl.ANY)] * 6,
        out_specs=pl.BlockSpec(memory_space=pltpu.VMEM),
        scratch_shapes=scratch,
        compiler_params=pltpu.CompilerParams(
            collective_id=0, has_side_effects=True, vmem_limit_bytes=63 * 1024 * 1024),
    )(tokens.T, expert_ids.T, combine_weights.T, gate_weight.transpose(0, 2, 1),
      up_weight.transpose(0, 2, 1), down_weight)
    return mixed.T


def local(tokens, expert_ids, combine_weights, gate_weight, up_weight, down_weight):
    ep_count = lax.axis_size("ep")
    tp_count = lax.axis_size("tp")
    exp_local = gate_weight.shape[0]
    experts = exp_local * ep_count
    tok_rows = expert_ids.shape[0]
    top_count = expert_ids.shape[1]
    capacity = 2 * tok_rows * top_count // experts
    feat_width = tokens.shape[1]
    ff_width = gate_weight.shape[2]
    width = feat_width * tp_count
    f32, bf16 = jnp.float32, jnp.bfloat16
    if (ep_count, tp_count, exp_local, top_count) == (8, 4, 2, 4) and capacity % 128 == 0:
        return fused(tokens, expert_ids, combine_weights, gate_weight, up_weight, down_weight,
                     ep_count // 2, capacity)

    ids_all = lax.all_gather(expert_ids.T, "ep")
    weights_all = lax.all_gather(combine_weights.T, "ep")
    first = lax.axis_index("ep") * exp_local
    mine = first + jnp.arange(exp_local, dtype=jnp.int32)
    hit = ids_all[:, None, :, :] == mine[None, :, None, None]
    chosen = jnp.any(hit, axis=2)
    weight = jnp.sum(jnp.where(hit, weights_all[:, None, :, :], 0.0), axis=2)

    ahead = jnp.triu(jnp.ones((tok_rows, tok_rows), bf16), 1)
    slot = lax.dot_general(
        chosen.reshape(-1, tok_rows).astype(bf16), ahead, (((1,), (0,)), ((), ())),
        preferred_element_type=f32,
    ).astype(jnp.int32).reshape(chosen.shape)
    place = jnp.where(chosen, slot, -1)
    take = place[:, :, None, :] == jnp.arange(capacity, dtype=jnp.int32)[None, None, :, None]
    slot_weight = jnp.sum(jnp.where(take, weight[:, :, None, :], 0.0), axis=3)
    take = take.astype(bf16)

    paired = tp_count == 2 * 2 and ep_count % 2 == 0
    spread = gather_all(tokens, ep_count, tp_count) if paired else lax.all_gather(
        tokens, ("ep", "tp")
    )
    gathered = spread.reshape(
        ep_count, tp_count, tok_rows, feat_width
    )
    routed = jnp.einsum(
        "sect,sjtf->escjf", take, gathered, preferred_element_type=f32
    ).astype(bf16)
    rows = routed.reshape(exp_local, ep_count * capacity, width)
    gate_new = jnp.einsum("erd,edf->erf", rows, gate_weight, preferred_element_type=f32)
    up_new = jnp.einsum("erd,edf->erf", rows, up_weight, preferred_element_type=f32)
    row_weight = slot_weight.transpose(1, 0, 2).reshape(exp_local, ep_count * capacity, 1)
    hidden = (activate(gate_new, up_new) * row_weight).astype(bf16)
    expert_out = jnp.einsum(
        "erf,efd->erd", hidden, down_weight, preferred_element_type=f32
    ).astype(bf16)
    expert_out = expert_out.reshape(exp_local, ep_count, capacity, tp_count, feat_width)
    partial = jnp.einsum(
        "sect,escjf->sjtf", take, expert_out, preferred_element_type=f32
    ).astype(bf16)
    partial = partial.reshape(ep_count * tp_count, tok_rows, feat_width)
    if paired:
        return scatter_sum(partial, ep_count)
    mixed = lax.psum_scatter(partial, ("ep", "tp"), scatter_dimension=0, tiled=True)
    return mixed.reshape(tok_rows, feat_width)


def solution(mesh):
    in_specs = (
        P("ep", "tp"),
        P("ep", None),
        P("ep", None),
        P("ep", None, "tp"),
        P("ep", None, "tp"),
        P("ep", "tp", None),
    )
    out_specs = P("ep", "tp")
    return jax.shard_map(local, mesh=mesh, in_specs=in_specs, out_specs=out_specs, check_vma=False)
```

```python
import functools

import jax
import jax.numpy as jnp
from jax import lax
from jax.experimental import pallas as pl
from jax.experimental.pallas import tpu as pltpu
from jax.sharding import PartitionSpec as P


def activate(gate_acc, up_acc):
    return (up_acc + 1.0) * gate_acc * jax.nn.sigmoid(1.702 * gate_acc)


MESH = pl.DeviceIdType.MESH


class Place:
    def __init__(self, depth):
        self.depth = depth
        e, t = lax.axis_index("ep"), lax.axis_index("tp")
        self.z, self.x, self.y, self.c = e // 2, e % 2, t // 2, t % 2

    def device(self, k=0, dx=0, dy=0, dc=0):
        ep = (self.z + k) % self.depth * 2 + (self.x + dx) % 2
        tp = (self.y + dy) % 2 * 2 + (self.c + dc) % 2
        return ep, tp

    def block(self, k=0, dx=0, dy=0, dc=0):
        ep, tp = self.device(k, dx, dy, dc)
        return ep * 4 + tp

    def greet(self):
        barrier = pltpu.get_barrier_semaphore()
        near = [self.device(k=k) for k in range(1, self.depth)]
        near += [self.device(dx=1), self.device(dy=1), self.device(dc=1)]
        for who in near:
            pl.semaphore_signal(barrier, inc=1, device_id=who, device_id_type=MESH)
        pl.semaphore_wait(barrier, len(near))


def gather_kernel(depth, own, out, lane_recv, pair_recv, lane_send, pair_send, own_sem):
    here = Place(depth)
    half = own.shape[0] // 2
    sent = []

    def piece(k, dx, dy, part):
        rows = pl.ds(part * half, half)
        if (k, dx, dy) == (0, 0, 0):
            return own.at[rows]
        return out.at[here.block(k, dx, dy), rows]

    def lane_slot(k, dx, dy):
        ep, tp = here.device(k, dx, dy)
        return ep * 2 + tp // 2

    def push(k, dx, dy, part, to):
        rows = pl.ds(part * half, half)
        copy = pltpu.make_async_remote_copy(
            src_ref=piece(k, dx, dy, part), dst_ref=out.at[here.block(k, dx, dy), rows],
            send_sem=lane_send.at[len(sent)], recv_sem=lane_recv.at[lane_slot(k, dx, dy), part],
            device_id=to, device_id_type=MESH)
        copy.start()
        sent.append(copy)

    def pair(k, dx, dy, part):
        rows = pl.ds(part * half, half)
        slot = lane_slot(k, dx, dy)
        copy = pltpu.make_async_remote_copy(
            src_ref=piece(k, dx, dy, part), dst_ref=out.at[here.block(k, dx, dy), rows],
            send_sem=pair_send.at[slot, part], recv_sem=pair_recv.at[slot, part],
            device_id=here.device(dc=1), device_id_type=MESH)
        copy.start()

    def landed(k, dx, dy, part, to):
        rows = pl.ds(part * half, half)
        ref = out.at[here.block(k, dx, dy), rows]
        pltpu.make_async_remote_copy(
            src_ref=ref, dst_ref=ref, send_sem=lane_send.at[0],
            recv_sem=lane_recv.at[lane_slot(k, dx, dy), part],
            device_id=to, device_id_type=MESH).wait_recv()

    here.greet()
    over_x, over_y = here.device(dx=1), here.device(dy=1)
    for k in range(1, depth):
        for part in (0, 1):
            push(0, 0, 0, part, here.device(k=depth - k))
    store = pltpu.make_async_copy(own, out.at[here.block()], own_sem)
    store.start()
    for k in range(depth):
        if k:
            landed(k, 0, 0, 0, here.device(k=k))
            landed(k, 0, 0, 1, here.device(k=k))
        push(k, 0, 0, 0, over_x)
        push(k, 0, 0, 1, over_y)
        push(k, 0, 0, 0, over_y)
        push(k, 0, 0, 1, over_x)
        pair(k, 0, 0, 0)
        pair(k, 0, 0, 1)
        landed(k, 1, 0, 0, over_x)
        push(k, 1, 0, 0, over_y)
        pair(k, 1, 0, 0)
        landed(k, 0, 1, 1, over_y)
        push(k, 0, 1, 1, over_x)
        pair(k, 0, 1, 1)
    for k in range(depth):
        landed(k, 0, 1, 0, over_y)
        pair(k, 0, 1, 0)
        landed(k, 1, 0, 1, over_x)
        pair(k, 1, 0, 1)
        landed(k, 1, 1, 0, over_y)
        pair(k, 1, 1, 0)
        landed(k, 1, 1, 1, over_x)
        pair(k, 1, 1, 1)
    store.wait()
    for copy in sent:
        copy.wait_send()
    for k in range(depth):
        for dx in (0, 1):
            for dy in (0, 1):
                slot = lane_slot(k, dx, dy)
                for part in (0, 1):
                    rows = pl.ds(part * half, half)
                    copy = pltpu.make_async_remote_copy(
                        src_ref=piece(k, dx, dy, part),
                        dst_ref=out.at[here.block(k, dx, dy, 1), rows],
                        send_sem=pair_send.at[slot, part], recv_sem=pair_recv.at[slot, part],
                        device_id=here.device(dc=1), device_id_type=MESH)
                    copy.wait_send()
                    copy.wait_recv()


def gather_all(tokens, ep_count, tp_count):
    rows, width = tokens.shape
    depth = ep_count // 2
    blocks = ep_count * tp_count
    sends = 2 * (depth - 1) + 6 * depth
    dma = pltpu.SemaphoreType.DMA
    return pl.pallas_call(
        functools.partial(gather_kernel, depth),
        out_shape=jax.ShapeDtypeStruct((blocks, rows, width), tokens.dtype),
        in_specs=[pl.BlockSpec(memory_space=pltpu.VMEM)],
        out_specs=pl.BlockSpec(memory_space=pl.ANY),
        scratch_shapes=[dma((blocks // 2, 2)), dma((blocks // 2, 2)), dma((sends,)),
                        dma((blocks // 2, 2)), dma(())],
        compiler_params=pltpu.CompilerParams(collective_id=0, has_side_effects=True),
    )(tokens)


def scatter_kernel(depth, part_ref, out, acc, inc, from_y, from_x, last_x, last_y, from_z,
                   load_sem, pair_send, pair_recv, send_sem, recv_sem):
    here = Place(depth)
    rows = out.shape[0]
    half = rows // 2
    low, high = pl.ds(0, half), pl.ds(half, half)
    order = list(range(1, depth)) + [0]
    spread = ((1, 1), (0, 1), (1, 0), (0, 0))
    over_x, over_y = here.device(dx=1), here.device(dy=1)
    sent = []
    loads, pairs = {}, {}
    cell = lambda k, dx, dy: (k * 2 + dx) * 2 + dy

    def add(at, part, got):
        acc[at, part] = (acc[at, part].astype(jnp.float32) + got.astype(jnp.float32)).astype(acc.dtype)

    def send(src, dst, to):
        copy = pltpu.make_async_remote_copy(
            src_ref=src, dst_ref=dst, send_sem=send_sem.at[len(sent)],
            recv_sem=recv_sem.at[len(sent)], device_id=to, device_id_type=MESH)
        copy.start()
        sent.append(copy)
        return copy

    here.greet()
    for k in order:
        for dx, dy in spread:
            i = cell(k, dx, dy)
            pairs[i] = pltpu.make_async_remote_copy(
                src_ref=part_ref.at[here.block(k, dx, dy, 1)], dst_ref=inc.at[i],
                send_sem=pair_send.at[i], recv_sem=pair_recv.at[i],
                device_id=here.device(dc=1), device_id_type=MESH)
            pairs[i].start()
            loads[i] = pltpu.make_async_copy(
                part_ref.at[here.block(k, dx, dy)], acc.at[i], load_sem.at[i])
            loads[i].start()

    wait_for = {}

    def first(k):
        for dx, dy in spread:
            i = cell(k, dx, dy)
            loads[i].wait()
            pairs[i].wait_recv()
            add(i, pl.ds(0, rows), inc[i])
            if dy:
                wait_for["y", k, dx] = send(acc.at[i, low], from_y.at[k * 2 + dx], over_y)
            if dx:
                wait_for["x", k, dy] = send(acc.at[i, high], from_x.at[k * 2 + dy], over_x)

    def second(k):
        wait_for["y", k, 1].wait_recv()
        add(cell(k, 1, 0), low, from_y[k * 2 + 1])
        wait_for["lx", k] = send(acc.at[cell(k, 1, 0), low], last_x.at[k], over_x)
        wait_for["x", k, 1].wait_recv()
        add(cell(k, 0, 1), high, from_x[k * 2 + 1])
        wait_for["ly", k] = send(acc.at[cell(k, 0, 1), high], last_y.at[k], over_y)
        wait_for["y", k, 0].wait_recv()
        add(cell(k, 0, 0), low, from_y[k * 2])
        wait_for["x", k, 0].wait_recv()
        add(cell(k, 0, 0), high, from_x[k * 2])

    def third(k):
        wait_for["lx", k].wait_recv()
        add(cell(k, 0, 0), low, last_x[k])
        wait_for["ly", k].wait_recv()
        add(cell(k, 0, 0), high, last_y[k])
        if k:
            wait_for["z", k] = send(acc.at[cell(k, 0, 0)], from_z.at[k - 1], here.device(k=k))

    for i in range(depth + 2):
        if i < depth:
            first(order[i])
        if 0 <= i - 1 < depth:
            second(order[i - 1])
        if 0 <= i - 2:
            third(order[i - 2])
    total = acc[0].astype(jnp.float32)
    for k in range(1, depth):
        wait_for["z", k].wait_recv()
        total = total + from_z[k - 1].astype(jnp.float32)
    out[...] = total.astype(out.dtype)
    for copy in sent:
        copy.wait_send()
    for copy in pairs.values():
        copy.wait_send()


def scatter_sum(partial, ep_count):
    blocks, rows, width = partial.shape
    depth = ep_count // 2
    lane, half = blocks // 2, rows // 2
    sends = 6 * depth + depth - 1
    dma, kind = pltpu.SemaphoreType.DMA, partial.dtype
    return pl.pallas_call(
        functools.partial(scatter_kernel, depth),
        out_shape=jax.ShapeDtypeStruct((rows, width), kind),
        in_specs=[pl.BlockSpec(memory_space=pl.ANY)],
        out_specs=pl.BlockSpec(memory_space=pltpu.VMEM),
        scratch_shapes=[
            pltpu.VMEM((lane, rows, width), kind), pltpu.VMEM((lane, rows, width), kind),
            pltpu.VMEM((2 * depth, half, width), kind), pltpu.VMEM((2 * depth, half, width), kind),
            pltpu.VMEM((depth, half, width), kind), pltpu.VMEM((depth, half, width), kind),
            pltpu.VMEM((depth - 1, rows, width), kind),
            dma((lane,)), dma((lane,)), dma((lane,)), dma((sends,)), dma((sends,)),
        ],
        compiler_params=pltpu.CompilerParams(
            collective_id=1, has_side_effects=True, vmem_limit_bytes=48 * 1024 * 1024),
    )(partial)


def act_weighted(gate_acc, up_acc, weight):
    return (activate(gate_acc, up_acc) * weight).astype(jnp.bfloat16)


STEP = 240
def when(condition, run):
    if isinstance(condition, bool):
        if condition:
            run()
    else:
        pl.when(condition)(run)


PUSHES = (((0, 0), 0, "x"), ((0, 0), 1, "y"), ((0, 0), 0, "y"), ((0, 0), 1, "x"),
          ((1, 0), 0, "y"), ((0, 1), 1, "x"))


class Grid:
    def __init__(self):
        e, t = lax.axis_index("ep"), lax.axis_index("tp")
        self.ep, self.tp = e, t
        self.z, self.x, self.y, self.c = e // 2, e % 2, t // 2, t % 2
        self.mid = (self.z + 1) // 2 % 2

    def away(self, m, dx=0, dy=0, dc=0):
        z = (self.z // 2 + m // 2) % 2 * 2 + (self.z % 2 + m % 2) % 2
        return z * 2 + (self.x + dx) % 2, (self.y + dy) % 2 * 2 + (self.c + dc) % 2

    def device(self, k=0, dx=0, dy=0, dc=0):
        return self.away((k + self.mid * (4 - 2 * k)) % 4, dx, dy, dc)

    def seen(self, k):
        return 3 - 2 * self.mid if k % 2 else k


def fused_kernel(tokens, ids, scales, gate, up, down, out, buf, inc, from_y, from_x, last_x, last_y,
                 from_z, aside, passing, wide, deep, stage, rows, hid, take, back, weigh, place, all_ids, all_scales,
                 own_sem, w_sem, meta_send, meta_recv, z_send, z_recv, lane_send, lane_recv,
                 pair_send, pair_recv, sp_send, sp_recv, sx_send, sx_recv, sz_send, sz_recv,
                 cross_send, cross_recv, ferry_send, ferry_recv, detour_sem):
    f32, bf16 = jnp.float32, jnp.bfloat16
    here = Grid()
    depth = from_z.shape[0] + 1
    feat, tok = buf.shape[1], buf.shape[2]
    experts, cap = wide.shape[1], rows.shape[2] // wide.shape[1]
    ff, width = wide.shape[2], wide.shape[3]
    half = from_y.shape[1]
    low, high = pl.ds(0, half), pl.ds(half, feat - half)
    parts = (low, high)
    over = {"x": here.device(dx=1), "y": here.device(dy=1)}
    partner = here.device(dc=1)

    def cell(k, dx, dy, dc):
        return k * 8 + dx * 4 + dy * 2 + dc

    def remote(src, dst, send, recv, to):
        return pltpu.make_async_remote_copy(
            src_ref=src, dst_ref=dst, send_sem=send, recv_sem=recv,
            device_id=to, device_id_type=MESH)

    near, other = here.away(1), here.away(3)
    mid, end = here.mid == 1, here.mid == 0

    def flow(n, p):
        source, label = ((None, here.seen(1)), (None, 1), (1, 2), (3, 2), (2, 3))[n]
        src = tokens if source is None else buf.at[cell(source, 0, 0, 0)]
        return remote(src.at[parts[p]], buf.at[cell(label, 0, 0, 0), parts[p]],
                      z_send.at[n, p], z_recv.at[label, p], other if n in (1, 3) else near)

    def flow_start(n):
        flow(n, 0).start()
        flow(n, 1).start()

    def flow_sent(n):
        flow(n, 0).wait_send()
        flow(n, 1).wait_send()

    def arrive(k):
        for p in (0, 1):
            at = buf.at[cell(k, 0, 0, 0), parts[p]]
            remote(at, at, z_send.at[0, p], z_recv.at[k, p], near).wait_recv()

    def lane_push(k, n):
        (dx, dy), p, axis = PUSHES[n]
        to = (1 - dx, dy) if axis == "x" else (dx, 1 - dy)
        return remote(buf.at[cell(k, dx, dy, 0), parts[p]], buf.at[cell(k, *to, 0), parts[p]],
                      lane_send.at[k, n], lane_recv.at[k, n], over[axis])

    def pair(k, dx, dy, p):
        n = (dx * 2 + dy) * 2 + p
        return remote(buf.at[cell(k, dx, dy, 0), parts[p]], buf.at[cell(k, dx, dy, 1), parts[p]],
                      pair_send.at[k, n], pair_recv.at[k, n], partner)

    class Both:
        def __init__(self, *copies):
            self.copies = copies

        def start(self):
            for copy in self.copies:
                copy.start()

        def wait_recv(self):
            for copy in self.copies:
                copy.wait_recv()

        def wait_send(self):
            for copy in self.copies:
                copy.wait_send()

    def meta_push(k, dx, to_me=False):
        to = here.device(k=k, dx=dx)
        n = k * 2 + dx if to_me else here.seen(k) * 2 + dx
        return Both(remote(ids, all_ids.at[n], meta_send.at[0, n], meta_recv.at[0, n], to),
                    remote(scales, all_scales.at[n], meta_send.at[1, n], meta_recv.at[1, n], to))

    def gather_a(k):
        for n in range(4):
            lane_push(k, n).start()
        pair(k, 0, 0, 0).start()
        pair(k, 0, 0, 1).start()

    def column(k):
        if k == 3:
            when(end, lambda: arrive(3))
        else:
            arrive(k)
            when(mid, lambda: flow_start(2 if k == 1 else 4))
        gather_a(k)

    def turn_early():
        arrive(3)
        flow_start(3)

    def cross(n, p):
        source, label = ((0, 3), (2, 3), (1, 2))[n]
        return remote(buf.at[cell(source, 1, 1, 0), parts[p]],
                      buf.at[cell(label, 1, 1, 0), parts[p]],
                      cross_send.at[n, p], cross_recv.at[label - 2, p], near)

    def crossed(k, p):
        at = buf.at[cell(k, 1, 1, 0), parts[p]]
        remote(at, at, cross_send.at[0, p], cross_recv.at[k - 2, p], near).wait_recv()

    def inside(k):
        if isinstance(k, int):
            return (True, True, mid, False)[k]
        return k < 2 + here.mid

    def outside(k):
        if isinstance(k, int):
            return (False, False, end, True)[k]
        return k >= 2 + here.mid

    def gather_b(k):
        lane_push(k, 0).wait_recv()
        when(inside(k), lambda: lane_push(k, 4).start())
        pair(k, 1, 0, 0).start()
        lane_push(k, 1).wait_recv()
        when(inside(k), lambda: lane_push(k, 5).start())
        pair(k, 0, 1, 1).start()

    def gather_c(k, first):
        if first:
            lane_push(k, 2).wait_recv()
            pair(k, 0, 1, 0).start()
            lane_push(k, 3).wait_recv()
            pair(k, 1, 0, 1).start()
        else:
            for p in (0, 1):
                def relayed():
                    lane_push(k, 4 + p).wait_recv()
                    if isinstance(k, int):
                        if k == 0:
                            when(end, lambda: cross(0, p).start())
                        if k == 1:
                            when(mid, lambda: cross(2, p).start())
                    else:
                        when((k == 2) & mid, lambda: cross(1, p).start())
                when(inside(k), relayed)
                when(outside(k), lambda: crossed(k, p))
                pair(k, 1, 1, p).start()

    def gather_d(k):
        for dx in (0, 1):
            for dy in (0, 1):
                for p in (0, 1):
                    pair(k, dx, dy, p).wait_recv()

    def gather_sent(k):
        for n in range(4):
            lane_push(k, n).wait_send()

        def relayed():
            for p in (0, 1):
                lane_push(k, 4 + p).wait_send()
        when(inside(k), relayed)
        for at, n, side in ((0, 0, end), (2, 1, mid), (1, 2, mid)):
            @pl.when((k == at) & side)
            def _():
                cross(n, 0).wait_send()
                cross(n, 1).wait_send()

        @pl.when(mid)
        def _():
            for at, n in ((1, 2), (3, 3), (2, 4)):
                @pl.when(k == at)
                def _():
                    flow_sent(n)

        for dx in (0, 1):
            for dy in (0, 1):
                for p in (0, 1):
                    pair(k, dx, dy, p).wait_send()

    def give(k, dx, dy):
        n = dx * 2 + dy
        return remote(buf.at[cell(k, dx, dy, 1)], inc.at[k * 4 + n],
                      sp_send.at[k, n], sp_recv.at[k, n], partner)

    def hop(k, n):
        src, dst, axis = (
            (buf.at[cell(k, 1, 1, 0), low], from_y.at[k * 2 + 1], "y"),
            (buf.at[cell(k, 0, 1, 0), low], from_y.at[k * 2], "y"),
            (buf.at[cell(k, 1, 1, 0), high], from_x.at[k * 2 + 1], "x"),
            (buf.at[cell(k, 1, 0, 0), high], from_x.at[k * 2], "x"),
            (buf.at[cell(k, 1, 0, 0), low], last_x.at[k], "x"),
            (buf.at[cell(k, 0, 1, 0), high], last_y.at[k], "y"))[n]
        return remote(src, dst, sx_send.at[k, n], sx_recv.at[k, n], over[axis])

    def home(k, p, to_me=False):
        at = k if to_me else here.seen(k)
        return remote(buf.at[cell(k, 0, 0, 0), parts[p]], from_z.at[at - 1, parts[p]],
                      sz_send.at[k, p], sz_recv.at[at, p], here.device(k=k))

    def detour():
        return remote(buf.at[cell(3, 0, 0, 0), high], passing,
                      detour_sem.at[0], detour_sem.at[1], here.device(k=2))

    def onward():
        detour().wait_recv()
        add(cell(3, 0, 0, 0), high, passing[...])
        home(3, 1).start()

    def add(at, part, got):
        buf[at, part] = (buf[at, part].astype(f32) + got.astype(f32)).astype(bf16)

    def ferry(k):
        slot = 1 - here.mid if k == 1 else k - 2
        return remote(buf.at[cell(k, 1, 1, 0)], aside.at[slot], ferry_send.at[k - 1],
                      ferry_recv.at[slot], here.away(1 + 2 * here.mid) if k == 1 else near)

    def ferried(k, slot):
        remote(aside.at[slot], aside.at[slot], ferry_send.at[0], ferry_recv.at[slot],
               near).wait_recv()
        add(cell(k, 1, 1, 0), pl.ds(0, feat), aside[slot])

    def merge(k, dx, dy):
        give(k, dx, dy).wait_recv()
        add(cell(k, dx, dy, 0), pl.ds(0, feat), inc[k * 4 + dx * 2 + dy])

    def scatter_ferry(k):
        merge(k, 1, 1)
        ferry(k).start()

    def scatter_near(k):
        if k == 1:
            scatter_ferry(k)
        merge(k, 0, 1)
        hop(k, 1).start()
        hop(k, 5).start()
        merge(k, 1, 0)
        hop(k, 3).start()
        hop(k, 4).start()
        merge(k, 0, 0)

    def scatter_sides(k):
        merge(k, 0, 1)
        hop(k, 1).start()
        merge(k, 1, 0)
        hop(k, 3).start()
        merge(k, 0, 0)

    def scatter_corner(k):
        merge(k, 1, 1)
        if k == 0:
            when(mid, lambda: ferried(0, 0))
            when(mid, lambda: ferried(0, 1))
        if k == 3:
            when(end, lambda: ferried(3, 0))
        hop(k, 0).start()
        hop(k, 2).start()

    def scatter_far(k):
        scatter_corner(k)
        scatter_sides(k)

    def scatter_turn(k):
        hop(k, 0).wait_recv()
        add(cell(k, 1, 0, 0), low, from_y[k * 2 + 1])
        hop(k, 4).start()
        hop(k, 2).wait_recv()
        add(cell(k, 0, 1, 0), high, from_x[k * 2 + 1])
        hop(k, 5).start()

    def scatter_end(k):
        hop(k, 1).wait_recv()
        add(cell(k, 0, 0, 0), low, from_y[k * 2])
        hop(k, 3).wait_recv()
        add(cell(k, 0, 0, 0), high, from_x[k * 2])
        hop(k, 4).wait_recv()
        add(cell(k, 0, 0, 0), low, last_x[k])
        hop(k, 5).wait_recv()
        add(cell(k, 0, 0, 0), high, last_y[k])
        if k == 3:
            when(end, lambda: detour().start())
            home(3, 0).start()
        elif k:
            home(k, 0).start()
            home(k, 1).start()

    own = [pltpu.make_async_copy(tokens, buf.at[cell(0, 0, 0, 0)], own_sem.at[0]),
           pltpu.make_async_copy(ids, all_ids.at[0], own_sem.at[1]),
           pltpu.make_async_copy(scales, all_scales.at[0], own_sem.at[2])]
    for copy in own:
        copy.start()
    barrier = pltpu.get_barrier_semaphore()
    greeted = [here.device(k=k, dx=dx) for k in range(depth) for dx in (0, 1) if k or dx]
    greeted += [over["y"], partner]
    for who in greeted:
        pl.semaphore_signal(barrier, inc=1, device_id=who, device_id_type=MESH)
    pl.semaphore_wait(barrier, len(greeted))
    for k in range(depth):
        for dx in (0, 1):
            if k or dx:
                meta_push(k, dx).start()
    flow_start(0)
    when(mid, lambda: flow_start(1))
    for copy in own:
        copy.wait()
    gather_a(0)
    loads = [pltpu.make_async_copy(ref.at[e], wide.at[side, e], w_sem.at[side, e])
             for side, ref in enumerate((gate, up)) for e in range(experts)]
    deeps = [pltpu.make_async_copy(down.at[e], stage, w_sem.at[2, e]) for e in range(experts)]
    deeps[0].start()
    for load in loads:
        load.start()
    place[...] = jnp.zeros(place.shape, f32)

    def turn(e):
        deeps[e].wait()
        for n in range(0, width, 256):
            size = min(256, width - n)
            eye = (lax.broadcasted_iota(jnp.int32, (size, size), 0)
                   == lax.broadcasted_iota(jnp.int32, (size, size), 1)).astype(f32).astype(bf16)
            got = lax.dot_general(eye, stage[:, pl.ds(n, size)], (((1,), (1,)), ((), ())),
                                  preferred_element_type=f32)
            deep[e, pl.ds(n, size), :] = got.astype(bf16)
        if e + 1 < experts:
            deeps[e + 1].start()

    turn(0)
    gather_b(0)
    when(mid, turn_early)
    column(1)
    ahead = (lax.broadcasted_iota(jnp.int32, (tok, tok), 0)
             < lax.broadcasted_iota(jnp.int32, (tok, tok), 1)).astype(f32).astype(bf16)
    slot_row = lax.broadcasted_iota(jnp.int32, (cap, tok), 0).astype(f32)
    slot_col = lax.broadcasted_iota(jnp.int32, (tok, cap), 1).astype(f32)
    row_at = lax.broadcasted_iota(jnp.int32, (8, tok), 0)

    def masks(k):
        picked = jnp.zeros((8, tok), f32)
        known = jnp.zeros((8, tok), f32)
        for dx in (0, 1):
            named, scaled = all_ids[k * 2 + dx], all_scales[k * 2 + dx]
            for e in range(experts):
                n = dx * experts + e
                hit = (named == here.ep * experts + e).astype(f32)
                chosen = jnp.sum(hit, axis=0, keepdims=True)
                picked = jnp.where(row_at == n, chosen, picked)
                held = jnp.sum(hit * scaled, axis=0, keepdims=True)
                known = jnp.where(row_at == 2 * experts + n, held, known)
        slot = jnp.dot(picked.astype(bf16), ahead, preferred_element_type=f32)
        slot = jnp.where(picked > 0.5, slot, -1.0)
        place[0:8, :] = jnp.where(row_at < 2 * experts, slot, known)
        turned = jnp.transpose(place[...])
        for dx in (0, 1):
            for e in range(experts):
                n = dx * experts + e
                at = pl.ds(e * cap, cap)
                take[k, dx, at, :] = (slot_row == slot[n:n + 1, :]).astype(f32).astype(bf16)
                hot = (slot_col == turned[:, n:n + 1]).astype(f32)
                back[k, dx, :, at] = hot.astype(bf16)
                held = turned[:, 2 * experts + n:2 * experts + n + 1]
                weigh[k, e, :, pl.ds(dx * cap, cap)] = jnp.broadcast_to(
                    jnp.sum(hot * held, axis=0, keepdims=True), (8, cap))

    def prepare(k, carry):
        @pl.when(k > 0)
        def _():
            meta_push(k, 0, True).wait_recv()
        meta_push(k, 1, True).wait_recv()
        masks(k)
        return carry

    for e in range(1, experts):
        turn(e)
    lax.fori_loop(0, depth, prepare, 0)
    gather_c(0, True)
    gather_c(0, False)
    for load in loads:
        load.wait()

    def block(k, dx, j):
        return cell(k, dx, (here.y + j // 2) % 2, (here.c + j % 2) % 2)

    def dispatch(k):
        for dx in (0, 1):
            for j in range(4):
                got = jnp.dot(buf[block(k, dx, j)], back[k, dx], preferred_element_type=f32)
                rows[dx, pl.ds(j * feat, feat), :] = got.astype(bf16)

    def enter(k, e):
        at = pl.ds(e * cap, cap)
        held = jnp.concatenate([rows[0, :, at], rows[1, :, at]], axis=1)
        for n in range(0, ff, STEP):
            part = pl.ds(n, min(STEP, ff - n))
            g = jnp.dot(wide[0, e, part, :], held, preferred_element_type=f32)
            u = jnp.dot(wide[1, e, part, :], held, preferred_element_type=f32)
            hid[part, :] = act_weighted(g, u, weigh[k, e, 0:1, :])

    def leave(e):
        at = pl.ds(e * cap, cap)
        for n in range(0, width, 2 * STEP):
            part = pl.ds(n, min(2 * STEP, width - n))
            got = jnp.dot(deep[e, part, :], hid[...], preferred_element_type=f32).astype(bf16)
            rows[0, part, at] = got[:, 0:cap]
            rows[1, part, at] = got[:, cap:2 * cap]

    def combine(k, dx):
        for j in range(4):
            got = jnp.dot(rows[dx, pl.ds(j * feat, feat), :], take[k, dx], preferred_element_type=f32)
            buf[block(k, dx, j)] = got.astype(bf16)

    def at(condition):
        return pl.when(condition)

    def plane(step, carry):
        last = depth - 1
        k = (step + here.mid) % depth
        ahead_of = (k < last) & (end | (k > 0))
        gather_d(k)
        dispatch(k)

        @at((k == 0) & mid)
        def _():
            scatter_far(3)
            scatter_end(2)

        @at(k == last)
        def _():
            when(mid, lambda: scatter_ferry(2))
            when(end, lambda: scatter_far(2))
        enter(k, 0)

        @at((k == 0) & end)
        def _():
            gather_b(1)

        @at(k == 1)
        def _():
            gather_b(2)
            column(3)

        @at(k == 2)
        def _():
            scatter_near(1)

        @at(k == last)
        def _():
            when(mid, lambda: scatter_near(2))
            scatter_end(1)
        leave(0)

        @at((k == 0) & end)
        def _():
            column(2)

        @at((k == 0) & mid)
        def _():
            scatter_turn(3)
        enter(k, 1)

        @at(k == 2)
        def _():
            gather_b(3)

        @at(ahead_of)
        def _():
            gather_c(k + 1, True)

        leave(1)

        @at((k == last) & end)
        def _():
            scatter_turn(2)
        gather_sent(k)

        @at(ahead_of)
        def _():
            gather_c(k + 1, False)
        for dx in (1, 0):
            combine(k, dx)
            give(k, dx, 1).start()
            give(k, dx, 0).start()
        return carry

    @pl.when(mid)
    def _():
        gather_b(1)
        column(2)
        gather_c(1, True)
        gather_c(1, False)
    lax.fori_loop(0, depth, plane, 0)

    @pl.when(end)
    def _():
        scatter_far(3)
        scatter_end(2)
        scatter_turn(3)

    scatter_far(0)
    scatter_end(3)
    scatter_turn(0)
    when(mid, onward)
    scatter_end(0)
    for p in (0, 1):
        total = buf[cell(0, 0, 0, 0), parts[p]].astype(f32)
        for k in range(1, depth - p):
            home(k, p, True).wait_recv()
            total = total + from_z[k - 1, parts[p]].astype(f32)
        if p == 0:
            out[low, :] = total.astype(out.dtype)
        else:
            when(end, lambda: out.__setitem__((high, slice(None)), total.astype(out.dtype)))

            @pl.when(mid)
            def _():
                home(3, 1, True).wait_recv()
                out[high, :] = (total + from_z[2, high].astype(f32)).astype(out.dtype)
    for k in range(depth):
        for dx in (0, 1):
            if k or dx:
                meta_push(k, dx).wait_send()
            for dy in (0, 1):
                give(k, dx, dy).wait_send()
        for n in (1, 3, 4, 5):
            hop(k, n).wait_send()

        def cornered():
            hop(k, 0).wait_send()
            hop(k, 2).wait_send()
        if k == 2:
            when(end, cornered)
        elif k != 1:
            cornered()
        if k:
            home(k, 0).wait_send()
        if k in (1, 2):
            home(k, 1).wait_send()
    when(end, lambda: detour().wait_send())
    ferry(1).wait_send()
    flow_sent(0)

    @pl.when(mid)
    def _():
        ferry(2).wait_send()
        flow_sent(1)
        home(3, 1).wait_send()


def fused(tokens, expert_ids, combine_weights, gate_weight, up_weight, down_weight, depth, capacity):
    tok, feat = tokens.shape
    experts, width, ff = gate_weight.shape
    top = expert_ids.shape[1]
    f32, bf16 = jnp.float32, jnp.bfloat16
    half = -(-feat // 32) * 16
    rest = feat - half
    dma = pltpu.SemaphoreType.DMA
    scratch = [
        pltpu.VMEM((depth * 8, feat, tok), bf16), pltpu.VMEM((depth * 4, feat, tok), bf16),
        pltpu.VMEM((depth * 2, half, tok), bf16), pltpu.VMEM((depth * 2, rest, tok), bf16),
        pltpu.VMEM((depth, half, tok), bf16), pltpu.VMEM((depth, rest, tok), bf16),
        pltpu.VMEM((depth - 1, feat, tok), bf16), pltpu.VMEM((2, feat, tok), bf16),
        pltpu.VMEM((rest, tok), bf16),
        pltpu.VMEM((2, experts, ff, width), bf16), pltpu.VMEM((experts, width, ff), bf16),
        pltpu.VMEM((ff, width), bf16),
        pltpu.VMEM((2, width, experts * capacity), bf16),
        pltpu.VMEM((ff, 2 * capacity), bf16),
        pltpu.VMEM((depth, 2, experts * capacity, tok), bf16),
        pltpu.VMEM((depth, 2, tok, experts * capacity), bf16),
        pltpu.VMEM((depth, experts, 8, 2 * capacity), f32), pltpu.VMEM((128, tok), f32),
        pltpu.VMEM((depth * 2, top, tok), jnp.int32), pltpu.VMEM((depth * 2, top, tok), f32),
        dma((3,)), dma((3, experts)), dma((2, depth * 2)), dma((2, depth * 2)),
        dma((5, 2)), dma((depth, 2)), dma((depth, 6)), dma((depth, 6)),
        dma((depth, 8)), dma((depth, 8)), dma((depth, 4)), dma((depth, 4)),
        dma((depth, 6)), dma((depth, 6)), dma((depth, 2)), dma((depth, 2)),
        dma((3, 2)), dma((2, 2)), dma((2,)), dma((2,)), dma((2,)),
    ]
    mixed = pl.pallas_call(
        fused_kernel,
        out_shape=jax.ShapeDtypeStruct((feat, tok), bf16),
        in_specs=[pl.BlockSpec(memory_space=pl.ANY)] * 6,
        out_specs=pl.BlockSpec(memory_space=pltpu.VMEM),
        scratch_shapes=scratch,
        compiler_params=pltpu.CompilerParams(
            collective_id=0, has_side_effects=True, vmem_limit_bytes=63 * 1024 * 1024),
    )(tokens.T, expert_ids.T, combine_weights.T, gate_weight.transpose(0, 2, 1),
      up_weight.transpose(0, 2, 1), down_weight)
    return mixed.T


def local(tokens, expert_ids, combine_weights, gate_weight, up_weight, down_weight):
    ep_count = lax.axis_size("ep")
    tp_count = lax.axis_size("tp")
    exp_local = gate_weight.shape[0]
    experts = exp_local * ep_count
    tok_rows = expert_ids.shape[0]
    top_count = expert_ids.shape[1]
    capacity = 2 * tok_rows * top_count // experts
    feat_width = tokens.shape[1]
    ff_width = gate_weight.shape[2]
    width = feat_width * tp_count
    f32, bf16 = jnp.float32, jnp.bfloat16
    if (ep_count, tp_count, exp_local, top_count) == (8, 4, 2, 4) and capacity % 128 == 0:
        return fused(tokens, expert_ids, combine_weights, gate_weight, up_weight, down_weight,
                     ep_count // 2, capacity)

    ids_all = lax.all_gather(expert_ids.T, "ep")
    weights_all = lax.all_gather(combine_weights.T, "ep")
    first = lax.axis_index("ep") * exp_local
    mine = first + jnp.arange(exp_local, dtype=jnp.int32)
    hit = ids_all[:, None, :, :] == mine[None, :, None, None]
    chosen = jnp.any(hit, axis=2)
    weight = jnp.sum(jnp.where(hit, weights_all[:, None, :, :], 0.0), axis=2)

    ahead = jnp.triu(jnp.ones((tok_rows, tok_rows), bf16), 1)
    slot = lax.dot_general(
        chosen.reshape(-1, tok_rows).astype(bf16), ahead, (((1,), (0,)), ((), ())),
        preferred_element_type=f32,
    ).astype(jnp.int32).reshape(chosen.shape)
    place = jnp.where(chosen, slot, -1)
    take = place[:, :, None, :] == jnp.arange(capacity, dtype=jnp.int32)[None, None, :, None]
    slot_weight = jnp.sum(jnp.where(take, weight[:, :, None, :], 0.0), axis=3)
    take = take.astype(bf16)

    paired = tp_count == 2 * 2 and ep_count % 2 == 0
    spread = gather_all(tokens, ep_count, tp_count) if paired else lax.all_gather(
        tokens, ("ep", "tp")
    )
    gathered = spread.reshape(
        ep_count, tp_count, tok_rows, feat_width
    )
    routed = jnp.einsum(
        "sect,sjtf->escjf", take, gathered, preferred_element_type=f32
    ).astype(bf16)
    rows = routed.reshape(exp_local, ep_count * capacity, width)
    gate_new = jnp.einsum("erd,edf->erf", rows, gate_weight, preferred_element_type=f32)
    up_new = jnp.einsum("erd,edf->erf", rows, up_weight, preferred_element_type=f32)
    row_weight = slot_weight.transpose(1, 0, 2).reshape(exp_local, ep_count * capacity, 1)
    hidden = (activate(gate_new, up_new) * row_weight).astype(bf16)
    expert_out = jnp.einsum(
        "erf,efd->erd", hidden, down_weight, preferred_element_type=f32
    ).astype(bf16)
    expert_out = expert_out.reshape(exp_local, ep_count, capacity, tp_count, feat_width)
    partial = jnp.einsum(
        "sect,escjf->sjtf", take, expert_out, preferred_element_type=f32
    ).astype(bf16)
    partial = partial.reshape(ep_count * tp_count, tok_rows, feat_width)
    if paired:
        return scatter_sum(partial, ep_count)
    mixed = lax.psum_scatter(partial, ("ep", "tp"), scatter_dimension=0, tiled=True)
    return mixed.reshape(tok_rows, feat_width)


def solution(mesh):
    in_specs = (
        P("ep", "tp"),
        P("ep", None),
        P("ep", None),
        P("ep", None, "tp"),
        P("ep", None, "tp"),
        P("ep", "tp", None),
    )
    out_specs = P("ep", "tp")
    return jax.shard_map(local, mesh=mesh, in_specs=in_specs, out_specs=out_specs, check_vma=False)
```

```python
import functools

import jax
import jax.numpy as jnp
from jax import lax
from jax.experimental import pallas as pl
from jax.experimental.pallas import tpu as pltpu
from jax.sharding import PartitionSpec as P


def activate(gate_acc, up_acc):
    return (up_acc + 1.0) * gate_acc * jax.nn.sigmoid(1.702 * gate_acc)


MESH = pl.DeviceIdType.MESH


class Place:
    def __init__(self, depth):
        self.depth = depth
        e, t = lax.axis_index("ep"), lax.axis_index("tp")
        self.z, self.x, self.y, self.c = e // 2, e % 2, t // 2, t % 2

    def device(self, k=0, dx=0, dy=0, dc=0):
        ep = (self.z + k) % self.depth * 2 + (self.x + dx) % 2
        tp = (self.y + dy) % 2 * 2 + (self.c + dc) % 2
        return ep, tp

    def block(self, k=0, dx=0, dy=0, dc=0):
        ep, tp = self.device(k, dx, dy, dc)
        return ep * 4 + tp

    def greet(self):
        barrier = pltpu.get_barrier_semaphore()
        near = [self.device(k=k) for k in range(1, self.depth)]
        near += [self.device(dx=1), self.device(dy=1), self.device(dc=1)]
        for who in near:
            pl.semaphore_signal(barrier, inc=1, device_id=who, device_id_type=MESH)
        pl.semaphore_wait(barrier, len(near))


def gather_kernel(depth, own, out, lane_recv, pair_recv, lane_send, pair_send, own_sem):
    here = Place(depth)
    half = own.shape[0] // 2
    sent = []

    def piece(k, dx, dy, part):
        rows = pl.ds(part * half, half)
        if (k, dx, dy) == (0, 0, 0):
            return own.at[rows]
        return out.at[here.block(k, dx, dy), rows]

    def lane_slot(k, dx, dy):
        ep, tp = here.device(k, dx, dy)
        return ep * 2 + tp // 2

    def push(k, dx, dy, part, to):
        rows = pl.ds(part * half, half)
        copy = pltpu.make_async_remote_copy(
            src_ref=piece(k, dx, dy, part), dst_ref=out.at[here.block(k, dx, dy), rows],
            send_sem=lane_send.at[len(sent)], recv_sem=lane_recv.at[lane_slot(k, dx, dy), part],
            device_id=to, device_id_type=MESH)
        copy.start()
        sent.append(copy)

    def pair(k, dx, dy, part):
        rows = pl.ds(part * half, half)
        slot = lane_slot(k, dx, dy)
        copy = pltpu.make_async_remote_copy(
            src_ref=piece(k, dx, dy, part), dst_ref=out.at[here.block(k, dx, dy), rows],
            send_sem=pair_send.at[slot, part], recv_sem=pair_recv.at[slot, part],
            device_id=here.device(dc=1), device_id_type=MESH)
        copy.start()

    def landed(k, dx, dy, part, to):
        rows = pl.ds(part * half, half)
        ref = out.at[here.block(k, dx, dy), rows]
        pltpu.make_async_remote_copy(
            src_ref=ref, dst_ref=ref, send_sem=lane_send.at[0],
            recv_sem=lane_recv.at[lane_slot(k, dx, dy), part],
            device_id=to, device_id_type=MESH).wait_recv()

    here.greet()
    over_x, over_y = here.device(dx=1), here.device(dy=1)
    for k in range(1, depth):
        for part in (0, 1):
            push(0, 0, 0, part, here.device(k=depth - k))
    store = pltpu.make_async_copy(own, out.at[here.block()], own_sem)
    store.start()
    for k in range(depth):
        if k:
            landed(k, 0, 0, 0, here.device(k=k))
            landed(k, 0, 0, 1, here.device(k=k))
        push(k, 0, 0, 0, over_x)
        push(k, 0, 0, 1, over_y)
        push(k, 0, 0, 0, over_y)
        push(k, 0, 0, 1, over_x)
        pair(k, 0, 0, 0)
        pair(k, 0, 0, 1)
        landed(k, 1, 0, 0, over_x)
        push(k, 1, 0, 0, over_y)
        pair(k, 1, 0, 0)
        landed(k, 0, 1, 1, over_y)
        push(k, 0, 1, 1, over_x)
        pair(k, 0, 1, 1)
    for k in range(depth):
        landed(k, 0, 1, 0, over_y)
        pair(k, 0, 1, 0)
        landed(k, 1, 0, 1, over_x)
        pair(k, 1, 0, 1)
        landed(k, 1, 1, 0, over_y)
        pair(k, 1, 1, 0)
        landed(k, 1, 1, 1, over_x)
        pair(k, 1, 1, 1)
    store.wait()
    for copy in sent:
        copy.wait_send()
    for k in range(depth):
        for dx in (0, 1):
            for dy in (0, 1):
                slot = lane_slot(k, dx, dy)
                for part in (0, 1):
                    rows = pl.ds(part * half, half)
                    copy = pltpu.make_async_remote_copy(
                        src_ref=piece(k, dx, dy, part),
                        dst_ref=out.at[here.block(k, dx, dy, 1), rows],
                        send_sem=pair_send.at[slot, part], recv_sem=pair_recv.at[slot, part],
                        device_id=here.device(dc=1), device_id_type=MESH)
                    copy.wait_send()
                    copy.wait_recv()


def gather_all(tokens, ep_count, tp_count):
    rows, width = tokens.shape
    depth = ep_count // 2
    blocks = ep_count * tp_count
    sends = 2 * (depth - 1) + 6 * depth
    dma = pltpu.SemaphoreType.DMA
    return pl.pallas_call(
        functools.partial(gather_kernel, depth),
        out_shape=jax.ShapeDtypeStruct((blocks, rows, width), tokens.dtype),
        in_specs=[pl.BlockSpec(memory_space=pltpu.VMEM)],
        out_specs=pl.BlockSpec(memory_space=pl.ANY),
        scratch_shapes=[dma((blocks // 2, 2)), dma((blocks // 2, 2)), dma((sends,)),
                        dma((blocks // 2, 2)), dma(())],
        compiler_params=pltpu.CompilerParams(collective_id=0, has_side_effects=True),
    )(tokens)


def scatter_kernel(depth, part_ref, out, acc, inc, from_y, from_x, last_x, last_y, from_z,
                   load_sem, pair_send, pair_recv, send_sem, recv_sem):
    here = Place(depth)
    rows = out.shape[0]
    half = rows // 2
    low, high = pl.ds(0, half), pl.ds(half, half)
    order = list(range(1, depth)) + [0]
    spread = ((1, 1), (0, 1), (1, 0), (0, 0))
    over_x, over_y = here.device(dx=1), here.device(dy=1)
    sent = []
    loads, pairs = {}, {}
    cell = lambda k, dx, dy: (k * 2 + dx) * 2 + dy

    def add(at, part, got):
        acc[at, part] = (acc[at, part].astype(jnp.float32) + got.astype(jnp.float32)).astype(acc.dtype)

    def send(src, dst, to):
        copy = pltpu.make_async_remote_copy(
            src_ref=src, dst_ref=dst, send_sem=send_sem.at[len(sent)],
            recv_sem=recv_sem.at[len(sent)], device_id=to, device_id_type=MESH)
        copy.start()
        sent.append(copy)
        return copy

    here.greet()
    for k in order:
        for dx, dy in spread:
            i = cell(k, dx, dy)
            pairs[i] = pltpu.make_async_remote_copy(
                src_ref=part_ref.at[here.block(k, dx, dy, 1)], dst_ref=inc.at[i],
                send_sem=pair_send.at[i], recv_sem=pair_recv.at[i],
                device_id=here.device(dc=1), device_id_type=MESH)
            pairs[i].start()
            loads[i] = pltpu.make_async_copy(
                part_ref.at[here.block(k, dx, dy)], acc.at[i], load_sem.at[i])
            loads[i].start()

    wait_for = {}

    def first(k):
        for dx, dy in spread:
            i = cell(k, dx, dy)
            loads[i].wait()
            pairs[i].wait_recv()
            add(i, pl.ds(0, rows), inc[i])
            if dy:
                wait_for["y", k, dx] = send(acc.at[i, low], from_y.at[k * 2 + dx], over_y)
            if dx:
                wait_for["x", k, dy] = send(acc.at[i, high], from_x.at[k * 2 + dy], over_x)

    def second(k):
        wait_for["y", k, 1].wait_recv()
        add(cell(k, 1, 0), low, from_y[k * 2 + 1])
        wait_for["lx", k] = send(acc.at[cell(k, 1, 0), low], last_x.at[k], over_x)
        wait_for["x", k, 1].wait_recv()
        add(cell(k, 0, 1), high, from_x[k * 2 + 1])
        wait_for["ly", k] = send(acc.at[cell(k, 0, 1), high], last_y.at[k], over_y)
        wait_for["y", k, 0].wait_recv()
        add(cell(k, 0, 0), low, from_y[k * 2])
        wait_for["x", k, 0].wait_recv()
        add(cell(k, 0, 0), high, from_x[k * 2])

    def third(k):
        wait_for["lx", k].wait_recv()
        add(cell(k, 0, 0), low, last_x[k])
        wait_for["ly", k].wait_recv()
        add(cell(k, 0, 0), high, last_y[k])
        if k:
            wait_for["z", k] = send(acc.at[cell(k, 0, 0)], from_z.at[k - 1], here.device(k=k))

    for i in range(depth + 2):
        if i < depth:
            first(order[i])
        if 0 <= i - 1 < depth:
            second(order[i - 1])
        if 0 <= i - 2:
            third(order[i - 2])
    total = acc[0].astype(jnp.float32)
    for k in range(1, depth):
        wait_for["z", k].wait_recv()
        total = total + from_z[k - 1].astype(jnp.float32)
    out[...] = total.astype(out.dtype)
    for copy in sent:
        copy.wait_send()
    for copy in pairs.values():
        copy.wait_send()


def scatter_sum(partial, ep_count):
    blocks, rows, width = partial.shape
    depth = ep_count // 2
    lane, half = blocks // 2, rows // 2
    sends = 6 * depth + depth - 1
    dma, kind = pltpu.SemaphoreType.DMA, partial.dtype
    return pl.pallas_call(
        functools.partial(scatter_kernel, depth),
        out_shape=jax.ShapeDtypeStruct((rows, width), kind),
        in_specs=[pl.BlockSpec(memory_space=pl.ANY)],
        out_specs=pl.BlockSpec(memory_space=pltpu.VMEM),
        scratch_shapes=[
            pltpu.VMEM((lane, rows, width), kind), pltpu.VMEM((lane, rows, width), kind),
            pltpu.VMEM((2 * depth, half, width), kind), pltpu.VMEM((2 * depth, half, width), kind),
            pltpu.VMEM((depth, half, width), kind), pltpu.VMEM((depth, half, width), kind),
            pltpu.VMEM((depth - 1, rows, width), kind),
            dma((lane,)), dma((lane,)), dma((lane,)), dma((sends,)), dma((sends,)),
        ],
        compiler_params=pltpu.CompilerParams(
            collective_id=1, has_side_effects=True, vmem_limit_bytes=48 * 1024 * 1024),
    )(partial)


def act_weighted(gate_acc, up_acc, weight):
    return (activate(gate_acc, up_acc) * weight).astype(jnp.bfloat16)


STEP = 240
def when(condition, run):
    if isinstance(condition, bool):
        if condition:
            run()
    else:
        pl.when(condition)(run)


PUSHES = (((0, 0), 0, "x"), ((0, 0), 1, "y"), ((0, 0), 0, "y"), ((0, 0), 1, "x"),
          ((1, 0), 0, "y"), ((0, 1), 1, "x"))


class Grid:
    def __init__(self):
        e, t = lax.axis_index("ep"), lax.axis_index("tp")
        self.ep, self.tp = e, t
        self.z, self.x, self.y, self.c = e // 2, e % 2, t // 2, t % 2
        self.mid = (self.z + 1) // 2 % 2

    def away(self, m, dx=0, dy=0, dc=0):
        z = (self.z // 2 + m // 2) % 2 * 2 + (self.z % 2 + m % 2) % 2
        return z * 2 + (self.x + dx) % 2, (self.y + dy) % 2 * 2 + (self.c + dc) % 2

    def device(self, k=0, dx=0, dy=0, dc=0):
        return self.away((k + self.mid * (4 - 2 * k)) % 4, dx, dy, dc)

    def seen(self, k):
        return 3 - 2 * self.mid if k % 2 else k


def fused_kernel(tokens, ids, scales, gate, up, down, out, buf, inc, from_y, from_x, last_x, last_y,
                 from_z, aside, passing, wide, deep, stage, rows, hid, take, back, weigh, place, all_ids, all_scales,
                 own_sem, w_sem, meta_send, meta_recv, z_send, z_recv, lane_send, lane_recv,
                 pair_send, pair_recv, sp_send, sp_recv, sx_send, sx_recv, sz_send, sz_recv,
                 cross_send, cross_recv, ferry_send, ferry_recv, detour_sem):
    f32, bf16 = jnp.float32, jnp.bfloat16
    here = Grid()
    depth = from_z.shape[0] + 1
    feat, tok = buf.shape[1], buf.shape[2]
    experts, cap = wide.shape[1], rows.shape[2] // wide.shape[1]
    ff, width = wide.shape[2], wide.shape[3]
    half = from_y.shape[1]
    low, high = pl.ds(0, half), pl.ds(half, feat - half)
    parts = (low, high)
    over = {"x": here.device(dx=1), "y": here.device(dy=1)}
    partner = here.device(dc=1)

    def cell(k, dx, dy, dc):
        return k * 8 + dx * 4 + dy * 2 + dc

    def remote(src, dst, send, recv, to):
        return pltpu.make_async_remote_copy(
            src_ref=src, dst_ref=dst, send_sem=send, recv_sem=recv,
            device_id=to, device_id_type=MESH)

    near, other = here.away(1), here.away(3)
    mid, end = here.mid == 1, here.mid == 0

    def flow(n, p):
        source, label = ((None, here.seen(1)), (None, 1), (1, 2), (3, 2), (2, 3))[n]
        src = tokens if source is None else buf.at[cell(source, 0, 0, 0)]
        return remote(src.at[parts[p]], buf.at[cell(label, 0, 0, 0), parts[p]],
                      z_send.at[n, p], z_recv.at[label, p], other if n in (1, 3) else near)

    def flow_start(n):
        flow(n, 0).start()
        flow(n, 1).start()

    def flow_sent(n):
        flow(n, 0).wait_send()
        flow(n, 1).wait_send()

    def arrive(k):
        for p in (0, 1):
            at = buf.at[cell(k, 0, 0, 0), parts[p]]
            remote(at, at, z_send.at[0, p], z_recv.at[k, p], near).wait_recv()

    def lane_push(k, n):
        (dx, dy), p, axis = PUSHES[n]
        to = (1 - dx, dy) if axis == "x" else (dx, 1 - dy)
        return remote(buf.at[cell(k, dx, dy, 0), parts[p]], buf.at[cell(k, *to, 0), parts[p]],
                      lane_send.at[k, n], lane_recv.at[k, n], over[axis])

    def pair(k, dx, dy, p):
        n = (dx * 2 + dy) * 2 + p
        return remote(buf.at[cell(k, dx, dy, 0), parts[p]], buf.at[cell(k, dx, dy, 1), parts[p]],
                      pair_send.at[k, n], pair_recv.at[k, n], partner)

    class Both:
        def __init__(self, *copies):
            self.copies = copies

        def start(self):
            for copy in self.copies:
                copy.start()

        def wait_recv(self):
            for copy in self.copies:
                copy.wait_recv()

        def wait_send(self):
            for copy in self.copies:
                copy.wait_send()

    def meta_push(k, dx, to_me=False):
        to = here.device(k=k, dx=dx)
        n = k * 2 + dx if to_me else here.seen(k) * 2 + dx
        return Both(remote(ids, all_ids.at[n], meta_send.at[0, n], meta_recv.at[0, n], to),
                    remote(scales, all_scales.at[n], meta_send.at[1, n], meta_recv.at[1, n], to))

    def gather_a(k):
        for n in range(4):
            lane_push(k, n).start()
        pair(k, 0, 0, 0).start()
        pair(k, 0, 0, 1).start()

    def column(k):
        if k == 3:
            when(end, lambda: arrive(3))
        else:
            arrive(k)
            when(mid, lambda: flow_start(2 if k == 1 else 4))
        gather_a(k)

    def turn_early():
        arrive(3)
        flow_start(3)

    def cross(n, p):
        source, label = ((0, 3), (2, 3), (1, 2))[n]
        return remote(buf.at[cell(source, 1, 1, 0), parts[p]],
                      buf.at[cell(label, 1, 1, 0), parts[p]],
                      cross_send.at[n, p], cross_recv.at[label - 2, p], near)

    def crossed(k, p):
        at = buf.at[cell(k, 1, 1, 0), parts[p]]
        remote(at, at, cross_send.at[0, p], cross_recv.at[k - 2, p], near).wait_recv()

    def inside(k):
        if isinstance(k, int):
            return (True, True, mid, False)[k]
        return k < 2 + here.mid

    def outside(k):
        if isinstance(k, int):
            return (False, False, end, True)[k]
        return k >= 2 + here.mid

    def gather_b(k):
        lane_push(k, 0).wait_recv()
        when(inside(k), lambda: lane_push(k, 4).start())
        pair(k, 1, 0, 0).start()
        lane_push(k, 1).wait_recv()
        when(inside(k), lambda: lane_push(k, 5).start())
        pair(k, 0, 1, 1).start()

    def gather_c(k, first):
        if first:
            lane_push(k, 2).wait_recv()
            pair(k, 0, 1, 0).start()
            lane_push(k, 3).wait_recv()
            pair(k, 1, 0, 1).start()
        else:
            for p in (0, 1):
                def relayed():
                    lane_push(k, 4 + p).wait_recv()
                    if isinstance(k, int):
                        if k == 0:
                            when(end, lambda: cross(0, p).start())
                        if k == 1:
                            when(mid, lambda: cross(2, p).start())
                    else:
                        when((k == 2) & mid, lambda: cross(1, p).start())
                when(inside(k), relayed)
                when(outside(k), lambda: crossed(k, p))
                pair(k, 1, 1, p).start()

    def gather_d(k):
        for dx in (0, 1):
            for dy in (0, 1):
                for p in (0, 1):
                    pair(k, dx, dy, p).wait_recv()

    def gather_sent(k):
        for n in range(4):
            lane_push(k, n).wait_send()

        def relayed():
            for p in (0, 1):
                lane_push(k, 4 + p).wait_send()
        when(inside(k), relayed)
        for at, n, side in ((0, 0, end), (2, 1, mid), (1, 2, mid)):
            @pl.when((k == at) & side)
            def _():
                cross(n, 0).wait_send()
                cross(n, 1).wait_send()

        @pl.when(mid)
        def _():
            for at, n in ((1, 2), (3, 3), (2, 4)):
                @pl.when(k == at)
                def _():
                    flow_sent(n)

        for dx in (0, 1):
            for dy in (0, 1):
                for p in (0, 1):
                    pair(k, dx, dy, p).wait_send()

    def give(k, dx, dy):
        n = dx * 2 + dy
        return remote(buf.at[cell(k, dx, dy, 1)], inc.at[k * 4 + n],
                      sp_send.at[k, n], sp_recv.at[k, n], partner)

    def hop(k, n):
        src, dst, axis = (
            (buf.at[cell(k, 1, 1, 0), low], from_y.at[k * 2 + 1], "y"),
            (buf.at[cell(k, 0, 1, 0), low], from_y.at[k * 2], "y"),
            (buf.at[cell(k, 1, 1, 0), high], from_x.at[k * 2 + 1], "x"),
            (buf.at[cell(k, 1, 0, 0), high], from_x.at[k * 2], "x"),
            (buf.at[cell(k, 1, 0, 0), low], last_x.at[k], "x"),
            (buf.at[cell(k, 0, 1, 0), high], last_y.at[k], "y"))[n]
        return remote(src, dst, sx_send.at[k, n], sx_recv.at[k, n], over[axis])

    def home(k, p, to_me=False):
        at = k if to_me else here.seen(k)
        return remote(buf.at[cell(k, 0, 0, 0), parts[p]], from_z.at[at - 1, parts[p]],
                      sz_send.at[k, p], sz_recv.at[at, p], here.device(k=k))

    def detour():
        return remote(buf.at[cell(3, 0, 0, 0), high], passing,
                      detour_sem.at[0], detour_sem.at[1], here.device(k=2))

    def onward():
        detour().wait_recv()
        add(cell(3, 0, 0, 0), high, passing[...])
        home(3, 1).start()

    def add(at, part, got):
        buf[at, part] = (buf[at, part].astype(f32) + got.astype(f32)).astype(bf16)

    def ferry(k):
        slot = (2, 1 - here.mid, 0)[k]
        return remote(buf.at[cell(k, 1, 1, 0)], aside.at[slot], ferry_send.at[k],
                      ferry_recv.at[slot], here.away(1 + 2 * here.mid) if k == 1 else near)

    def ferried(k, slot):
        remote(aside.at[slot], aside.at[slot], ferry_send.at[0], ferry_recv.at[slot],
               near).wait_recv()
        add(cell(k, 1, 1, 0), pl.ds(0, feat), aside[slot])

    def merge(k, dx, dy):
        give(k, dx, dy).wait_recv()
        add(cell(k, dx, dy, 0), pl.ds(0, feat), inc[k * 4 + dx * 2 + dy])

    def scatter_ferry(k):
        merge(k, 1, 1)
        ferry(k).start()

    def scatter_near(k):
        if k == 1:
            scatter_ferry(k)
        merge(k, 0, 1)
        hop(k, 1).start()
        hop(k, 5).start()
        merge(k, 1, 0)
        hop(k, 3).start()
        hop(k, 4).start()
        merge(k, 0, 0)

    def scatter_sides(k):
        merge(k, 0, 1)
        hop(k, 1).start()
        merge(k, 1, 0)
        hop(k, 3).start()
        merge(k, 0, 0)

    def scatter_corner(k):
        merge(k, 1, 1)
        if k == 0:
            when(mid, lambda: ferried(0, 0))
            when(mid, lambda: ferried(0, 1))
        if k == 3:
            when(end, lambda: ferried(3, 0))
            when(mid, lambda: ferried(3, 2))
        hop(k, 0).start()
        hop(k, 2).start()

    def scatter_far(k):
        scatter_corner(k)
        scatter_sides(k)

    def scatter_turn(k):
        hop(k, 0).wait_recv()
        add(cell(k, 1, 0, 0), low, from_y[k * 2 + 1])
        hop(k, 4).start()
        hop(k, 2).wait_recv()
        add(cell(k, 0, 1, 0), high, from_x[k * 2 + 1])
        hop(k, 5).start()

    def scatter_end(k):
        hop(k, 1).wait_recv()
        add(cell(k, 0, 0, 0), low, from_y[k * 2])
        hop(k, 3).wait_recv()
        add(cell(k, 0, 0, 0), high, from_x[k * 2])
        hop(k, 4).wait_recv()
        add(cell(k, 0, 0, 0), low, last_x[k])
        hop(k, 5).wait_recv()
        add(cell(k, 0, 0, 0), high, last_y[k])
        if k == 3:
            when(end, lambda: detour().start())
            home(3, 0).start()
            when(end, lambda: home(2, 1).start())
        elif k == 2:
            home(2, 0).start()
            when(mid, lambda: home(2, 1).start())
        elif k:
            home(k, 0).start()
            home(k, 1).start()

    own = [pltpu.make_async_copy(tokens, buf.at[cell(0, 0, 0, 0)], own_sem.at[0]),
           pltpu.make_async_copy(ids, all_ids.at[0], own_sem.at[1]),
           pltpu.make_async_copy(scales, all_scales.at[0], own_sem.at[2])]
    for copy in own:
        copy.start()
    barrier = pltpu.get_barrier_semaphore()
    greeted = [here.device(k=k, dx=dx) for k in range(depth) for dx in (0, 1) if k or dx]
    greeted += [over["y"], partner]
    for who in greeted:
        pl.semaphore_signal(barrier, inc=1, device_id=who, device_id_type=MESH)
    pl.semaphore_wait(barrier, len(greeted))
    for k in range(depth):
        for dx in (0, 1):
            if k or dx:
                meta_push(k, dx).start()
    flow_start(0)
    when(mid, lambda: flow_start(1))
    for copy in own:
        copy.wait()
    gather_a(0)
    loads = [pltpu.make_async_copy(ref.at[e], wide.at[side, e], w_sem.at[side, e])
             for side, ref in enumerate((gate, up)) for e in range(experts)]
    deeps = [pltpu.make_async_copy(down.at[e], stage, w_sem.at[2, e]) for e in range(experts)]
    deeps[0].start()
    for load in loads:
        load.start()
    place[...] = jnp.zeros(place.shape, f32)

    def turn(e):
        deeps[e].wait()
        for n in range(0, width, 256):
            size = min(256, width - n)
            eye = (lax.broadcasted_iota(jnp.int32, (size, size), 0)
                   == lax.broadcasted_iota(jnp.int32, (size, size), 1)).astype(f32).astype(bf16)
            got = lax.dot_general(eye, stage[:, pl.ds(n, size)], (((1,), (1,)), ((), ())),
                                  preferred_element_type=f32)
            deep[e, pl.ds(n, size), :] = got.astype(bf16)
        if e + 1 < experts:
            deeps[e + 1].start()

    turn(0)
    gather_b(0)
    when(mid, turn_early)
    column(1)
    ahead = (lax.broadcasted_iota(jnp.int32, (tok, tok), 0)
             < lax.broadcasted_iota(jnp.int32, (tok, tok), 1)).astype(f32).astype(bf16)
    slot_row = lax.broadcasted_iota(jnp.int32, (cap, tok), 0).astype(f32)
    slot_col = lax.broadcasted_iota(jnp.int32, (tok, cap), 1).astype(f32)
    row_at = lax.broadcasted_iota(jnp.int32, (8, tok), 0)

    def masks(k):
        picked = jnp.zeros((8, tok), f32)
        known = jnp.zeros((8, tok), f32)
        for dx in (0, 1):
            named, scaled = all_ids[k * 2 + dx], all_scales[k * 2 + dx]
            for e in range(experts):
                n = dx * experts + e
                hit = (named == here.ep * experts + e).astype(f32)
                chosen = jnp.sum(hit, axis=0, keepdims=True)
                picked = jnp.where(row_at == n, chosen, picked)
                held = jnp.sum(hit * scaled, axis=0, keepdims=True)
                known = jnp.where(row_at == 2 * experts + n, held, known)
        slot = jnp.dot(picked.astype(bf16), ahead, preferred_element_type=f32)
        slot = jnp.where(picked > 0.5, slot, -1.0)
        place[0:8, :] = jnp.where(row_at < 2 * experts, slot, known)
        turned = jnp.transpose(place[...])
        for dx in (0, 1):
            for e in range(experts):
                n = dx * experts + e
                at = pl.ds(e * cap, cap)
                take[k, dx, at, :] = (slot_row == slot[n:n + 1, :]).astype(f32).astype(bf16)
                hot = (slot_col == turned[:, n:n + 1]).astype(f32)
                back[k, dx, :, at] = hot.astype(bf16)
                held = turned[:, 2 * experts + n:2 * experts + n + 1]
                weigh[k, e, :, pl.ds(dx * cap, cap)] = jnp.broadcast_to(
                    jnp.sum(hot * held, axis=0, keepdims=True), (8, cap))

    def prepare(k, carry):
        @pl.when(k > 0)
        def _():
            meta_push(k, 0, True).wait_recv()
        meta_push(k, 1, True).wait_recv()
        masks(k)
        return carry

    for e in range(1, experts):
        turn(e)
    lax.fori_loop(0, depth, prepare, 0)
    gather_c(0, True)
    gather_c(0, False)
    for load in loads:
        load.wait()

    def block(k, dx, j):
        return cell(k, dx, (here.y + j // 2) % 2, (here.c + j % 2) % 2)

    def dispatch(k):
        for dx in (0, 1):
            for j in range(4):
                got = jnp.dot(buf[block(k, dx, j)], back[k, dx], preferred_element_type=f32)
                rows[dx, pl.ds(j * feat, feat), :] = got.astype(bf16)

    def enter(k, e):
        at = pl.ds(e * cap, cap)
        held = jnp.concatenate([rows[0, :, at], rows[1, :, at]], axis=1)
        for n in range(0, ff, STEP):
            part = pl.ds(n, min(STEP, ff - n))
            g = jnp.dot(wide[0, e, part, :], held, preferred_element_type=f32)
            u = jnp.dot(wide[1, e, part, :], held, preferred_element_type=f32)
            hid[part, :] = act_weighted(g, u, weigh[k, e, 0:1, :])

    def leave(e):
        at = pl.ds(e * cap, cap)
        for n in range(0, width, 2 * STEP):
            part = pl.ds(n, min(2 * STEP, width - n))
            got = jnp.dot(deep[e, part, :], hid[...], preferred_element_type=f32).astype(bf16)
            rows[0, part, at] = got[:, 0:cap]
            rows[1, part, at] = got[:, cap:2 * cap]

    def combine(k, dx):
        for j in range(4):
            got = jnp.dot(rows[dx, pl.ds(j * feat, feat), :], take[k, dx], preferred_element_type=f32)
            buf[block(k, dx, j)] = got.astype(bf16)

    def at(condition):
        return pl.when(condition)

    def plane(step, carry):
        last = depth - 1
        k = (step + here.mid) % depth
        ahead_of = (k < last) & (end | (k > 0))
        gather_d(k)
        dispatch(k)

        @at((k == 0) & mid)
        def _():
            scatter_far(3)
            scatter_end(2)

        @at(k == last)
        def _():
            when(mid, lambda: scatter_ferry(2))
            when(end, lambda: scatter_far(2))
        enter(k, 0)

        @at((k == 0) & end)
        def _():
            gather_b(1)

        @at(k == 1)
        def _():
            gather_b(2)
            column(3)

        @at(k == 2)
        def _():
            scatter_near(1)
            when(end, lambda: scatter_ferry(0))

        @at(k == last)
        def _():
            when(mid, lambda: scatter_near(2))
            scatter_end(1)
        leave(0)

        @at((k == 0) & end)
        def _():
            column(2)

        @at((k == 0) & mid)
        def _():
            scatter_turn(3)
        enter(k, 1)

        @at(k == 2)
        def _():
            gather_b(3)

        @at(ahead_of)
        def _():
            gather_c(k + 1, True)

        @at((k == last) & end)
        def _():
            scatter_turn(2)

        leave(1)

        gather_sent(k)

        @at(ahead_of)
        def _():
            gather_c(k + 1, False)
        for dx in (1, 0):
            combine(k, dx)
            give(k, dx, 1).start()
            give(k, dx, 0).start()
        return carry

    @pl.when(mid)
    def _():
        gather_b(1)
        column(2)
        gather_c(1, True)
        gather_c(1, False)
    lax.fori_loop(0, depth, plane, 0)

    @pl.when(end)
    def _():
        scatter_far(3)
        scatter_end(2)
        scatter_turn(3)
        scatter_near(0)
        scatter_end(3)

    @pl.when(mid)
    def _():
        scatter_far(0)
        scatter_end(3)
        scatter_turn(0)
        onward()
    scatter_end(0)
    for p in (0, 1):
        total = buf[cell(0, 0, 0, 0), parts[p]].astype(f32)
        for k in range(1, depth - p):
            home(k, p, True).wait_recv()
            total = total + from_z[k - 1, parts[p]].astype(f32)
        if p == 0:
            out[low, :] = total.astype(out.dtype)
        else:
            when(end, lambda: out.__setitem__((high, slice(None)), total.astype(out.dtype)))

            @pl.when(mid)
            def _():
                home(3, 1, True).wait_recv()
                out[high, :] = (total + from_z[2, high].astype(f32)).astype(out.dtype)
    for k in range(depth):
        for dx in (0, 1):
            if k or dx:
                meta_push(k, dx).wait_send()
            for dy in (0, 1):
                give(k, dx, dy).wait_send()
        for n in (1, 3, 4, 5):
            hop(k, n).wait_send()

        def cornered():
            hop(k, 0).wait_send()
            hop(k, 2).wait_send()
        if k == 3:
            cornered()
        elif k != 1:
            when(end if k else mid, cornered)
        if k:
            home(k, 0).wait_send()
        if k in (1, 2):
            home(k, 1).wait_send()

    @pl.when(end)
    def _():
        detour().wait_send()
        ferry(0).wait_send()
    ferry(1).wait_send()
    flow_sent(0)

    @pl.when(mid)
    def _():
        ferry(2).wait_send()
        flow_sent(1)
        home(3, 1).wait_send()


def fused(tokens, expert_ids, combine_weights, gate_weight, up_weight, down_weight, depth, capacity):
    tok, feat = tokens.shape
    experts, width, ff = gate_weight.shape
    top = expert_ids.shape[1]
    f32, bf16 = jnp.float32, jnp.bfloat16
    half = -(-feat // 32) * 16
    rest = feat - half
    dma = pltpu.SemaphoreType.DMA
    scratch = [
        pltpu.VMEM((depth * 8, feat, tok), bf16), pltpu.VMEM((depth * 4, feat, tok), bf16),
        pltpu.VMEM((depth * 2, half, tok), bf16), pltpu.VMEM((depth * 2, rest, tok), bf16),
        pltpu.VMEM((depth, half, tok), bf16), pltpu.VMEM((depth, rest, tok), bf16),
        pltpu.VMEM((depth - 1, feat, tok), bf16), pltpu.VMEM((3, feat, tok), bf16),
        pltpu.VMEM((rest, tok), bf16),
        pltpu.VMEM((2, experts, ff, width), bf16), pltpu.VMEM((experts, width, ff), bf16),
        pltpu.VMEM((ff, width), bf16),
        pltpu.VMEM((2, width, experts * capacity), bf16),
        pltpu.VMEM((ff, 2 * capacity), bf16),
        pltpu.VMEM((depth, 2, experts * capacity, tok), bf16),
        pltpu.VMEM((depth, 2, tok, experts * capacity), bf16),
        pltpu.VMEM((depth, experts, 8, 2 * capacity), f32), pltpu.VMEM((128, tok), f32),
        pltpu.VMEM((depth * 2, top, tok), jnp.int32), pltpu.VMEM((depth * 2, top, tok), f32),
        dma((3,)), dma((3, experts)), dma((2, depth * 2)), dma((2, depth * 2)),
        dma((5, 2)), dma((depth, 2)), dma((depth, 6)), dma((depth, 6)),
        dma((depth, 8)), dma((depth, 8)), dma((depth, 4)), dma((depth, 4)),
        dma((depth, 6)), dma((depth, 6)), dma((depth, 2)), dma((depth, 2)),
        dma((3, 2)), dma((2, 2)), dma((3,)), dma((3,)), dma((2,)),
    ]
    mixed = pl.pallas_call(
        fused_kernel,
        out_shape=jax.ShapeDtypeStruct((feat, tok), bf16),
        in_specs=[pl.BlockSpec(memory_space=pl.ANY)] * 6,
        out_specs=pl.BlockSpec(memory_space=pltpu.VMEM),
        scratch_shapes=scratch,
        compiler_params=pltpu.CompilerParams(
            collective_id=0, has_side_effects=True, vmem_limit_bytes=63 * 1024 * 1024),
    )(tokens.T, expert_ids.T, combine_weights.T, gate_weight.transpose(0, 2, 1),
      up_weight.transpose(0, 2, 1), down_weight)
    return mixed.T


def local(tokens, expert_ids, combine_weights, gate_weight, up_weight, down_weight):
    ep_count = lax.axis_size("ep")
    tp_count = lax.axis_size("tp")
    exp_local = gate_weight.shape[0]
    experts = exp_local * ep_count
    tok_rows = expert_ids.shape[0]
    top_count = expert_ids.shape[1]
    capacity = 2 * tok_rows * top_count // experts
    feat_width = tokens.shape[1]
    ff_width = gate_weight.shape[2]
    width = feat_width * tp_count
    f32, bf16 = jnp.float32, jnp.bfloat16
    if (ep_count, tp_count, exp_local, top_count) == (8, 4, 2, 4) and capacity % 128 == 0:
        return fused(tokens, expert_ids, combine_weights, gate_weight, up_weight, down_weight,
                     ep_count // 2, capacity)

    ids_all = lax.all_gather(expert_ids.T, "ep")
    weights_all = lax.all_gather(combine_weights.T, "ep")
    first = lax.axis_index("ep") * exp_local
    mine = first + jnp.arange(exp_local, dtype=jnp.int32)
    hit = ids_all[:, None, :, :] == mine[None, :, None, None]
    chosen = jnp.any(hit, axis=2)
    weight = jnp.sum(jnp.where(hit, weights_all[:, None, :, :], 0.0), axis=2)

    ahead = jnp.triu(jnp.ones((tok_rows, tok_rows), bf16), 1)
    slot = lax.dot_general(
        chosen.reshape(-1, tok_rows).astype(bf16), ahead, (((1,), (0,)), ((), ())),
        preferred_element_type=f32,
    ).astype(jnp.int32).reshape(chosen.shape)
    place = jnp.where(chosen, slot, -1)
    take = place[:, :, None, :] == jnp.arange(capacity, dtype=jnp.int32)[None, None, :, None]
    slot_weight = jnp.sum(jnp.where(take, weight[:, :, None, :], 0.0), axis=3)
    take = take.astype(bf16)

    paired = tp_count == 2 * 2 and ep_count % 2 == 0
    spread = gather_all(tokens, ep_count, tp_count) if paired else lax.all_gather(
        tokens, ("ep", "tp")
    )
    gathered = spread.reshape(
        ep_count, tp_count, tok_rows, feat_width
    )
    routed = jnp.einsum(
        "sect,sjtf->escjf", take, gathered, preferred_element_type=f32
    ).astype(bf16)
    rows = routed.reshape(exp_local, ep_count * capacity, width)
    gate_new = jnp.einsum("erd,edf->erf", rows, gate_weight, preferred_element_type=f32)
    up_new = jnp.einsum("erd,edf->erf", rows, up_weight, preferred_element_type=f32)
    row_weight = slot_weight.transpose(1, 0, 2).reshape(exp_local, ep_count * capacity, 1)
    hidden = (activate(gate_new, up_new) * row_weight).astype(bf16)
    expert_out = jnp.einsum(
        "erf,efd->erd", hidden, down_weight, preferred_element_type=f32
    ).astype(bf16)
    expert_out = expert_out.reshape(exp_local, ep_count, capacity, tp_count, feat_width)
    partial = jnp.einsum(
        "sect,escjf->sjtf", take, expert_out, preferred_element_type=f32
    ).astype(bf16)
    partial = partial.reshape(ep_count * tp_count, tok_rows, feat_width)
    if paired:
        return scatter_sum(partial, ep_count)
    mixed = lax.psum_scatter(partial, ("ep", "tp"), scatter_dimension=0, tiled=True)
    return mixed.reshape(tok_rows, feat_width)


def solution(mesh):
    in_specs = (
        P("ep", "tp"),
        P("ep", None),
        P("ep", None),
        P("ep", None, "tp"),
        P("ep", None, "tp"),
        P("ep", "tp", None),
    )
    out_specs = P("ep", "tp")
    return jax.shard_map(local, mesh=mesh, in_specs=in_specs, out_specs=out_specs, check_vma=False)
```

```python
import functools

import jax
import jax.numpy as jnp
from jax import lax
from jax.experimental import pallas as pl
from jax.experimental.pallas import tpu as pltpu
from jax.sharding import PartitionSpec as P


def activate(gate_acc, up_acc):
    return (up_acc + 1.0) * gate_acc * jax.nn.sigmoid(1.702 * gate_acc)


MESH = pl.DeviceIdType.MESH


class Place:
    def __init__(self, depth):
        self.depth = depth
        e, t = lax.axis_index("ep"), lax.axis_index("tp")
        self.z, self.x, self.y, self.c = e // 2, e % 2, t // 2, t % 2

    def device(self, k=0, dx=0, dy=0, dc=0):
        ep = (self.z + k) % self.depth * 2 + (self.x + dx) % 2
        tp = (self.y + dy) % 2 * 2 + (self.c + dc) % 2
        return ep, tp

    def block(self, k=0, dx=0, dy=0, dc=0):
        ep, tp = self.device(k, dx, dy, dc)
        return ep * 4 + tp

    def greet(self):
        barrier = pltpu.get_barrier_semaphore()
        near = [self.device(k=k) for k in range(1, self.depth)]
        near += [self.device(dx=1), self.device(dy=1), self.device(dc=1)]
        for who in near:
            pl.semaphore_signal(barrier, inc=1, device_id=who, device_id_type=MESH)
        pl.semaphore_wait(barrier, len(near))


def gather_kernel(depth, own, out, lane_recv, pair_recv, lane_send, pair_send, own_sem):
    here = Place(depth)
    half = own.shape[0] // 2
    sent = []

    def piece(k, dx, dy, part):
        rows = pl.ds(part * half, half)
        if (k, dx, dy) == (0, 0, 0):
            return own.at[rows]
        return out.at[here.block(k, dx, dy), rows]

    def lane_slot(k, dx, dy):
        ep, tp = here.device(k, dx, dy)
        return ep * 2 + tp // 2

    def push(k, dx, dy, part, to):
        rows = pl.ds(part * half, half)
        copy = pltpu.make_async_remote_copy(
            src_ref=piece(k, dx, dy, part), dst_ref=out.at[here.block(k, dx, dy), rows],
            send_sem=lane_send.at[len(sent)], recv_sem=lane_recv.at[lane_slot(k, dx, dy), part],
            device_id=to, device_id_type=MESH)
        copy.start()
        sent.append(copy)

    def pair(k, dx, dy, part):
        rows = pl.ds(part * half, half)
        slot = lane_slot(k, dx, dy)
        copy = pltpu.make_async_remote_copy(
            src_ref=piece(k, dx, dy, part), dst_ref=out.at[here.block(k, dx, dy), rows],
            send_sem=pair_send.at[slot, part], recv_sem=pair_recv.at[slot, part],
            device_id=here.device(dc=1), device_id_type=MESH)
        copy.start()

    def landed(k, dx, dy, part, to):
        rows = pl.ds(part * half, half)
        ref = out.at[here.block(k, dx, dy), rows]
        pltpu.make_async_remote_copy(
            src_ref=ref, dst_ref=ref, send_sem=lane_send.at[0],
            recv_sem=lane_recv.at[lane_slot(k, dx, dy), part],
            device_id=to, device_id_type=MESH).wait_recv()

    here.greet()
    over_x, over_y = here.device(dx=1), here.device(dy=1)
    for k in range(1, depth):
        for part in (0, 1):
            push(0, 0, 0, part, here.device(k=depth - k))
    store = pltpu.make_async_copy(own, out.at[here.block()], own_sem)
    store.start()
    for k in range(depth):
        if k:
            landed(k, 0, 0, 0, here.device(k=k))
            landed(k, 0, 0, 1, here.device(k=k))
        push(k, 0, 0, 0, over_x)
        push(k, 0, 0, 1, over_y)
        push(k, 0, 0, 0, over_y)
        push(k, 0, 0, 1, over_x)
        pair(k, 0, 0, 0)
        pair(k, 0, 0, 1)
        landed(k, 1, 0, 0, over_x)
        push(k, 1, 0, 0, over_y)
        pair(k, 1, 0, 0)
        landed(k, 0, 1, 1, over_y)
        push(k, 0, 1, 1, over_x)
        pair(k, 0, 1, 1)
    for k in range(depth):
        landed(k, 0, 1, 0, over_y)
        pair(k, 0, 1, 0)
        landed(k, 1, 0, 1, over_x)
        pair(k, 1, 0, 1)
        landed(k, 1, 1, 0, over_y)
        pair(k, 1, 1, 0)
        landed(k, 1, 1, 1, over_x)
        pair(k, 1, 1, 1)
    store.wait()
    for copy in sent:
        copy.wait_send()
    for k in range(depth):
        for dx in (0, 1):
            for dy in (0, 1):
                slot = lane_slot(k, dx, dy)
                for part in (0, 1):
                    rows = pl.ds(part * half, half)
                    copy = pltpu.make_async_remote_copy(
                        src_ref=piece(k, dx, dy, part),
                        dst_ref=out.at[here.block(k, dx, dy, 1), rows],
                        send_sem=pair_send.at[slot, part], recv_sem=pair_recv.at[slot, part],
                        device_id=here.device(dc=1), device_id_type=MESH)
                    copy.wait_send()
                    copy.wait_recv()


def gather_all(tokens, ep_count, tp_count):
    rows, width = tokens.shape
    depth = ep_count // 2
    blocks = ep_count * tp_count
    sends = 2 * (depth - 1) + 6 * depth
    dma = pltpu.SemaphoreType.DMA
    return pl.pallas_call(
        functools.partial(gather_kernel, depth),
        out_shape=jax.ShapeDtypeStruct((blocks, rows, width), tokens.dtype),
        in_specs=[pl.BlockSpec(memory_space=pltpu.VMEM)],
        out_specs=pl.BlockSpec(memory_space=pl.ANY),
        scratch_shapes=[dma((blocks // 2, 2)), dma((blocks // 2, 2)), dma((sends,)),
                        dma((blocks // 2, 2)), dma(())],
        compiler_params=pltpu.CompilerParams(collective_id=0, has_side_effects=True),
    )(tokens)


def scatter_kernel(depth, part_ref, out, acc, inc, from_y, from_x, last_x, last_y, from_z,
                   load_sem, pair_send, pair_recv, send_sem, recv_sem):
    here = Place(depth)
    rows = out.shape[0]
    half = rows // 2
    low, high = pl.ds(0, half), pl.ds(half, half)
    order = list(range(1, depth)) + [0]
    spread = ((1, 1), (0, 1), (1, 0), (0, 0))
    over_x, over_y = here.device(dx=1), here.device(dy=1)
    sent = []
    loads, pairs = {}, {}
    cell = lambda k, dx, dy: (k * 2 + dx) * 2 + dy

    def add(at, part, got):
        acc[at, part] = (acc[at, part].astype(jnp.float32) + got.astype(jnp.float32)).astype(acc.dtype)

    def send(src, dst, to):
        copy = pltpu.make_async_remote_copy(
            src_ref=src, dst_ref=dst, send_sem=send_sem.at[len(sent)],
            recv_sem=recv_sem.at[len(sent)], device_id=to, device_id_type=MESH)
        copy.start()
        sent.append(copy)
        return copy

    here.greet()
    for k in order:
        for dx, dy in spread:
            i = cell(k, dx, dy)
            pairs[i] = pltpu.make_async_remote_copy(
                src_ref=part_ref.at[here.block(k, dx, dy, 1)], dst_ref=inc.at[i],
                send_sem=pair_send.at[i], recv_sem=pair_recv.at[i],
                device_id=here.device(dc=1), device_id_type=MESH)
            pairs[i].start()
            loads[i] = pltpu.make_async_copy(
                part_ref.at[here.block(k, dx, dy)], acc.at[i], load_sem.at[i])
            loads[i].start()

    wait_for = {}

    def first(k):
        for dx, dy in spread:
            i = cell(k, dx, dy)
            loads[i].wait()
            pairs[i].wait_recv()
            add(i, pl.ds(0, rows), inc[i])
            if dy:
                wait_for["y", k, dx] = send(acc.at[i, low], from_y.at[k * 2 + dx], over_y)
            if dx:
                wait_for["x", k, dy] = send(acc.at[i, high], from_x.at[k * 2 + dy], over_x)

    def second(k):
        wait_for["y", k, 1].wait_recv()
        add(cell(k, 1, 0), low, from_y[k * 2 + 1])
        wait_for["lx", k] = send(acc.at[cell(k, 1, 0), low], last_x.at[k], over_x)
        wait_for["x", k, 1].wait_recv()
        add(cell(k, 0, 1), high, from_x[k * 2 + 1])
        wait_for["ly", k] = send(acc.at[cell(k, 0, 1), high], last_y.at[k], over_y)
        wait_for["y", k, 0].wait_recv()
        add(cell(k, 0, 0), low, from_y[k * 2])
        wait_for["x", k, 0].wait_recv()
        add(cell(k, 0, 0), high, from_x[k * 2])

    def third(k):
        wait_for["lx", k].wait_recv()
        add(cell(k, 0, 0), low, last_x[k])
        wait_for["ly", k].wait_recv()
        add(cell(k, 0, 0), high, last_y[k])
        if k:
            wait_for["z", k] = send(acc.at[cell(k, 0, 0)], from_z.at[k - 1], here.device(k=k))

    for i in range(depth + 2):
        if i < depth:
            first(order[i])
        if 0 <= i - 1 < depth:
            second(order[i - 1])
        if 0 <= i - 2:
            third(order[i - 2])
    total = acc[0].astype(jnp.float32)
    for k in range(1, depth):
        wait_for["z", k].wait_recv()
        total = total + from_z[k - 1].astype(jnp.float32)
    out[...] = total.astype(out.dtype)
    for copy in sent:
        copy.wait_send()
    for copy in pairs.values():
        copy.wait_send()


def scatter_sum(partial, ep_count):
    blocks, rows, width = partial.shape
    depth = ep_count // 2
    lane, half = blocks // 2, rows // 2
    sends = 6 * depth + depth - 1
    dma, kind = pltpu.SemaphoreType.DMA, partial.dtype
    return pl.pallas_call(
        functools.partial(scatter_kernel, depth),
        out_shape=jax.ShapeDtypeStruct((rows, width), kind),
        in_specs=[pl.BlockSpec(memory_space=pl.ANY)],
        out_specs=pl.BlockSpec(memory_space=pltpu.VMEM),
        scratch_shapes=[
            pltpu.VMEM((lane, rows, width), kind), pltpu.VMEM((lane, rows, width), kind),
            pltpu.VMEM((2 * depth, half, width), kind), pltpu.VMEM((2 * depth, half, width), kind),
            pltpu.VMEM((depth, half, width), kind), pltpu.VMEM((depth, half, width), kind),
            pltpu.VMEM((depth - 1, rows, width), kind),
            dma((lane,)), dma((lane,)), dma((lane,)), dma((sends,)), dma((sends,)),
        ],
        compiler_params=pltpu.CompilerParams(
            collective_id=1, has_side_effects=True, vmem_limit_bytes=48 * 1024 * 1024),
    )(partial)


def act_weighted(gate_acc, up_acc, weight):
    return (activate(gate_acc, up_acc) * weight).astype(jnp.bfloat16)


STEP = 240
def when(condition, run):
    if isinstance(condition, bool):
        if condition:
            run()
    else:
        pl.when(condition)(run)


PUSHES = (((0, 0), 0, "x"), ((0, 0), 1, "y"), ((0, 0), 0, "y"), ((0, 0), 1, "x"),
          ((1, 0), 0, "y"), ((0, 1), 1, "x"))


class Grid:
    def __init__(self):
        e, t = lax.axis_index("ep"), lax.axis_index("tp")
        self.ep, self.tp = e, t
        self.z, self.x, self.y, self.c = e // 2, e % 2, t // 2, t % 2
        self.mid = (self.z + 1) // 2 % 2

    def away(self, m, dx=0, dy=0, dc=0):
        z = (self.z // 2 + m // 2) % 2 * 2 + (self.z % 2 + m % 2) % 2
        return z * 2 + (self.x + dx) % 2, (self.y + dy) % 2 * 2 + (self.c + dc) % 2

    def device(self, k=0, dx=0, dy=0, dc=0):
        return self.away((k + self.mid * (4 - 2 * k)) % 4, dx, dy, dc)

    def seen(self, k):
        return 3 - 2 * self.mid if k % 2 else k


def fused_kernel(tokens, ids, scales, gate, up, down, out, buf, inc, from_y, from_x, last_x, last_y,
                 from_z, aside, passing, wide, deep, stage, rows, hid, take, back, weigh, place, all_ids, all_scales,
                 own_sem, w_sem, meta_send, meta_recv, z_send, z_recv, lane_send, lane_recv,
                 pair_send, pair_recv, sp_send, sp_recv, sx_send, sx_recv, sz_send, sz_recv,
                 cross_send, cross_recv, ferry_send, ferry_recv, detour_sem):
    f32, bf16 = jnp.float32, jnp.bfloat16
    here = Grid()
    depth = from_z.shape[0] + 1
    feat, tok = buf.shape[1], buf.shape[2]
    experts, cap = wide.shape[1], rows.shape[2] // wide.shape[1]
    ff, width = wide.shape[2], wide.shape[3]
    half = from_y.shape[1]
    low, high = pl.ds(0, half), pl.ds(half, feat - half)
    parts = (low, high)
    over = {"x": here.device(dx=1), "y": here.device(dy=1)}
    partner = here.device(dc=1)

    def cell(k, dx, dy, dc):
        return k * 8 + dx * 4 + dy * 2 + dc

    def remote(src, dst, send, recv, to):
        return pltpu.make_async_remote_copy(
            src_ref=src, dst_ref=dst, send_sem=send, recv_sem=recv,
            device_id=to, device_id_type=MESH)

    near, other = here.away(1), here.away(3)
    mid, end = here.mid == 1, here.mid == 0

    def flow(n, p):
        source, label = ((None, here.seen(1)), (None, 1), (1, 2), (3, 2), (2, 3))[n]
        src = tokens if source is None else buf.at[cell(source, 0, 0, 0)]
        return remote(src.at[parts[p]], buf.at[cell(label, 0, 0, 0), parts[p]],
                      z_send.at[n, p], z_recv.at[label, p], other if n in (1, 3) else near)

    def flow_start(n):
        flow(n, 0).start()
        flow(n, 1).start()

    def flow_sent(n):
        flow(n, 0).wait_send()
        flow(n, 1).wait_send()

    def arrive(k):
        for p in (0, 1):
            at = buf.at[cell(k, 0, 0, 0), parts[p]]
            remote(at, at, z_send.at[0, p], z_recv.at[k, p], near).wait_recv()

    def lane_push(k, n):
        (dx, dy), p, axis = PUSHES[n]
        to = (1 - dx, dy) if axis == "x" else (dx, 1 - dy)
        return remote(buf.at[cell(k, dx, dy, 0), parts[p]], buf.at[cell(k, *to, 0), parts[p]],
                      lane_send.at[k, n], lane_recv.at[k, n], over[axis])

    def pair(k, dx, dy, p):
        n = (dx * 2 + dy) * 2 + p
        return remote(buf.at[cell(k, dx, dy, 0), parts[p]], buf.at[cell(k, dx, dy, 1), parts[p]],
                      pair_send.at[k, n], pair_recv.at[k, n], partner)

    class Both:
        def __init__(self, *copies):
            self.copies = copies

        def start(self):
            for copy in self.copies:
                copy.start()

        def wait_recv(self):
            for copy in self.copies:
                copy.wait_recv()

        def wait_send(self):
            for copy in self.copies:
                copy.wait_send()

    def meta_push(k, dx, to_me=False):
        to = here.device(k=k, dx=dx)
        n = k * 2 + dx if to_me else here.seen(k) * 2 + dx
        return Both(remote(ids, all_ids.at[n], meta_send.at[0, n], meta_recv.at[0, n], to),
                    remote(scales, all_scales.at[n], meta_send.at[1, n], meta_recv.at[1, n], to))

    def gather_a(k):
        for n in range(4):
            lane_push(k, n).start()
        pair(k, 0, 0, 0).start()
        pair(k, 0, 0, 1).start()

    def column(k):
        if k == 3:
            when(end, lambda: arrive(3))
        else:
            arrive(k)
            when(mid, lambda: flow_start(2 if k == 1 else 4))
        gather_a(k)

    def turn_early():
        arrive(3)
        flow_start(3)

    def cross(n, p):
        source, label = ((0, 3), (2, 3), (1, 2))[n]
        return remote(buf.at[cell(source, 1, 1, 0), parts[p]],
                      buf.at[cell(label, 1, 1, 0), parts[p]],
                      cross_send.at[n, p], cross_recv.at[label - 2, p], near)

    def crossed(k, p):
        at = buf.at[cell(k, 1, 1, 0), parts[p]]
        remote(at, at, cross_send.at[0, p], cross_recv.at[k - 2, p], near).wait_recv()

    def inside(k):
        if isinstance(k, int):
            return (True, True, mid, False)[k]
        return k < 2 + here.mid

    def outside(k):
        if isinstance(k, int):
            return (False, False, end, True)[k]
        return k >= 2 + here.mid

    def gather_b(k):
        lane_push(k, 0).wait_recv()
        when(inside(k), lambda: lane_push(k, 4).start())
        pair(k, 1, 0, 0).start()
        lane_push(k, 1).wait_recv()
        when(inside(k), lambda: lane_push(k, 5).start())
        pair(k, 0, 1, 1).start()

    def gather_c(k, first):
        if first:
            lane_push(k, 2).wait_recv()
            pair(k, 0, 1, 0).start()
            lane_push(k, 3).wait_recv()
            pair(k, 1, 0, 1).start()
        else:
            for p in (0, 1):
                def relayed():
                    lane_push(k, 4 + p).wait_recv()
                    if isinstance(k, int):
                        if k == 0:
                            when(end, lambda: cross(0, p).start())
                        if k == 1:
                            when(mid, lambda: cross(2, p).start())
                    else:
                        when((k == 2) & mid, lambda: cross(1, p).start())
                when(inside(k), relayed)
                when(outside(k), lambda: crossed(k, p))
                pair(k, 1, 1, p).start()

    def gather_d(k):
        for dx in (0, 1):
            for dy in (0, 1):
                for p in (0, 1):
                    pair(k, dx, dy, p).wait_recv()

    def gather_sent(k):
        for n in range(4):
            lane_push(k, n).wait_send()

        def relayed():
            for p in (0, 1):
                lane_push(k, 4 + p).wait_send()
        when(inside(k), relayed)
        for at, n, side in ((0, 0, end), (2, 1, mid), (1, 2, mid)):
            @pl.when((k == at) & side)
            def _():
                cross(n, 0).wait_send()
                cross(n, 1).wait_send()

        @pl.when(mid)
        def _():
            for at, n in ((1, 2), (3, 3), (2, 4)):
                @pl.when(k == at)
                def _():
                    flow_sent(n)

        for dx in (0, 1):
            for dy in (0, 1):
                for p in (0, 1):
                    pair(k, dx, dy, p).wait_send()

    def give(k, dx, dy):
        n = dx * 2 + dy
        return remote(buf.at[cell(k, dx, dy, 1)], inc.at[k * 4 + n],
                      sp_send.at[k, n], sp_recv.at[k, n], partner)

    def hop(k, n):
        src, dst, axis = (
            (buf.at[cell(k, 1, 1, 0), low], from_y.at[k * 2 + 1], "y"),
            (buf.at[cell(k, 0, 1, 0), low], from_y.at[k * 2], "y"),
            (buf.at[cell(k, 1, 1, 0), high], from_x.at[k * 2 + 1], "x"),
            (buf.at[cell(k, 1, 0, 0), high], from_x.at[k * 2], "x"),
            (buf.at[cell(k, 1, 0, 0), low], last_x.at[k], "x"),
            (buf.at[cell(k, 0, 1, 0), high], last_y.at[k], "y"))[n]
        return remote(src, dst, sx_send.at[k, n], sx_recv.at[k, n], over[axis])

    def home(k, p, to_me=False):
        at = k if to_me else here.seen(k)
        return remote(buf.at[cell(k, 0, 0, 0), parts[p]], from_z.at[at - 1, parts[p]],
                      sz_send.at[k, p], sz_recv.at[at, p], here.device(k=k))

    def detour():
        return remote(buf.at[cell(3, 0, 0, 0), high], passing,
                      detour_sem.at[0], detour_sem.at[1], here.device(k=2))

    def onward():
        detour().wait_recv()
        add(cell(3, 0, 0, 0), high, passing[...])
        home(3, 1).start()

    def add(at, part, got):
        buf[at, part] = (buf[at, part].astype(f32) + got.astype(f32)).astype(bf16)

    def ferry(k):
        slot = (2, 1 - here.mid, 0)[k]
        return remote(buf.at[cell(k, 1, 1, 0)], aside.at[slot], ferry_send.at[k],
                      ferry_recv.at[slot], here.away(1 + 2 * here.mid) if k == 1 else near)

    def ferried(k, slot):
        remote(aside.at[slot], aside.at[slot], ferry_send.at[0], ferry_recv.at[slot],
               near).wait_recv()
        add(cell(k, 1, 1, 0), pl.ds(0, feat), aside[slot])

    def merge(k, dx, dy):
        give(k, dx, dy).wait_recv()
        add(cell(k, dx, dy, 0), pl.ds(0, feat), inc[k * 4 + dx * 2 + dy])

    def scatter_ferry(k):
        merge(k, 1, 1)
        ferry(k).start()

    def scatter_near(k):
        if k == 1:
            scatter_ferry(k)
        merge(k, 0, 1)
        hop(k, 1).start()
        hop(k, 5).start()
        merge(k, 1, 0)
        hop(k, 3).start()
        hop(k, 4).start()
        merge(k, 0, 0)

    def scatter_sides(k):
        merge(k, 0, 1)
        hop(k, 1).start()
        merge(k, 1, 0)
        hop(k, 3).start()
        merge(k, 0, 0)

    def scatter_corner(k):
        merge(k, 1, 1)
        if k == 0:
            when(mid, lambda: ferried(0, 0))
            when(mid, lambda: ferried(0, 1))
        if k == 3:
            when(end, lambda: ferried(3, 0))
            when(mid, lambda: ferried(3, 2))
        hop(k, 0).start()
        hop(k, 2).start()

    def scatter_far(k):
        scatter_corner(k)
        scatter_sides(k)

    def scatter_turn(k):
        hop(k, 0).wait_recv()
        add(cell(k, 1, 0, 0), low, from_y[k * 2 + 1])
        hop(k, 4).start()
        hop(k, 2).wait_recv()
        add(cell(k, 0, 1, 0), high, from_x[k * 2 + 1])
        hop(k, 5).start()

    def scatter_end(k):
        hop(k, 1).wait_recv()
        add(cell(k, 0, 0, 0), low, from_y[k * 2])
        hop(k, 3).wait_recv()
        add(cell(k, 0, 0, 0), high, from_x[k * 2])
        hop(k, 4).wait_recv()
        add(cell(k, 0, 0, 0), low, last_x[k])
        hop(k, 5).wait_recv()
        add(cell(k, 0, 0, 0), high, last_y[k])
        if k == 3:
            when(end, lambda: detour().start())
            home(3, 0).start()
            when(end, lambda: home(2, 1).start())
        elif k == 2:
            home(2, 0).start()
            when(mid, lambda: home(2, 1).start())
        elif k:
            home(k, 0).start()
            home(k, 1).start()

    own = [pltpu.make_async_copy(tokens, buf.at[cell(0, 0, 0, 0)], own_sem.at[0]),
           pltpu.make_async_copy(ids, all_ids.at[0], own_sem.at[1]),
           pltpu.make_async_copy(scales, all_scales.at[0], own_sem.at[2])]
    for copy in own:
        copy.start()
    barrier = pltpu.get_barrier_semaphore()
    greeted = [here.device(k=k, dx=dx) for k in range(depth) for dx in (0, 1) if k or dx]
    greeted += [over["y"], partner]
    for who in greeted:
        pl.semaphore_signal(barrier, inc=1, device_id=who, device_id_type=MESH)
    pl.semaphore_wait(barrier, len(greeted))
    for k in range(depth):
        for dx in (0, 1):
            if k or dx:
                meta_push(k, dx).start()
    flow_start(0)
    when(mid, lambda: flow_start(1))
    for copy in own:
        copy.wait()
    gather_a(0)
    loads = [pltpu.make_async_copy(ref.at[e], wide.at[side, e], w_sem.at[side, e])
             for side, ref in enumerate((gate, up)) for e in range(experts)]
    deeps = [pltpu.make_async_copy(down.at[e], stage, w_sem.at[2, e]) for e in range(experts)]
    deeps[0].start()
    for load in loads:
        load.start()
    place[...] = jnp.zeros(place.shape, f32)

    def turn(e):
        deeps[e].wait()
        for n in range(0, width, 256):
            size = min(256, width - n)
            eye = (lax.broadcasted_iota(jnp.int32, (size, size), 0)
                   == lax.broadcasted_iota(jnp.int32, (size, size), 1)).astype(f32).astype(bf16)
            got = lax.dot_general(eye, stage[:, pl.ds(n, size)], (((1,), (1,)), ((), ())),
                                  preferred_element_type=f32)
            deep[e, pl.ds(n, size), :] = got.astype(bf16)
        if e + 1 < experts:
            deeps[e + 1].start()

    turn(0)
    gather_b(0)
    when(mid, turn_early)
    column(1)
    ahead = (lax.broadcasted_iota(jnp.int32, (tok, tok), 0)
             < lax.broadcasted_iota(jnp.int32, (tok, tok), 1)).astype(f32).astype(bf16)
    slot_row = lax.broadcasted_iota(jnp.int32, (cap, tok), 0).astype(f32)
    slot_col = lax.broadcasted_iota(jnp.int32, (tok, cap), 1).astype(f32)
    row_at = lax.broadcasted_iota(jnp.int32, (8, tok), 0)

    def masks(k):
        picked = jnp.zeros((8, tok), f32)
        known = jnp.zeros((8, tok), f32)
        for dx in (0, 1):
            named, scaled = all_ids[k * 2 + dx], all_scales[k * 2 + dx]
            for e in range(experts):
                n = dx * experts + e
                hit = (named == here.ep * experts + e).astype(f32)
                chosen = jnp.sum(hit, axis=0, keepdims=True)
                picked = jnp.where(row_at == n, chosen, picked)
                held = jnp.sum(hit * scaled, axis=0, keepdims=True)
                known = jnp.where(row_at == 2 * experts + n, held, known)
        slot = jnp.dot(picked.astype(bf16), ahead, preferred_element_type=f32)
        slot = jnp.where(picked > 0.5, slot, -1.0)
        place[0:8, :] = jnp.where(row_at < 2 * experts, slot, known)
        turned = jnp.transpose(place[...])
        for dx in (0, 1):
            for e in range(experts):
                n = dx * experts + e
                at = pl.ds(e * cap, cap)
                take[k, dx, at, :] = (slot_row == slot[n:n + 1, :]).astype(f32).astype(bf16)
                hot = (slot_col == turned[:, n:n + 1]).astype(f32)
                back[k, dx, :, at] = hot.astype(bf16)
                held = turned[:, 2 * experts + n:2 * experts + n + 1]
                weigh[k, e, :, pl.ds(dx * cap, cap)] = jnp.broadcast_to(
                    jnp.sum(hot * held, axis=0, keepdims=True), (8, cap))

    def prepare(k, carry):
        @pl.when(k > 0)
        def _():
            meta_push(k, 0, True).wait_recv()
        meta_push(k, 1, True).wait_recv()
        masks(k)
        return carry

    for e in range(1, experts):
        turn(e)
    lax.fori_loop(0, depth, prepare, 0)
    gather_c(0, True)
    gather_c(0, False)
    for load in loads:
        load.wait()

    def block(k, dx, j):
        return cell(k, dx, (here.y + j // 2) % 2, (here.c + j % 2) % 2)

    def dispatch(k):
        for dx in (0, 1):
            for j in range(4):
                got = jnp.dot(buf[block(k, dx, j)], back[k, dx], preferred_element_type=f32)
                rows[dx, pl.ds(j * feat, feat), :] = got.astype(bf16)

    def enter(k, e):
        at = pl.ds(e * cap, cap)
        held = jnp.concatenate([rows[0, :, at], rows[1, :, at]], axis=1)
        for n in range(0, ff, STEP):
            part = pl.ds(n, min(STEP, ff - n))
            g = jnp.dot(wide[0, e, part, :], held, preferred_element_type=f32)
            u = jnp.dot(wide[1, e, part, :], held, preferred_element_type=f32)
            hid[part, :] = act_weighted(g, u, weigh[k, e, 0:1, :])

    def leave(e):
        at = pl.ds(e * cap, cap)
        for n in range(0, width, 2 * STEP):
            part = pl.ds(n, min(2 * STEP, width - n))
            got = jnp.dot(deep[e, part, :], hid[...], preferred_element_type=f32).astype(bf16)
            rows[0, part, at] = got[:, 0:cap]
            rows[1, part, at] = got[:, cap:2 * cap]

    def combine(k, dx):
        for j in range(4):
            got = jnp.dot(rows[dx, pl.ds(j * feat, feat), :], take[k, dx], preferred_element_type=f32)
            buf[block(k, dx, j)] = got.astype(bf16)

    def at(condition):
        return pl.when(condition)

    def plane(step, carry):
        last = depth - 1
        k = (step + here.mid) % depth
        ahead_of = (k < last) & (end | (k > 0))
        gather_d(k)
        dispatch(k)

        @at((k == 0) & mid)
        def _():
            scatter_corner(3)

        @at(k == last)
        def _():
            when(mid, lambda: scatter_ferry(2))
            when(end, lambda: scatter_corner(2))
        enter(k, 0)

        @at((k == 0) & mid)
        def _():
            scatter_sides(3)
            scatter_end(2)

        @at((k == 0) & end)
        def _():
            gather_b(1)

        @at(k == 1)
        def _():
            gather_b(2)
            column(3)

        @at(k == 2)
        def _():
            scatter_near(1)
            when(end, lambda: scatter_ferry(0))

        @at(k == last)
        def _():
            when(mid, lambda: scatter_near(2))
            when(end, lambda: scatter_sides(2))
            scatter_end(1)
        leave(0)

        @at((k == 0) & end)
        def _():
            column(2)

        @at((k == 0) & mid)
        def _():
            scatter_turn(3)
        enter(k, 1)

        @at(k == 2)
        def _():
            gather_b(3)

        @at(ahead_of)
        def _():
            gather_c(k + 1, True)

        @at((k == last) & end)
        def _():
            scatter_turn(2)

        leave(1)

        gather_sent(k)

        @at(ahead_of)
        def _():
            gather_c(k + 1, False)
        for dx in (1, 0):
            combine(k, dx)
            give(k, dx, 1).start()
            give(k, dx, 0).start()
        return carry

    @pl.when(mid)
    def _():
        gather_b(1)
        column(2)
        gather_c(1, True)
        gather_c(1, False)
    lax.fori_loop(0, depth, plane, 0)

    @pl.when(end)
    def _():
        scatter_far(3)
        scatter_end(2)
        scatter_turn(3)
        scatter_near(0)
        scatter_end(3)

    @pl.when(mid)
    def _():
        scatter_far(0)
        scatter_end(3)
        scatter_turn(0)
        onward()
    scatter_end(0)
    for p in (0, 1):
        total = buf[cell(0, 0, 0, 0), parts[p]].astype(f32)
        for k in range(1, depth - p):
            home(k, p, True).wait_recv()
            total = total + from_z[k - 1, parts[p]].astype(f32)
        if p == 0:
            out[low, :] = total.astype(out.dtype)
        else:
            when(end, lambda: out.__setitem__((high, slice(None)), total.astype(out.dtype)))

            @pl.when(mid)
            def _():
                home(3, 1, True).wait_recv()
                out[high, :] = (total + from_z[2, high].astype(f32)).astype(out.dtype)
    for k in range(depth):
        for dx in (0, 1):
            if k or dx:
                meta_push(k, dx).wait_send()
            for dy in (0, 1):
                give(k, dx, dy).wait_send()
        for n in (1, 3, 4, 5):
            hop(k, n).wait_send()

        def cornered():
            hop(k, 0).wait_send()
            hop(k, 2).wait_send()
        if k == 3:
            cornered()
        elif k != 1:
            when(end if k else mid, cornered)
        if k:
            home(k, 0).wait_send()
        if k in (1, 2):
            home(k, 1).wait_send()

    @pl.when(end)
    def _():
        detour().wait_send()
        ferry(0).wait_send()
    ferry(1).wait_send()
    flow_sent(0)

    @pl.when(mid)
    def _():
        ferry(2).wait_send()
        flow_sent(1)
        home(3, 1).wait_send()


def fused(tokens, expert_ids, combine_weights, gate_weight, up_weight, down_weight, depth, capacity):
    tok, feat = tokens.shape
    experts, width, ff = gate_weight.shape
    top = expert_ids.shape[1]
    f32, bf16 = jnp.float32, jnp.bfloat16
    half = -(-feat // 32) * 16
    rest = feat - half
    dma = pltpu.SemaphoreType.DMA
    scratch = [
        pltpu.VMEM((depth * 8, feat, tok), bf16), pltpu.VMEM((depth * 4, feat, tok), bf16),
        pltpu.VMEM((depth * 2, half, tok), bf16), pltpu.VMEM((depth * 2, rest, tok), bf16),
        pltpu.VMEM((depth, half, tok), bf16), pltpu.VMEM((depth, rest, tok), bf16),
        pltpu.VMEM((depth - 1, feat, tok), bf16), pltpu.VMEM((3, feat, tok), bf16),
        pltpu.VMEM((rest, tok), bf16),
        pltpu.VMEM((2, experts, ff, width), bf16), pltpu.VMEM((experts, width, ff), bf16),
        pltpu.VMEM((ff, width), bf16),
        pltpu.VMEM((2, width, experts * capacity), bf16),
        pltpu.VMEM((ff, 2 * capacity), bf16),
        pltpu.VMEM((depth, 2, experts * capacity, tok), bf16),
        pltpu.VMEM((depth, 2, tok, experts * capacity), bf16),
        pltpu.VMEM((depth, experts, 8, 2 * capacity), f32), pltpu.VMEM((128, tok), f32),
        pltpu.VMEM((depth * 2, top, tok), jnp.int32), pltpu.VMEM((depth * 2, top, tok), f32),
        dma((3,)), dma((3, experts)), dma((2, depth * 2)), dma((2, depth * 2)),
        dma((5, 2)), dma((depth, 2)), dma((depth, 6)), dma((depth, 6)),
        dma((depth, 8)), dma((depth, 8)), dma((depth, 4)), dma((depth, 4)),
        dma((depth, 6)), dma((depth, 6)), dma((depth, 2)), dma((depth, 2)),
        dma((3, 2)), dma((2, 2)), dma((3,)), dma((3,)), dma((2,)),
    ]
    mixed = pl.pallas_call(
        fused_kernel,
        out_shape=jax.ShapeDtypeStruct((feat, tok), bf16),
        in_specs=[pl.BlockSpec(memory_space=pl.ANY)] * 6,
        out_specs=pl.BlockSpec(memory_space=pltpu.VMEM),
        scratch_shapes=scratch,
        compiler_params=pltpu.CompilerParams(
            collective_id=0, has_side_effects=True, vmem_limit_bytes=63 * 1024 * 1024),
    )(tokens.T, expert_ids.T, combine_weights.T, gate_weight.transpose(0, 2, 1),
      up_weight.transpose(0, 2, 1), down_weight)
    return mixed.T


def local(tokens, expert_ids, combine_weights, gate_weight, up_weight, down_weight):
    ep_count = lax.axis_size("ep")
    tp_count = lax.axis_size("tp")
    exp_local = gate_weight.shape[0]
    experts = exp_local * ep_count
    tok_rows = expert_ids.shape[0]
    top_count = expert_ids.shape[1]
    capacity = 2 * tok_rows * top_count // experts
    feat_width = tokens.shape[1]
    ff_width = gate_weight.shape[2]
    width = feat_width * tp_count
    f32, bf16 = jnp.float32, jnp.bfloat16
    if (ep_count, tp_count, exp_local, top_count) == (8, 4, 2, 4) and capacity % 128 == 0:
        return fused(tokens, expert_ids, combine_weights, gate_weight, up_weight, down_weight,
                     ep_count // 2, capacity)

    ids_all = lax.all_gather(expert_ids.T, "ep")
    weights_all = lax.all_gather(combine_weights.T, "ep")
    first = lax.axis_index("ep") * exp_local
    mine = first + jnp.arange(exp_local, dtype=jnp.int32)
    hit = ids_all[:, None, :, :] == mine[None, :, None, None]
    chosen = jnp.any(hit, axis=2)
    weight = jnp.sum(jnp.where(hit, weights_all[:, None, :, :], 0.0), axis=2)

    ahead = jnp.triu(jnp.ones((tok_rows, tok_rows), bf16), 1)
    slot = lax.dot_general(
        chosen.reshape(-1, tok_rows).astype(bf16), ahead, (((1,), (0,)), ((), ())),
        preferred_element_type=f32,
    ).astype(jnp.int32).reshape(chosen.shape)
    place = jnp.where(chosen, slot, -1)
    take = place[:, :, None, :] == jnp.arange(capacity, dtype=jnp.int32)[None, None, :, None]
    slot_weight = jnp.sum(jnp.where(take, weight[:, :, None, :], 0.0), axis=3)
    take = take.astype(bf16)

    paired = tp_count == 2 * 2 and ep_count % 2 == 0
    spread = gather_all(tokens, ep_count, tp_count) if paired else lax.all_gather(
        tokens, ("ep", "tp")
    )
    gathered = spread.reshape(
        ep_count, tp_count, tok_rows, feat_width
    )
    routed = jnp.einsum(
        "sect,sjtf->escjf", take, gathered, preferred_element_type=f32
    ).astype(bf16)
    rows = routed.reshape(exp_local, ep_count * capacity, width)
    gate_new = jnp.einsum("erd,edf->erf", rows, gate_weight, preferred_element_type=f32)
    up_new = jnp.einsum("erd,edf->erf", rows, up_weight, preferred_element_type=f32)
    row_weight = slot_weight.transpose(1, 0, 2).reshape(exp_local, ep_count * capacity, 1)
    hidden = (activate(gate_new, up_new) * row_weight).astype(bf16)
    expert_out = jnp.einsum(
        "erf,efd->erd", hidden, down_weight, preferred_element_type=f32
    ).astype(bf16)
    expert_out = expert_out.reshape(exp_local, ep_count, capacity, tp_count, feat_width)
    partial = jnp.einsum(
        "sect,escjf->sjtf", take, expert_out, preferred_element_type=f32
    ).astype(bf16)
    partial = partial.reshape(ep_count * tp_count, tok_rows, feat_width)
    if paired:
        return scatter_sum(partial, ep_count)
    mixed = lax.psum_scatter(partial, ("ep", "tp"), scatter_dimension=0, tiled=True)
    return mixed.reshape(tok_rows, feat_width)


def solution(mesh):
    in_specs = (
        P("ep", "tp"),
        P("ep", None),
        P("ep", None),
        P("ep", None, "tp"),
        P("ep", None, "tp"),
        P("ep", "tp", None),
    )
    out_specs = P("ep", "tp")
    return jax.shard_map(local, mesh=mesh, in_specs=in_specs, out_specs=out_specs, check_vma=False)
```
